32 devices in a mesh: row: 4 (over z), col: 8 (over y, x, core).
Axes of the slice: x: 2, y: 2, z: 4, core: 2. Of those that a mesh axis runs over, the one named last changes fastest.
Arguments:
- obj: float32 [2, 1536, 3072], P(None, 'row', 'col'), may hold values from -6 to 6
- probe: float32 [4, 2, 128, 128], replicated, may hold values from -3 to 3
- positions: int32 [4, 8, 8, 2], P('row', 'col'), may hold values from 0 to 383
- counts: int32 [4, 8], P('row', 'col'), may hold values from 2 to 8, as said below
- offsets: int32 [8, 4], replicated, may hold values from 0 to 3, each once within a row
- measured: float32 [4, 8, 8, 128, 128], P('row', 'col'), may hold values from 0.3 to 5
Outputs:
- new_object: float32 [2, 1536, 3072], P(None, 'row', 'col')
The draws below stay inside these ranges and needn't reach their ends.
Inputs may be any that keep to these rules, and one draw needn't show every extreme that they name: `counts`: some device uses all 8 slots. At each scan slot the beams have different offsets.
All inputs are finite; a program needn't handle non-finite values.
Results may differ from the reference program's by a relative error of at most 0.0003.
Values sent between devices are 32-bit elements; how exact they have to be, the bound alone decides.
No kernel may reach another device: no remote copies, remote signals or barrier semaphores. Data moves between devices by JAX's collectives and lax.ppermute only.
A program may use at most 128 MiB of HBM per device.

```python
import math
import jax
import jax.numpy as jnp
from jax import lax

P_SIZE = 128
BEAMS = 4
TILE = 384
SCANS = 8
NR = 1536
NC = 3072
N_ROW = 4
N_COL = 8


def draw_counts(key, part):
    first_key, second_key = jax.random.split(key)
    drawn_counts = jax.random.randint(first_key, (N_ROW * N_COL,), max(1, SCANS // 4), SCANS + 1)
    chosen = jax.random.randint(second_key, (), 0, N_ROW * N_COL)
    filled = jnp.where(jnp.arange(N_ROW * N_COL) == chosen, SCANS, drawn_counts)
    return filled.reshape(N_ROW, N_COL).astype(jnp.int32)


def place_ends(drawn, key, least, high):
    longest = drawn.shape.index(max(drawn.shape))
    spots = []
    for shift in (0, 1):
        where = [jax.random.randint(jax.random.fold_in(key, axis), (), 0, length) for axis, length in enumerate(drawn.shape)]
        where[longest] = (where[longest] + shift) % drawn.shape[longest]
        spots.append(tuple(where))
    return drawn.at[spots[0]].set(least).at[spots[1]].set(high)


def levels(own_key, dims, shards, low, largest):
    factor_of = 1.0
    for dim, blocks in shards:
        steps = jax.random.uniform(jax.random.fold_in(jax.random.fold_in(own_key, 6), dim), (blocks,), jnp.float32, low / len(shards), largest / len(shards))
        factor_of = factor_of * jnp.repeat(jnp.exp(steps), dims[dim] // blocks).reshape((-1,) + (1,) * (len(dims) - 1 - dim))
    return factor_of


def centred(own_key, shape, scale, limit, cuts=(), held_as=jnp.bfloat16):
    array = scale * jax.random.normal(own_key, shape, jnp.float32)
    if cuts:
        array = array * levels(own_key, shape, cuts, -0.22, 0.18)
    return jnp.clip(array, -limit, limit).astype(held_as)


def setup_inputs(seed: int = 0) -> dict:
    key_list = jax.random.split(jax.random.key(seed), 7)
    obj = centred(key_list[0], (2, NR, NC), 1.0, 6.0, ((1, 4), (2, 8)), jnp.float32)
    probe = centred(key_list[1], (BEAMS, 2, P_SIZE, P_SIZE), 0.5, 3.0, (), jnp.float32)
    positions = place_ends(jax.random.randint(key_list[2], (N_ROW, N_COL, SCANS, 2), 0, TILE), jax.random.fold_in(key_list[2], 1), 0, TILE - 1).astype(jnp.int32)
    counts = draw_counts(jax.random.fold_in(key_list[6], 71), 0)
    offsets = jax.vmap(lambda own: jax.random.permutation(own, BEAMS))(jax.random.split(key_list[4], SCANS)).reshape((SCANS, BEAMS)).astype(jnp.int32)
    measured = jnp.clip(jnp.exp(math.log(5.0) - 2.8134107 * jax.random.uniform(key_list[5], (N_ROW, N_COL, SCANS, P_SIZE, P_SIZE), jnp.float32) ** levels(key_list[5], (N_ROW, N_COL, SCANS, P_SIZE, P_SIZE), ((0, 4), (1, 8)), -0.2, 0.2)), 0.3, 5.0)
    return {"obj": obj, "probe": probe, "positions": positions, "counts": counts, "offsets": offsets, "measured": measured}


EPSILON = 0.5
DAMPING = 0.5

def reference(obj, probe, positions, counts, offsets, measured):
    half = P_SIZE // 2
    padded = jnp.pad(obj, ((0, 0), (half, half), (half, half)))
    probe_c = probe[:, 0] + 1j * probe[:, 1]
    accum = jnp.zeros((3, NR + P_SIZE, NC + P_SIZE), obj.dtype)

    def device_step(accum, device):
        row_idx = (device // N_COL).astype(jnp.int32)
        col_idx = (device % N_COL).astype(jnp.int32)
        spots = positions[row_idx, col_idx]
        live = (jnp.arange(SCANS) < counts[row_idx, col_idx]).astype(obj.dtype)
        tile_rows = ((row_idx + offsets) % N_ROW * TILE).astype(jnp.int32)
        start_rows = (tile_rows + spots[:, 0][:, None]).astype(jnp.int32)
        start_cols = (col_idx * TILE + spots[:, 1][:, None] + jnp.zeros_like(start_rows)).astype(jnp.int32)
        zero_index = jnp.zeros((), jnp.int32)

        def cut(row_at, col_at):
            return lax.dynamic_slice(padded, (zero_index, row_at, col_at), (2, P_SIZE, P_SIZE))
        patches = jax.vmap(jax.vmap(cut))(start_rows, start_cols)
        patch_c = patches[:, :, 0] + 1j * patches[:, :, 1]
        exit_wave = probe_c[None] * patch_c
        far_wave = jnp.fft.fft2(exit_wave, norm='ortho')
        intensity = lax.optimization_barrier(jnp.sum(jnp.abs(far_wave) ** 2, axis=1))
        factor = measured[row_idx, col_idx] / jnp.sqrt(intensity + EPSILON)
        change = (jnp.fft.ifft2(far_wave * factor[:, None], norm='ortho') - exit_wave) * live[:, None, None, None]
        gradient = jnp.conj(probe_c)[None] * change
        illum = (jnp.abs(probe_c) ** 2)[None] * live[:, None, None, None]
        contrib = jnp.stack([jnp.real(gradient), jnp.imag(gradient), illum + jnp.zeros_like(jnp.real(gradient))], axis=2)

        def add_one(index, accum):
            slot = index // BEAMS
            beam = index % BEAMS
            start = (zero_index, start_rows[slot, beam], start_cols[slot, beam])
            current = lax.dynamic_slice(accum, start, (3, P_SIZE, P_SIZE))
            return lax.dynamic_update_slice(accum, current + contrib[slot, beam].astype(accum.dtype), start)
        accum = lax.fori_loop(0, SCANS * BEAMS, add_one, accum)
        return (accum, None)
    accum, unused = lax.scan(device_step, accum, jnp.arange(N_ROW * N_COL, dtype=jnp.int32))
    inner = accum[:, half:half + NR, half:half + NC]
    return obj + inner[:2] / (inner[2] + DAMPING)
```

```python
import functools
import math

import jax
import jax.numpy as jnp
import numpy as np
from jax import lax
from jax.experimental import pallas as pl
from jax.experimental.pallas import tpu as pltpu
from jax.sharding import PartitionSpec as P

EPSILON = 0.5
DAMPING = 0.5


SMEM = pl.BlockSpec(memory_space=pltpu.SMEM)
VMEM = pl.BlockSpec(memory_space=pltpu.VMEM)
F32 = jnp.float32
BF16 = jnp.bfloat16


def call(kernel, outs, specs, args, flops, scratch=(), aliases=None, name=None):
    return pl.pallas_call(
        kernel,
        out_shape=[jax.ShapeDtypeStruct(s, F32) for s in outs],
        in_specs=specs,
        out_specs=[VMEM] * len(outs),
        scratch_shapes=list(scratch),
        input_output_aliases=aliases or {},
        compiler_params=pltpu.CompilerParams(vmem_limit_bytes=28 * 2**20),
        cost_estimate=pl.CostEstimate(flops=flops, bytes_accessed=2**20, transcendentals=0),
        name=name,
    )(*args)


def dft_tables(length):
    index = np.arange(length)
    angle = (index[:, None] * index[None, :] % length) * (2.0 * math.pi / length)
    cos, sin = np.cos(angle) / math.sqrt(length), np.sin(angle) / math.sqrt(length)
    right = np.block([[cos, -sin], [sin, cos]])
    tables = []
    for table in (right, right.T):
        high = table.astype(BF16)
        tables += [high, (table - high.astype(np.float64)).astype(BF16)]
    return jnp.asarray(np.stack(tables))


def split(x):
    high = x.astype(BF16)
    return high, (x - high.astype(F32)).astype(BF16)


def dot3(a_high, a_low, b_high, b_low):
    dot = functools.partial(jnp.dot, preferred_element_type=F32)
    return dot(a_high, b_high) + (dot(a_low, b_high) + dot(a_high, b_low))


def lanes(rows, size):
    return lax.broadcasted_iota(jnp.int32, (rows, size), 1)


def turn(x):
    return pltpu.roll(x, x.shape[-1] // 2, 1)


def place(meta, slot, size):
    y, x = meta[2 * slot], meta[2 * slot + 1]
    return y, x // size, x % size


def frame_kernel(obj, top, bot, left, right, corner_l, corner_r, out):
    tiles, rows, size = out.shape[1:]
    half = size // 2
    inner = rows - size
    bands = (
        (0, half, top, corner_l, corner_r, 0),
        (half, inner, obj, left, right, 0),
        (half + inner, half, bot, corner_l, corner_r, half),
    )
    for start, count, body, side_l, side_r, at in bands:
        for first in range(0, count, half):
            low = lanes(half, size) < half
            src, side = pl.ds(first, half), pl.ds(at + first, half)
            for ch in range(2):
                parts = [turn(body[ch, src, t * size : (t + 1) * size]) for t in range(tiles - 1)]
                edge_l, edge_r = side_l[side, :], side_r[side, :]
                edge_l = edge_l if ch == 0 else turn(edge_l)
                edge_r = turn(edge_r) if ch == 0 else edge_r
                parts = [edge_l, *parts, edge_r]
                for t in range(tiles):
                    out[ch, t, pl.ds(start + first, half), :] = jnp.where(low, parts[t], parts[t + 1])


def forward_kernel(count, scans, *refs):
    metas, (beams, frame, probe, tables) = refs[:count], refs[count : count + 4]
    far, wave, power, x_high, x_low, y_high, y_low = refs[count + 4 :]
    size = probe.shape[-1]
    lane = lanes(size, size)
    for at in range(count):
        meta = metas[at]
        first = beams.shape[0] - count + at
        for slot in range(scans):
            y, tile, shift = place(meta, slot, size)
            beam = beams[first, slot]
            back = lax.rem(size - shift, size)
            patch = []
            for ch in range(2):
                near = pltpu.roll(frame[ch, tile, pl.ds(y, size), :], back, 1)
                rest = pltpu.roll(frame[ch, tile + 1, pl.ds(y, size), :], back, 1)
                patch.append(jnp.where(lane < size - shift, near, rest))
            probe_re, probe_im = probe[beam, 0], probe[beam, 1]
            waves = (
                probe_re * patch[0] - probe_im * patch[1],
                probe_re * patch[1] + probe_im * patch[0],
            )
            rows = slice(slot * size, (slot + 1) * size)
            for ch in range(2):
                wave[at, slot, ch] = waves[ch]
                columns = slice(ch * size, (ch + 1) * size)
                x_high[rows, columns], x_low[rows, columns] = split(waves[ch])
        for slot in range(0, scans, 2):
            rows = slice(slot * size, (slot + 2) * size)
            mid = dot3(x_high[rows, :], x_low[rows, :], tables[0], tables[1])
            for sub in range(2):
                columns = slice((slot + sub) * size, (slot + sub + 1) * size)
                for ch in range(2):
                    piece = mid[sub * size : (sub + 1) * size, ch * size : (ch + 1) * size]
                    into = slice(ch * size, (ch + 1) * size)
                    y_high[into, columns], y_low[into, columns] = split(piece)
            columns = slice(slot * size, (slot + 2) * size)
            result = dot3(tables[2], tables[3], y_high[:, columns], y_low[:, columns])
            far[at, :, columns] = result
            for sub in range(2):
                inside = slice(sub * size, (sub + 1) * size)
                re, im = result[:size, inside], result[size:, inside]
                power[at, slot + sub] = re * re + im * im


def add_patch(total, channel, meta, slot, value, size, lane):
    y, tile, shift = place(meta, slot, size)
    moved = pltpu.roll(value, shift, 1)
    rows = pl.ds(y, size)
    total[channel, tile, rows, :] += jnp.where(lane >= shift, moved, 0.0)
    total[channel, tile + 1, rows, :] += jnp.where(lane < shift, moved, 0.0)


def write_sides(total, side_l, side_r):
    channels, tiles, rows, size = total.shape
    half = size // 2
    low = lanes(rows, size) < half
    if channels == 1:
        side_l[...] = total[0, 0]
        side_r[...] = turn(total[0, tiles - 1])
    else:
        side_l[...] = jnp.where(low, total[0, 0], turn(total[1, 0]))
        side_r[...] = jnp.where(low, turn(total[0, tiles - 1]), total[1, tiles - 1])


def own_columns(total, channel, rows, low):
    tiles = total.shape[1]
    turned = [turn(total[channel, t, rows, :]) for t in range(tiles)]
    return [jnp.where(low, turned[t], turned[t + 1]) for t in range(tiles - 1)]


def write_rims(total, rim_top, rim_bot):
    channels, tiles, rows, size = total.shape
    half = size // 2
    low = lanes(half, size) < half
    for ch in range(channels):
        for start, out in ((0, rim_top), (rows - half, rim_bot)):
            for t, value in enumerate(own_columns(total, ch, pl.ds(start, half), low)):
                out[ch, :, t * size : (t + 1) * size] = value


def backward_kernel(scans, which, fresh, last, *refs):
    meta, beams, far, wave, factor, probe, tables = refs[:7]
    refs = refs[7:]
    if not fresh:
        refs = refs[1:]
    total, refs = refs[0], refs[1:]
    if last:
        (side_l, side_r, rim_top, rim_bot), refs = refs[:4], refs[4:]
    x_high, x_low, y_high, y_low = refs
    size = probe.shape[-1]
    lane = lanes(size, size)
    if fresh:
        total[...] = jnp.zeros_like(total)
    for slot in range(0, scans, 2):
        for sub in range(2):
            columns = slice((slot + sub) * size, (slot + sub + 1) * size)
            scale = factor[slot + sub]
            for ch in range(2):
                into = slice(ch * size, (ch + 1) * size)
                y_high[into, columns], y_low[into, columns] = split(far[into, columns] * scale)
        columns = slice(slot * size, (slot + 2) * size)
        mid = dot3(tables[0], tables[1], y_high[:, columns], y_low[:, columns])
        for sub in range(2):
            rows = slice((slot + sub) * size, (slot + sub + 1) * size)
            for ch in range(2):
                piece = mid[ch * size : (ch + 1) * size, sub * size : (sub + 1) * size]
                into = slice(ch * size, (ch + 1) * size)
                x_high[rows, into], x_low[rows, into] = split(piece)
        rows = slice(slot * size, (slot + 2) * size)
        result = dot3(x_high[rows, :], x_low[rows, :], tables[2], tables[3])
        for sub in range(2):
            live = (slot + sub < meta[2 * scans]).astype(F32)
            beam = beams[which, slot + sub]
            probe_re, probe_im = probe[beam, 0], probe[beam, 1]
            inside = slice(sub * size, (sub + 1) * size)
            change_re = (result[inside, :size] - wave[slot + sub, 0]) * live
            change_im = (result[inside, size:] - wave[slot + sub, 1]) * live
            grad_re = probe_re * change_re + probe_im * change_im
            grad_im = probe_re * change_im - probe_im * change_re
            add_patch(total, 0, meta, slot + sub, grad_re, size, lane)
            add_patch(total, 1, meta, slot + sub, grad_im, size, lane)
    if last:
        write_sides(total, side_l, side_r)
        write_rims(total, rim_top, rim_bot)


def weight_kernel(count, scans, *refs):
    metas, beams, probe = refs[:count], refs[count], refs[count + 1]
    total, side_l, side_r, rim_top, rim_bot = refs[count + 2 :]
    size = probe.shape[-1]
    lane = lanes(size, size)
    total[...] = jnp.zeros_like(total)
    for at in range(count):

        def add(slot, carry, at=at):
            beam = beams[at, slot]
            live = (slot < metas[at][2 * scans]).astype(F32)
            probe_re, probe_im = probe[beam, 0], probe[beam, 1]
            value = (probe_re * probe_re + probe_im * probe_im) * live
            add_patch(total, 0, metas[at], slot, value, size, lane)
            return carry

        lax.fori_loop(0, scans, add, 0)
    write_sides(total, side_l, side_r)
    write_rims(total, rim_top, rim_bot)


def gathered(total, side_l, side_r, in_top, in_bot, in_ctop, in_cbot, channel, chunk, half):
    channels, tiles, rows, size = total.shape
    chunks = (rows - size) // half
    low = lanes(half, size) < half
    ext = pl.ds((chunk + 1) * half, half)
    values = own_columns(total, channel, ext, low)

    def add_sides(from_l, from_r):
        from_l = from_l if channel == 0 else turn(from_l)
        from_r = turn(from_r) if channel == 0 else from_r
        values[0] += jnp.where(low, from_l, 0.0)
        values[-1] += jnp.where(low, 0.0, from_r)

    add_sides(side_l[ext, :], side_r[ext, :])
    for at, rim, corner in ((0, in_top, in_ctop), (chunks - 1, in_bot, in_cbot)):
        if chunk == at:
            for t in range(tiles - 1):
                values[t] += rim[channel, :, t * size : (t + 1) * size]
            add_sides(corner[0], corner[1])
    return values


def final_kernel(*refs):
    obj, out = refs[0], refs[-1]
    grads, weights = refs[1:8], refs[8:15]
    size = grads[0].shape[-1]
    half = size // 2
    for chunk in range(obj.shape[1] // half):
        weight = gathered(*weights, 0, chunk, half)
        scale = [1.0 / (w + DAMPING) for w in weight]
        rows = slice(chunk * half, (chunk + 1) * half)
        for ch in range(2):
            for t, value in enumerate(gathered(*grads, ch, chunk, half)):
                columns = slice(t * size, (t + 1) * size)
                out[ch, rows, columns] = obj[ch, rows, columns] + value * scale[t]


def line(axis, by):
    count = lax.axis_size(axis)
    return [(i, i + by) for i in range(count) if 0 <= i + by < count]


def ring(axis, by):
    count = lax.axis_size(axis)
    return [(i, (i + by) % count) for i in range(count)]


def send_rims(side_l, side_r, rim_top, rim_bot):
    rows, size = side_l.shape
    half = size // 2
    in_r = lax.ppermute(side_l, "col", line("col", -1))
    in_l = lax.ppermute(side_r, "col", line("col", 1))
    in_bot = lax.ppermute(rim_top, "row", line("row", -1))
    in_top = lax.ppermute(rim_bot, "row", line("row", 1))
    corner_top = jnp.stack([in_l[:half], in_r[:half]])
    corner_bot = jnp.stack([in_l[rows - half :], in_r[rows - half :]])
    in_cbot = lax.ppermute(corner_top, "row", line("row", -1))
    in_ctop = lax.ppermute(corner_bot, "row", line("row", 1))
    return in_l, in_r, in_top, in_bot, in_ctop, in_cbot


def on_device(obj, probe, positions, counts, offsets, measured):
    beams_count, _, size, _ = probe.shape
    scans = positions.shape[2]
    half = size // 2
    tile_rows, tile_columns = obj.shape[1:]
    rows, tiles = tile_rows + size, tile_columns // size + 1
    tables = dft_tables(size)

    meta = jnp.concatenate([positions.reshape(-1), counts.reshape(-1)])
    metas = [meta] + [lax.ppermute(meta, "row", ring("row", k)) for k in range(1, beams_count)]
    beams = jnp.argmax(offsets[None] == jnp.arange(beams_count)[:, None, None], axis=2).astype(jnp.int32)

    def packed(x):
        return jnp.concatenate([x[0], x[1]], axis=1)

    top = lax.ppermute(obj[:, tile_rows - half :], "row", line("row", 1))
    bot = lax.ppermute(obj[:, :half], "row", line("row", -1))
    left = lax.ppermute(packed(obj[:, :, tile_columns - half :]), "col", line("col", 1))
    right = lax.ppermute(packed(obj[:, :, :half]), "col", line("col", -1))
    rims = jnp.concatenate([top, bot], axis=1)
    corner_l = lax.ppermute(packed(rims[:, :, tile_columns - half :]), "col", line("col", 1))
    corner_r = lax.ppermute(packed(rims[:, :, :half]), "col", line("col", -1))
    (frame,) = call(
        frame_kernel,
        [(2, tiles, rows, size)],
        [VMEM] * 7,
        (obj, top, bot, left, right, corner_l, corner_r),
        10**6,
        name="frame",
    )

    work = [
        pltpu.VMEM((scans * size, 2 * size), BF16),
        pltpu.VMEM((scans * size, 2 * size), BF16),
        pltpu.VMEM((2 * size, scans * size), BF16),
        pltpu.VMEM((2 * size, scans * size), BF16),
    ]
    flops = scans * 2 * 3 * 2 * size * (2 * size) ** 2

    def forward(which, selected):
        return call(
            functools.partial(forward_kernel, 1, scans),
            [(1, 2 * size, scans * size), (1, scans, 2, size, size), (1, scans, size, size)],
            [SMEM, SMEM, VMEM, VMEM, VMEM],
            (metas[which], selected, frame, probe, tables),
            flops,
            work,
            name=f"forward{which}",
        )

    far, wave = {}, {}
    power = None
    for which in reversed(range(beams_count)):
        far[which], wave[which], own = forward(which, beams[which : which + 1])
        power = own[0] if power is None else own[0] + lax.ppermute(power, "row", ring("row", -1))
    factor = measured[0, 0] / jnp.sqrt(power + EPSILON)

    weights = call(
        functools.partial(weight_kernel, beams_count, scans),
        [(1, tiles, rows, size), (rows, size), (rows, size), (1, half, tile_columns), (1, half, tile_columns)],
        [SMEM] * (beams_count + 1) + [VMEM],
        (*metas, beams, probe),
        flops,
        name="weight",
    )
    weight_in = send_rims(*weights[1:])

    total = None
    for which in range(beams_count):
        if which:
            factor = lax.ppermute(factor, "row", ring("row", 1))
        fresh, last = which == 0, which == beams_count - 1
        outs = [(2, tiles, rows, size)]
        if last:
            outs += [(rows, size), (rows, size), (2, half, tile_columns), (2, half, tile_columns)]
        args = [metas[which], beams, far[which][0], wave[which][0], factor, probe, tables]
        specs = [SMEM, SMEM] + [VMEM] * 5
        if not fresh:
            args, specs = args + [total], specs + [VMEM]
        total, *sides = call(
            functools.partial(backward_kernel, scans, which, fresh, last),
            outs,
            specs,
            args,
            flops,
            work,
            {} if fresh else {7: 0},
            name=f"backward{which}",
        )
    grad_in = send_rims(*sides)

    (new_object,) = call(
        final_kernel,
        [obj.shape],
        [VMEM] * 15,
        (obj, total, *grad_in, weights[0], *weight_in),
        10**6,
        name="final",
    )
    return new_object


def solution(mesh):
    return jax.shard_map(
        on_device,
        mesh=mesh,
        in_specs=(
            P(None, "row", "col"),
            P(),
            P("row", "col", None, None),
            P("row", "col"),
            P(),
            P("row", "col", None, None, None),
        ),
        out_specs=P(None, "row", "col"),
        check_vma=False,
    )
```

```python
import functools
import math

import jax
import jax.numpy as jnp
import numpy as np
from jax import lax
from jax.experimental import pallas as pl
from jax.experimental.pallas import tpu as pltpu
from jax.sharding import PartitionSpec as P

EPSILON = 0.5
DAMPING = 0.5


SMEM = pl.BlockSpec(memory_space=pltpu.SMEM)
VMEM = pl.BlockSpec(memory_space=pltpu.VMEM)
F32 = jnp.float32
BF16 = jnp.bfloat16


def call(kernel, outs, specs, args, flops, scratch=(), aliases=None, name=None):
    return pl.pallas_call(
        kernel,
        out_shape=[jax.ShapeDtypeStruct(s, F32) for s in outs],
        in_specs=specs,
        out_specs=[VMEM] * len(outs),
        scratch_shapes=list(scratch),
        input_output_aliases=aliases or {},
        compiler_params=pltpu.CompilerParams(vmem_limit_bytes=28 * 2**20),
        cost_estimate=pl.CostEstimate(flops=flops, bytes_accessed=2**20, transcendentals=0),
        name=name,
    )(*args)


def dft_tables(length):
    index = np.arange(length)
    angle = (index[:, None] * index[None, :] % length) * (2.0 * math.pi / length)
    cos, sin = np.cos(angle) / math.sqrt(length), np.sin(angle) / math.sqrt(length)
    right = np.block([[cos, -sin], [sin, cos]])
    tables = []
    for table in (right, right.T):
        high = table.astype(BF16)
        tables += [high, (table - high.astype(np.float64)).astype(BF16)]
    return jnp.asarray(np.stack(tables))


def split(x):
    high = x.astype(BF16)
    return high, (x - high.astype(F32)).astype(BF16)


def dot3(a_high, a_low, b_high, b_low):
    dot = functools.partial(jnp.dot, preferred_element_type=F32)
    return dot(a_high, b_high) + (dot(a_low, b_high) + dot(a_high, b_low))


def lanes(rows, size):
    return lax.broadcasted_iota(jnp.int32, (rows, size), 1)


def turn(x):
    return pltpu.roll(x, x.shape[-1] // 2, 1)


def place(metas, which, slot, size):
    y, x = metas[which, 2 * slot], metas[which, 2 * slot + 1]
    return y, x // size, x % size


def frame_kernel(obj, top, bot, left, right, corner_l, corner_r, out):
    tiles, rows, size = out.shape[1:]
    half = size // 2
    inner = rows - size
    bands = (
        (0, half, top, corner_l, corner_r, 0),
        (half, inner, obj, left, right, 0),
        (half + inner, half, bot, corner_l, corner_r, half),
    )
    for start, count, body, side_l, side_r, at in bands:
        for first in range(0, count, half):
            low = lanes(half, size) < half
            src, side = pl.ds(first, half), pl.ds(at + first, half)
            for ch in range(2):
                parts = [turn(body[ch, src, t * size : (t + 1) * size]) for t in range(tiles - 1)]
                edge_l, edge_r = side_l[side, :], side_r[side, :]
                edge_l = edge_l if ch == 0 else turn(edge_l)
                edge_r = turn(edge_r) if ch == 0 else edge_r
                parts = [edge_l, *parts, edge_r]
                for t in range(tiles):
                    out[ch, t, pl.ds(start + first, half), :] = jnp.where(low, parts[t], parts[t + 1])


def forward_kernel(parts, *refs):
    metas, beams, frame, probe, tables = refs[:5]
    outs, (x_high, x_low, y_high, y_low) = refs[5:-4], refs[-4:]
    size = probe.shape[-1]
    lane = lanes(size, size)
    for at, (which, start, slots) in enumerate(parts):
        far, wave, power = outs[3 * at : 3 * at + 3]
        for index in range(slots):
            slot = start + index
            y, tile, shift = place(metas, which, slot, size)
            beam = beams[which, slot]
            back = lax.rem(size - shift, size)
            patch = []
            for ch in range(2):
                near = pltpu.roll(frame[ch, tile, pl.ds(y, size), :], back, 1)
                rest = pltpu.roll(frame[ch, tile + 1, pl.ds(y, size), :], back, 1)
                patch.append(jnp.where(lane < size - shift, near, rest))
            probe_re, probe_im = probe[beam, 0], probe[beam, 1]
            waves = (
                probe_re * patch[0] - probe_im * patch[1],
                probe_re * patch[1] + probe_im * patch[0],
            )
            rows = slice(index * size, (index + 1) * size)
            for ch in range(2):
                wave[index, ch] = waves[ch]
                columns = slice(ch * size, (ch + 1) * size)
                x_high[rows, columns], x_low[rows, columns] = split(waves[ch])
        for slot in range(0, slots, 2):
            rows = slice(slot * size, (slot + 2) * size)
            mid = dot3(x_high[rows, :], x_low[rows, :], tables[0], tables[1])
            for sub in range(2):
                columns = slice((slot + sub) * size, (slot + sub + 1) * size)
                for ch in range(2):
                    piece = mid[sub * size : (sub + 1) * size, ch * size : (ch + 1) * size]
                    into = slice(ch * size, (ch + 1) * size)
                    y_high[into, columns], y_low[into, columns] = split(piece)
            columns = slice(slot * size, (slot + 2) * size)
            result = dot3(tables[2], tables[3], y_high[:, columns], y_low[:, columns])
            far[:, columns] = result
            for sub in range(2):
                inside = slice(sub * size, (sub + 1) * size)
                re, im = result[:size, inside], result[size:, inside]
                power[slot + sub] = re * re + im * im


def add_patch(total, channel, y, tile, shift, value, lane):
    moved = pltpu.roll(value, shift, 1)
    rows = pl.ds(y, value.shape[0])
    total[channel, tile, rows, :] += jnp.where(lane >= shift, moved, 0.0)
    total[channel, tile + 1, rows, :] += jnp.where(lane < shift, moved, 0.0)


def write_sides(total, side_l, side_r):
    channels, tiles, rows, size = total.shape
    half = size // 2
    low = lanes(rows, size) < half
    if channels == 1:
        side_l[...] = total[0, 0]
        side_r[...] = turn(total[0, tiles - 1])
    else:
        side_l[...] = jnp.where(low, total[0, 0], turn(total[1, 0]))
        side_r[...] = jnp.where(low, turn(total[0, tiles - 1]), total[1, tiles - 1])


def own_columns(total, channel, rows, low):
    tiles = total.shape[1]
    turned = [turn(total[channel, t, rows, :]) for t in range(tiles)]
    return [jnp.where(low, turned[t], turned[t + 1]) for t in range(tiles - 1)]


def write_rims(total, rim_top, rim_bot):
    channels, tiles, rows, size = total.shape
    half = size // 2
    low = lanes(half, size) < half
    for ch in range(channels):
        for start, out in ((0, rim_top), (rows - half, rim_bot)):
            for t, value in enumerate(own_columns(total, ch, pl.ds(start, half), low)):
                out[ch, :, t * size : (t + 1) * size] = value


def backward_kernel(parts, fresh, last, *refs):
    metas, beams, probe, tables = refs[:4]
    inputs, refs = refs[4 : 4 + 3 * len(parts)], refs[4 + 3 * len(parts) :]
    if not fresh:
        refs = refs[1:]
    total, refs = refs[0], refs[1:]
    if last:
        (side_l, side_r, rim_top, rim_bot), refs = refs[:4], refs[4:]
    x_high, x_low, y_high, y_low = refs
    size = probe.shape[-1]
    scans = beams.shape[1]
    lane = lanes(size, size)
    if fresh:
        total[...] = jnp.zeros_like(total)
    for at, (which, start, slots) in enumerate(parts):
        far, wave, factor = inputs[3 * at : 3 * at + 3]
        for slot in range(0, slots, 2):
            for sub in range(2):
                columns = slice((slot + sub) * size, (slot + sub + 1) * size)
                scale = factor[slot + sub]
                for ch in range(2):
                    into = slice(ch * size, (ch + 1) * size)
                    y_high[into, columns], y_low[into, columns] = split(far[into, columns] * scale)
            columns = slice(slot * size, (slot + 2) * size)
            mid = dot3(tables[0], tables[1], y_high[:, columns], y_low[:, columns])
            for sub in range(2):
                rows = slice((slot + sub) * size, (slot + sub + 1) * size)
                for ch in range(2):
                    piece = mid[ch * size : (ch + 1) * size, sub * size : (sub + 1) * size]
                    into = slice(ch * size, (ch + 1) * size)
                    x_high[rows, into], x_low[rows, into] = split(piece)
            rows = slice(slot * size, (slot + 2) * size)
            result = dot3(x_high[rows, :], x_low[rows, :], tables[2], tables[3])
            for sub in range(2):
                true_slot = start + slot + sub
                live = (true_slot < metas[which, 2 * scans]).astype(F32)
                beam = beams[which, true_slot]
                probe_re, probe_im = probe[beam, 0], probe[beam, 1]
                inside = slice(sub * size, (sub + 1) * size)
                change_re = (result[inside, :size] - wave[slot + sub, 0]) * live
                change_im = (result[inside, size:] - wave[slot + sub, 1]) * live
                grad_re = probe_re * change_re + probe_im * change_im
                grad_im = probe_re * change_im - probe_im * change_re
                spot = place(metas, which, true_slot, size)
                add_patch(total, 0, *spot, grad_re, lane)
                add_patch(total, 1, *spot, grad_im, lane)
    if last:
        write_sides(total, side_l, side_r)
        write_rims(total, rim_top, rim_bot)


def weight_kernel(steps, spans, fresh, *refs):
    metas, (inside, beams, probe) = refs[: len(spans)], refs[len(spans) : len(spans) + 3]
    total = refs[-1]
    _, tiles, rows, size = total.shape
    half, scans = size // 2, beams.shape[1]
    own_rows, own_columns = rows - 2 * size, (tiles - 2) * size
    lane = lanes(size, size)
    if fresh:
        total[...] = jnp.zeros_like(total)
    else:
        total[...] = refs[-2][...]
    for meta, across in zip(metas, spans):
        for row, down, which in steps:

            def add(slot, carry, meta=meta, across=across, row=row, down=down, which=which):
                y = meta[row, 2 * slot] + (down * own_rows + half)
                x = meta[row, 2 * slot + 1] + (across * own_columns + half)
                near = (y > 0) & (y < rows - size) & (x > 0) & (x < (tiles - 1) * size)
                live = (slot < meta[row, 2 * scans]) & (inside[down + 1] > 0)

                @pl.when(near & live)
                def _():
                    beam = beams[which, slot]
                    probe_re, probe_im = probe[beam, 0], probe[beam, 1]
                    value = probe_re * probe_re + probe_im * probe_im
                    add_patch(total, 0, y, x // size, x % size, value, lane)

                return carry

            lax.fori_loop(0, scans, add, 0)


def gathered(total, side_l, side_r, in_top, in_bot, in_ctop, in_cbot, channel, chunk, half):
    channels, tiles, rows, size = total.shape
    chunks = (rows - size) // half
    low = lanes(half, size) < half
    ext = pl.ds((chunk + 1) * half, half)
    values = own_columns(total, channel, ext, low)

    def add_sides(from_l, from_r):
        from_l = from_l if channel == 0 else turn(from_l)
        from_r = turn(from_r) if channel == 0 else from_r
        values[0] += jnp.where(low, from_l, 0.0)
        values[-1] += jnp.where(low, 0.0, from_r)

    add_sides(side_l[ext, :], side_r[ext, :])
    for at, rim, corner in ((0, in_top, in_ctop), (chunks - 1, in_bot, in_cbot)):
        if chunk == at:
            for t in range(tiles - 1):
                values[t] += rim[channel, :, t * size : (t + 1) * size]
            add_sides(corner[0], corner[1])
    return values


def final_kernel(*refs):
    obj, weight, out = refs[0], refs[1], refs[-1]
    grads = refs[2:9]
    size = grads[0].shape[-1]
    half = size // 2
    tiles = obj.shape[2] // size
    for chunk in range(obj.shape[1] // half):
        wide = pl.ds(size + chunk * half, half)
        scale = [1.0 / (weight[0, t + 1, wide, :] + DAMPING) for t in range(tiles)]
        rows = slice(chunk * half, (chunk + 1) * half)
        for ch in range(2):
            for t, value in enumerate(gathered(*grads, ch, chunk, half)):
                columns = slice(t * size, (t + 1) * size)
                out[ch, rows, columns] = obj[ch, rows, columns] + value * scale[t]


def line(axis, by):
    count = lax.axis_size(axis)
    return [(i, i + by) for i in range(count) if 0 <= i + by < count]


def ring(axis, by):
    count = lax.axis_size(axis)
    return [(i, (i + by) % count) for i in range(count)]


def send_rims(side_l, side_r, rim_top, rim_bot):
    rows, size = side_l.shape
    half = size // 2
    in_r = lax.ppermute(side_l, "col", line("col", -1))
    in_l = lax.ppermute(side_r, "col", line("col", 1))
    in_bot = lax.ppermute(rim_top, "row", line("row", -1))
    in_top = lax.ppermute(rim_bot, "row", line("row", 1))
    corner_top = jnp.stack([in_l[:half], in_r[:half]])
    corner_bot = jnp.stack([in_l[rows - half :], in_r[rows - half :]])
    in_cbot = lax.ppermute(corner_top, "row", line("row", -1))
    in_ctop = lax.ppermute(corner_bot, "row", line("row", 1))
    return in_l, in_r, in_top, in_bot, in_ctop, in_cbot


def on_device(obj, probe, positions, counts, offsets, measured):
    offsets_count, _, size, _ = probe.shape
    scans = positions.shape[2]
    half = size // 2
    tile_rows, tile_columns = obj.shape[1:]
    rows, tiles = tile_rows + size, tile_columns // size + 1
    row_count = lax.axis_size("row")
    tables = dft_tables(size)

    def packed(x):
        return jnp.concatenate([x[0], x[1]], axis=1)

    top = lax.ppermute(obj[:, tile_rows - half :], "row", line("row", 1))
    bot = lax.ppermute(obj[:, :half], "row", line("row", -1))
    left = lax.ppermute(packed(obj[:, :, tile_columns - half :]), "col", line("col", 1))
    right = lax.ppermute(packed(obj[:, :, :half]), "col", line("col", -1))

    meta = jnp.concatenate([positions.reshape(1, -1), counts.reshape(1, -1)], axis=1)
    kept = min(row_count, offsets_count + 2)
    shifts = [k if k <= offsets_count else k - kept for k in range(kept)]
    metas = jnp.concatenate([meta] + [lax.ppermute(meta, "row", ring("row", k)) for k in shifts[1:]])
    beams = jnp.argmax(offsets[None] == jnp.arange(offsets_count)[:, None, None], axis=2).astype(jnp.int32)

    rims = jnp.concatenate([top, bot], axis=1)
    corner_l = lax.ppermute(packed(rims[:, :, tile_columns - half :]), "col", line("col", 1))
    corner_r = lax.ppermute(packed(rims[:, :, :half]), "col", line("col", -1))
    (frame,) = call(
        frame_kernel,
        [(2, tiles, rows, size)],
        [VMEM] * 7,
        (obj, top, bot, left, right, corner_l, corner_r),
        10**6,
        name="frame",
    )

    slots = scans // 2
    halves = ((0, slots), (slots, scans - slots))
    work = [
        pltpu.VMEM((slots * size, 2 * size), BF16),
        pltpu.VMEM((slots * size, 2 * size), BF16),
        pltpu.VMEM((2 * size, slots * size), BF16),
        pltpu.VMEM((2 * size, slots * size), BF16),
    ]
    flops = slots * 2 * 3 * 2 * size * (2 * size) ** 2

    far, wave, power = {}, {}, {}

    def forward(parts, metas):
        outs = []
        for _, _, count in parts:
            outs += [(2 * size, count * size), (count, 2, size, size), (count, size, size)]
        results = call(
            functools.partial(forward_kernel, parts),
            outs,
            [SMEM, SMEM, VMEM, VMEM, VMEM],
            (metas, beams, frame, probe, tables),
            flops * len(parts),
            work,
            name="forward",
        )
        for at, (which, start, _) in enumerate(parts):
            far[which, start], wave[which, start], power[which, start] = results[3 * at : 3 * at + 3]

    most = offsets_count - 1
    forward([(most, *halves[0])], metas)
    forward([(most, *halves[1])], metas)
    forward([(which, *part) for which in reversed(range(most)) for part in halves], metas)
    sums = {start: power[most, start] for start, _ in halves}
    for which in reversed(range(most)):
        for start, _ in halves:
            sums[start] = power[which, start] + lax.ppermute(sums[start], "row", ring("row", -1))
    factors = {
        start: measured[0, 0, start : start + count] / jnp.sqrt(sums[start] + EPSILON) for start, count in halves
    }

    late, _ = lax.optimization_barrier((metas, power[0, 0]))
    spans = {0: metas}
    spans[-1] = lax.ppermute(late, "col", line("col", 1))
    spans[1] = lax.ppermute(late, "col", line("col", -1))
    at_row = lax.axis_index("row")
    inside = jnp.stack([at_row > 0, at_row >= 0, at_row < row_count - 1]).astype(jnp.int32)
    steps = [
        ((which - down) % row_count if row_count <= offsets_count + 1 else (which - down) % kept, down, which)
        for down in (-1, 0, 1)
        for which in range(offsets_count)
    ]
    weight = None
    for across in (0, -1, 1):
        (weight,) = call(
            functools.partial(weight_kernel, steps, (across,), weight is None),
            [(1, tiles + 1, tile_rows + 2 * size, size)],
            [SMEM, SMEM, SMEM, VMEM] + ([] if weight is None else [VMEM]),
            (spans[across], inside, beams, probe) + (() if weight is None else (weight,)),
            flops,
            aliases={} if weight is None else {4: 0},
            name="weight",
        )

    total = None
    for which in range(offsets_count):
        if which:
            factors = {start: lax.ppermute(value, "row", ring("row", 1)) for start, value in factors.items()}
        groups = [[part] for part in halves] if which == most else [list(halves)]
        for group in groups:
            fresh, last = total is None, which == most and group[-1] == halves[-1]
            outs = [(2, tiles, rows, size)]
            if last:
                outs += [(rows, size), (rows, size), (2, half, tile_columns), (2, half, tile_columns)]
            args = [metas, beams, probe, tables]
            for start, _ in group:
                args += [far[which, start], wave[which, start], factors[start]]
            specs = [SMEM, SMEM] + [VMEM] * (len(args) - 2)
            if not fresh:
                args, specs = args + [total], specs + [VMEM]
            total, *sides = call(
                functools.partial(backward_kernel, [(which, *part) for part in group], fresh, last),
                outs,
                specs,
                args,
                flops * len(group),
                work,
                {} if fresh else {len(args) - 1: 0},
                name="backward",
            )
    grad_in = send_rims(*sides)

    (new_object,) = call(
        final_kernel,
        [obj.shape],
        [VMEM] * 9,
        (obj, weight, total, *grad_in),
        10**6,
        name="final",
    )
    return new_object


def solution(mesh):
    return jax.shard_map(
        on_device,
        mesh=mesh,
        in_specs=(
            P(None, "row", "col"),
            P(),
            P("row", "col", None, None),
            P("row", "col"),
            P(),
            P("row", "col", None, None, None),
        ),
        out_specs=P(None, "row", "col"),
        check_vma=False,
    )
```

```python
import functools
import math

import jax
import jax.numpy as jnp
import numpy as np
from jax import lax
from jax.experimental import pallas as pl
from jax.experimental.pallas import tpu as pltpu
from jax.sharding import PartitionSpec as P

EPSILON = 0.5
DAMPING = 0.5


SMEM = pl.BlockSpec(memory_space=pltpu.SMEM)
VMEM = pl.BlockSpec(memory_space=pltpu.VMEM)
F32 = jnp.float32
BF16 = jnp.bfloat16


def call(kernel, outs, specs, args, flops, scratch=(), aliases=None, name=None):
    return pl.pallas_call(
        kernel,
        out_shape=[jax.ShapeDtypeStruct(s, F32) for s in outs],
        in_specs=specs,
        out_specs=[VMEM] * len(outs),
        scratch_shapes=list(scratch),
        input_output_aliases=aliases or {},
        compiler_params=pltpu.CompilerParams(vmem_limit_bytes=16 * 2**20),
        cost_estimate=pl.CostEstimate(flops=flops, bytes_accessed=2**20, transcendentals=0),
        name=name,
    )(*args)


def dft_tables(length):
    index = np.arange(length)
    angle = (index[:, None] * index[None, :] % length) * (2.0 * math.pi / length)
    cos, sin = np.cos(angle) / math.sqrt(length), np.sin(angle) / math.sqrt(length)
    right = np.block([[cos, -sin], [sin, cos]])
    tables = []
    for table in (right, right.T):
        high = table.astype(BF16)
        tables += [high, (table - high.astype(np.float64)).astype(BF16)]
    return jnp.asarray(np.stack(tables))


def split(x):
    high = x.astype(BF16)
    return high, (x - high.astype(F32)).astype(BF16)


def dot3(a_high, a_low, b_high, b_low):
    dot = functools.partial(jnp.dot, preferred_element_type=F32)
    return dot(a_high, b_high) + (dot(a_low, b_high) + dot(a_high, b_low))


def lanes(rows, size):
    return lax.broadcasted_iota(jnp.int32, (rows, size), 1)


def turn(x):
    return pltpu.roll(x, x.shape[-1] // 2, 1)


def place(metas, which, slot, size):
    y, x = metas[which, 2 * slot], metas[which, 2 * slot + 1]
    return y, x // size, x % size


def frame_kernel(obj, top, bot, left, right, out):
    tiles, rows, size = out.shape[1:]
    half = size // 2
    low = lanes(half, size) < half
    for at in range(0, rows, half):
        body, src = obj, pl.ds(at - half, half)
        if at == 0:
            body, src = top, pl.ds(0, half)
        elif at == rows - half:
            body, src = bot, pl.ds(0, half)
        here = pl.ds(at, half)
        for ch in range(2):
            parts = [turn(body[ch, src, t * size : (t + 1) * size]) for t in range(tiles - 1)]
            edge_l, edge_r = left[here, :], right[here, :]
            edge_l = edge_l if ch == 0 else turn(edge_l)
            edge_r = turn(edge_r) if ch == 0 else edge_r
            parts = [edge_l, *parts, edge_r]
            for t in range(tiles):
                out[ch, t, here, :] = jnp.where(low, parts[t], parts[t + 1])


def forward_kernel(parts, *refs):
    metas, beams, frame, probe, tables = refs[:5]
    outs, (x_high, x_low, y_high, y_low) = refs[5:-4], refs[-4:]
    size = probe.shape[-1]
    lane = lanes(size, size)
    for at, (which, start, slots) in enumerate(parts):
        far, wave, power = outs[3 * at : 3 * at + 3]
        for index in range(slots):
            slot = start + index
            y, tile, shift = place(metas, which % metas.shape[0], slot, size)
            beam = beams[which, slot]
            back = lax.rem(size - shift, size)
            patch = []
            for ch in range(2):
                near = pltpu.roll(frame[ch, tile, pl.ds(y, size), :], back, 1)
                rest = pltpu.roll(frame[ch, tile + 1, pl.ds(y, size), :], back, 1)
                patch.append(jnp.where(lane < size - shift, near, rest))
            probe_re, probe_im = probe[beam, 0], probe[beam, 1]
            waves = (
                probe_re * patch[0] - probe_im * patch[1],
                probe_re * patch[1] + probe_im * patch[0],
            )
            rows = slice(index * size, (index + 1) * size)
            for ch in range(2):
                wave[index, ch] = waves[ch]
                columns = slice(ch * size, (ch + 1) * size)
                x_high[rows, columns], x_low[rows, columns] = split(waves[ch])
        for slot in range(0, slots, 2):
            rows = slice(slot * size, (slot + 2) * size)
            mid = dot3(x_high[rows, :], x_low[rows, :], tables[0], tables[1])
            for sub in range(2):
                columns = slice((slot + sub) * size, (slot + sub + 1) * size)
                for ch in range(2):
                    piece = mid[sub * size : (sub + 1) * size, ch * size : (ch + 1) * size]
                    into = slice(ch * size, (ch + 1) * size)
                    y_high[into, columns], y_low[into, columns] = split(piece)
            columns = slice(slot * size, (slot + 2) * size)
            result = dot3(tables[2], tables[3], y_high[:, columns], y_low[:, columns])
            far[:, columns] = result
            for sub in range(2):
                inside = slice(sub * size, (sub + 1) * size)
                re, im = result[:size, inside], result[size:, inside]
                power[slot + sub] = re * re + im * im


def add_patch(total, channel, y, tile, shift, value, lane):
    moved = pltpu.roll(value, shift, 1)
    rows = pl.ds(y, value.shape[0])
    total[channel, tile, rows, :] += jnp.where(lane >= shift, moved, 0.0)
    total[channel, tile + 1, rows, :] += jnp.where(lane < shift, moved, 0.0)


def write_sides(total, side_l, side_r):
    channels, tiles, rows, size = total.shape
    half = size // 2
    low = lanes(rows, size) < half
    if channels == 1:
        side_l[...] = total[0, 0]
        side_r[...] = turn(total[0, tiles - 1])
    else:
        side_l[...] = jnp.where(low, total[0, 0], turn(total[1, 0]))
        side_r[...] = jnp.where(low, turn(total[0, tiles - 1]), total[1, tiles - 1])


def own_columns(total, channel, rows, low):
    tiles = total.shape[1]
    turned = [turn(total[channel, t, rows, :]) for t in range(tiles)]
    return [jnp.where(low, turned[t], turned[t + 1]) for t in range(tiles - 1)]


def write_rims(total, rim_top, rim_bot):
    channels, tiles, rows, size = total.shape
    half = size // 2
    low = lanes(half, size) < half
    for ch in range(channels):
        for start, out in ((0, rim_top), (rows - half, rim_bot)):
            for t, value in enumerate(own_columns(total, ch, pl.ds(start, half), low)):
                out[ch, :, t * size : (t + 1) * size] = value


def backward_kernel(parts, fresh, last, *refs):
    metas, beams, probe, tables = refs[:4]
    inputs, refs = refs[4 : 4 + 3 * len(parts)], refs[4 + 3 * len(parts) :]
    if not fresh:
        refs = refs[1:]
    total, refs = refs[0], refs[1:]
    if last:
        (side_l, side_r, rim_top, rim_bot), refs = refs[:4], refs[4:]
    x_high, x_low, y_high, y_low = refs
    size = probe.shape[-1]
    scans = beams.shape[1]
    lane = lanes(size, size)
    if fresh:
        total[...] = jnp.zeros_like(total)
    for at, (which, start, slots) in enumerate(parts):
        far, wave, factor = inputs[3 * at : 3 * at + 3]
        for slot in range(0, slots, 2):
            for sub in range(2):
                columns = slice((slot + sub) * size, (slot + sub + 1) * size)
                scale = factor[slot + sub]
                for ch in range(2):
                    into = slice(ch * size, (ch + 1) * size)
                    y_high[into, columns], y_low[into, columns] = split(far[into, columns] * scale)
            columns = slice(slot * size, (slot + 2) * size)
            mid = dot3(tables[0], tables[1], y_high[:, columns], y_low[:, columns])
            for sub in range(2):
                rows = slice((slot + sub) * size, (slot + sub + 1) * size)
                for ch in range(2):
                    piece = mid[ch * size : (ch + 1) * size, sub * size : (sub + 1) * size]
                    into = slice(ch * size, (ch + 1) * size)
                    x_high[rows, into], x_low[rows, into] = split(piece)
            rows = slice(slot * size, (slot + 2) * size)
            result = dot3(x_high[rows, :], x_low[rows, :], tables[2], tables[3])
            for sub in range(2):
                true_slot = start + slot + sub
                live = (true_slot < metas[which, 2 * scans]).astype(F32)
                beam = beams[which, true_slot]
                probe_re, probe_im = probe[beam, 0], probe[beam, 1]
                inside = slice(sub * size, (sub + 1) * size)
                change_re = (result[inside, :size] - wave[slot + sub, 0]) * live
                change_im = (result[inside, size:] - wave[slot + sub, 1]) * live
                grad_re = probe_re * change_re + probe_im * change_im
                grad_im = probe_re * change_im - probe_im * change_re
                spot = place(metas, which, true_slot, size)
                add_patch(total, 0, *spot, grad_re, lane)
                add_patch(total, 1, *spot, grad_im, lane)
    if last:
        write_sides(total, side_l, side_r)
        write_rims(total, rim_top, rim_bot)


def weight_kernel(steps, spans, fresh, *refs):
    metas, (inside, beams, probe) = refs[: len(spans)], refs[len(spans) : len(spans) + 3]
    total = refs[-1]
    _, tiles, rows, size = total.shape
    half, scans = size // 2, beams.shape[1]
    own_rows, own_columns = rows - 2 * size, (tiles - 2) * size
    lane = lanes(size, size)
    if fresh:
        total[...] = jnp.zeros_like(total)
    else:
        total[...] = refs[-2][...]
    for meta, across in zip(metas, spans):
        for row, down, which in steps:

            def add(slot, carry, meta=meta, across=across, row=row, down=down, which=which):
                y = meta[row, 2 * slot] + (down * own_rows + half)
                x = meta[row, 2 * slot + 1] + (across * own_columns + half)
                near = (y > 0) & (y < rows - size) & (x > 0) & (x < (tiles - 1) * size)
                live = (slot < meta[row, 2 * scans]) & (inside[down + 1] > 0)

                @pl.when(near & live)
                def _():
                    beam = beams[which, slot]
                    probe_re, probe_im = probe[beam, 0], probe[beam, 1]
                    value = probe_re * probe_re + probe_im * probe_im
                    add_patch(total, 0, y, x // size, x % size, value, lane)

                return carry

            lax.fori_loop(0, scans, add, 0)


def gathered(total, side_l, side_r, in_top, in_bot, in_ctop, in_cbot, channel, chunk, half):
    channels, tiles, rows, size = total.shape
    chunks = (rows - size) // half
    low = lanes(half, size) < half
    ext = pl.ds((chunk + 1) * half, half)
    values = own_columns(total, channel, ext, low)

    def add_sides(from_l, from_r):
        from_l = from_l if channel == 0 else turn(from_l)
        from_r = turn(from_r) if channel == 0 else from_r
        values[0] += jnp.where(low, from_l, 0.0)
        values[-1] += jnp.where(low, 0.0, from_r)

    add_sides(side_l[ext, :], side_r[ext, :])
    for at, rim, corner in ((0, in_top, in_ctop), (chunks - 1, in_bot, in_cbot)):
        if chunk == at:
            for t in range(tiles - 1):
                values[t] += rim[channel, :, t * size : (t + 1) * size]
            add_sides(corner[0], corner[1])
    return values


def final_kernel(*refs):
    obj, weight, out = refs[0], refs[1], refs[-1]
    grads = refs[2:9]
    size = grads[0].shape[-1]
    half = size // 2
    tiles = obj.shape[2] // size
    for chunk in range(obj.shape[1] // half):
        wide = pl.ds(size + chunk * half, half)
        scale = [1.0 / (weight[0, t + 1, wide, :] + DAMPING) for t in range(tiles)]
        rows = slice(chunk * half, (chunk + 1) * half)
        for ch in range(2):
            for t, value in enumerate(gathered(*grads, ch, chunk, half)):
                columns = slice(t * size, (t + 1) * size)
                out[ch, rows, columns] = obj[ch, rows, columns] + value * scale[t]


def line(axis, by):
    count = lax.axis_size(axis)
    return [(i, i + by) for i in range(count) if 0 <= i + by < count]


def ring(axis, by):
    count = lax.axis_size(axis)
    return [(i, (i + by) % count) for i in range(count)]


def send_rims(side_l, side_r, rim_top, rim_bot):
    rows, size = side_l.shape
    half = size // 2
    in_r = lax.ppermute(side_l, "col", line("col", -1))
    in_l = lax.ppermute(side_r, "col", line("col", 1))
    in_bot = lax.ppermute(rim_top, "row", line("row", -1))
    in_top = lax.ppermute(rim_bot, "row", line("row", 1))
    corner_top = jnp.stack([in_l[:half], in_r[:half]])
    corner_bot = jnp.stack([in_l[rows - half :], in_r[rows - half :]])
    in_cbot = lax.ppermute(corner_top, "row", line("row", -1))
    in_ctop = lax.ppermute(corner_bot, "row", line("row", 1))
    return in_l, in_r, in_top, in_bot, in_ctop, in_cbot


def on_device(obj, probe, positions, counts, offsets, measured):
    offsets_count, _, size, _ = probe.shape
    scans = positions.shape[2]
    half = size // 2
    tile_rows, tile_columns = obj.shape[1:]
    rows, tiles = tile_rows + size, tile_columns // size + 1
    row_count = lax.axis_size("row")
    tables = dft_tables(size)

    def packed(x):
        return jnp.concatenate([x[0], x[1]], axis=1)

    top = lax.ppermute(obj[:, tile_rows - half :], "row", line("row", 1))
    bot = lax.ppermute(obj[:, :half], "row", line("row", -1))
    edges = lax.optimization_barrier((packed(obj[:, :, :half]), packed(obj[:, :, tile_columns - half :])))
    edge_l, edge_r = (
        jnp.concatenate([packed(top[:, :, part]), edge, packed(bot[:, :, part])])
        for part, edge in ((slice(0, half), edges[0]), (slice(tile_columns - half, None), edges[1]))
    )
    left = lax.ppermute(edge_r, "col", line("col", 1))
    right = lax.ppermute(edge_l, "col", line("col", -1))
    (frame,) = call(
        frame_kernel,
        [(2, tiles, rows, size)],
        [VMEM] * 5,
        (obj, top, bot, left, right),
        10**6,
        name="frame",
    )

    meta = jnp.concatenate([positions.reshape(1, -1), counts.reshape(1, -1)], axis=1)
    beams = jnp.argmax(offsets[None] == jnp.arange(offsets_count)[:, None, None], axis=2).astype(jnp.int32)
    most = offsets_count - 1
    first_metas = lax.ppermute(meta, "row", ring("row", most))

    slots = scans // 2
    halves = ((0, slots), (slots, scans - slots))
    work = [
        pltpu.VMEM((slots * size, 2 * size), BF16),
        pltpu.VMEM((slots * size, 2 * size), BF16),
        pltpu.VMEM((2 * size, slots * size), BF16),
        pltpu.VMEM((2 * size, slots * size), BF16),
    ]
    flops = slots * 2 * 3 * 2 * size * (2 * size) ** 2

    far, wave, power = {}, {}, {}

    def forward(parts, metas):
        outs = []
        for _, _, count in parts:
            outs += [(2 * size, count * size), (count, 2, size, size), (count, size, size)]
        results = call(
            functools.partial(forward_kernel, parts),
            outs,
            [SMEM, SMEM, VMEM, VMEM, VMEM],
            (metas, beams, frame, probe, tables),
            flops * len(parts),
            work,
            name="forward",
        )
        for at, (which, start, _) in enumerate(parts):
            far[which, start], wave[which, start], power[which, start] = results[3 * at : 3 * at + 3]

    forward([(most, *halves[0])], first_metas)
    sums = {0: power[most, 0]}
    arrived = {0: lax.ppermute(sums[0], "row", ring("row", -1))}
    after, _ = lax.optimization_barrier((first_metas, power[most, 0]))
    forward([(most, *halves[1])], after)
    later, _ = lax.optimization_barrier((meta, power[most, slots]))
    kept = min(row_count, offsets_count + 2)
    shifts = [k if k <= offsets_count else k - kept for k in range(kept)]
    metas = [meta] + [
        first_metas if k == most else lax.ppermute(later, "row", ring("row", k)) for k in shifts[1:]
    ]
    metas = jnp.concatenate(metas)
    sums[slots] = power[most, slots]
    arrived[slots] = lax.ppermute(sums[slots], "row", ring("row", -1))
    forward([(which, *part) for which in reversed(range(most)) for part in halves], metas)
    for which in reversed(range(most)):
        for start, _ in halves:
            sums[start] = power[which, start] + arrived[start]
            if which:
                arrived[start] = lax.ppermute(sums[start], "row", ring("row", -1))
    factors = {
        start: measured[0, 0, start : start + count] / jnp.sqrt(sums[start] + EPSILON) for start, count in halves
    }

    at_row = lax.axis_index("row")
    inside = jnp.stack([at_row > 0, at_row >= 0, at_row < row_count - 1]).astype(jnp.int32)
    steps = [
        ((which - down) % row_count if row_count <= offsets_count + 1 else (which - down) % kept, down, which)
        for down in (-1, 0, 1)
        for which in range(offsets_count)
    ]
    late, _ = lax.optimization_barrier((metas, power[0, 0]))
    spans = {
        0: late,
        -1: lax.ppermute(late, "col", line("col", 1)),
        1: lax.ppermute(late, "col", line("col", -1)),
    }

    def add_weight(across, weight, after):
        span, _ = lax.optimization_barrier((spans[across], after))
        (weight,) = call(
            functools.partial(weight_kernel, steps, (across,), weight is None),
            [(1, tiles + 1, tile_rows + 2 * size, size)],
            [SMEM, SMEM, SMEM, VMEM] + ([] if weight is None else [VMEM]),
            (span, inside, beams, probe) + (() if weight is None else (weight,)),
            flops,
            aliases={} if weight is None else {4: 0},
            name="weight",
        )
        return weight

    weight, weight_steps = None, [0, -1, 1]
    total = None
    for which in range(offsets_count):
        if which:
            for start, _ in halves:
                value = lax.ppermute(factors[start], "row", ring("row", 1))
                if weight_steps and which < most:
                    weight = add_weight(weight_steps.pop(0), weight, factors[start])
                    value, weight = lax.optimization_barrier((value, weight))
                factors[start] = value
        groups = [[part] for part in halves] if which == most else [list(halves)]
        for group in groups:
            fresh, last = total is None, which == most and group[-1] == halves[-1]
            outs = [(2, tiles, rows, size)]
            if last:
                outs += [(rows, size), (rows, size), (2, half, tile_columns), (2, half, tile_columns)]
            args = [metas, beams, probe, tables]
            for start, _ in group:
                args += [far[which, start], wave[which, start], factors[start]]
            specs = [SMEM, SMEM] + [VMEM] * (len(args) - 2)
            if not fresh:
                args, specs = args + [total], specs + [VMEM]
            total, *sides = call(
                functools.partial(backward_kernel, [(which, *part) for part in group], fresh, last),
                outs,
                specs,
                args,
                flops * len(group),
                work,
                {} if fresh else {len(args) - 1: 0},
                name="backward",
            )
    grad_in = send_rims(*sides)

    (new_object,) = call(
        final_kernel,
        [obj.shape],
        [VMEM] * 9,
        (obj, weight, total, *grad_in),
        10**6,
        name="final",
    )
    return new_object


def solution(mesh):
    return jax.shard_map(
        on_device,
        mesh=mesh,
        in_specs=(
            P(None, "row", "col"),
            P(),
            P("row", "col", None, None),
            P("row", "col"),
            P(),
            P("row", "col", None, None, None),
        ),
        out_specs=P(None, "row", "col"),
        check_vma=False,
    )
```

```python
import functools
import math

import jax
import jax.numpy as jnp
import numpy as np
from jax import lax
from jax.experimental import pallas as pl
from jax.experimental.pallas import tpu as pltpu
from jax.sharding import PartitionSpec as P

EPSILON = 0.5
DAMPING = 0.5


SMEM = pl.BlockSpec(memory_space=pltpu.SMEM)
VMEM = pl.BlockSpec(memory_space=pltpu.VMEM)
F32 = jnp.float32
BF16 = jnp.bfloat16


def call(kernel, outs, specs, args, flops, scratch=(), aliases=None):
    return pl.pallas_call(
        kernel,
        out_shape=[jax.ShapeDtypeStruct(s, F32) for s in outs],
        in_specs=specs,
        out_specs=[VMEM] * len(outs),
        scratch_shapes=list(scratch),
        input_output_aliases=aliases or {},
        compiler_params=pltpu.CompilerParams(vmem_limit_bytes=16 * 2**20),
        cost_estimate=pl.CostEstimate(flops=flops, bytes_accessed=2**20, transcendentals=0),
    )(*args)


def dft_tables(length):
    index = np.arange(length)
    angle = (index[:, None] * index[None, :] % length) * (2.0 * math.pi / length)
    cos, sin = np.cos(angle) / math.sqrt(length), np.sin(angle) / math.sqrt(length)
    right = np.block([[cos, -sin], [sin, cos]])
    tables = []
    for table in (right, right.T):
        high = table.astype(BF16)
        tables += [high, (table - high.astype(np.float64)).astype(BF16)]
    return jnp.asarray(np.stack(tables))


def split(x):
    high = x.astype(BF16)
    return high, (x - high.astype(F32)).astype(BF16)


def dot3(a_high, a_low, b_high, b_low):
    dot = functools.partial(jnp.dot, preferred_element_type=F32)
    return dot(a_high, b_high) + (dot(a_low, b_high) + dot(a_high, b_low))


def lanes(rows, size):
    return lax.broadcasted_iota(jnp.int32, (rows, size), 1)


def turn(x):
    return pltpu.roll(x, x.shape[-1] // 2, 1)


def place(metas, which, slot, size):
    y, x = metas[which, 2 * slot], metas[which, 2 * slot + 1]
    return y, x // size, x % size


def edge_kernel(obj, up, down, edge_l, edge_r):
    _, rows, columns = obj.shape
    half, size = up.shape[1], edge_l.shape[1]
    low = lanes(rows, size) < half
    for ch in range(2):
        down[ch] = obj[ch, :half, :]
        up[ch] = obj[ch, rows - half :, :]
    near, far = slice(0, size), slice(columns - size, columns)
    edge_l[...] = jnp.where(low, obj[0, :, near], turn(obj[1, :, near]))
    edge_r[...] = jnp.where(low, turn(obj[0, :, far]), obj[1, :, far])


def frame_kernel(obj, top, bot, left, right, out):
    tiles, rows, size = out.shape[1:]
    half = size // 2
    low = lanes(half, size) < half
    for at in range(0, rows, half):
        body, src = obj, pl.ds(at - half, half)
        if at == 0:
            body, src = top, pl.ds(0, half)
        elif at == rows - half:
            body, src = bot, pl.ds(0, half)
        here = pl.ds(at, half)
        for ch in range(2):
            parts = [turn(body[ch, src, t * size : (t + 1) * size]) for t in range(tiles - 1)]
            edge_l, edge_r = left[here, :], right[here, :]
            edge_l = edge_l if ch == 0 else turn(edge_l)
            edge_r = turn(edge_r) if ch == 0 else edge_r
            parts = [edge_l, *parts, edge_r]
            for t in range(tiles):
                out[ch, t, here, :] = jnp.where(low, parts[t], parts[t + 1])


def forward_kernel(parts, *refs):
    metas, beams, frame, probe, tables = refs[:5]
    outs, (x_high, x_low, y_high, y_low) = refs[5:-4], refs[-4:]
    size = probe.shape[-1]
    lane = lanes(size, size)
    for at, (which, start, slots) in enumerate(parts):
        far, wave, power = outs[3 * at : 3 * at + 3]
        for index in range(slots):
            slot = start + index
            y, tile, shift = place(metas, which, slot, size)
            beam = beams[which, slot]
            back = lax.rem(size - shift, size)
            patch = []
            for ch in range(2):
                near = pltpu.roll(frame[ch, tile, pl.ds(y, size), :], back, 1)
                rest = pltpu.roll(frame[ch, tile + 1, pl.ds(y, size), :], back, 1)
                patch.append(jnp.where(lane < size - shift, near, rest))
            probe_re, probe_im = probe[beam, 0], probe[beam, 1]
            waves = (
                probe_re * patch[0] - probe_im * patch[1],
                probe_re * patch[1] + probe_im * patch[0],
            )
            rows = slice(index * size, (index + 1) * size)
            for ch in range(2):
                wave[index, ch] = waves[ch]
                columns = slice(ch * size, (ch + 1) * size)
                x_high[rows, columns], x_low[rows, columns] = split(waves[ch])
        for slot in range(0, slots, 2):
            rows = slice(slot * size, (slot + 2) * size)
            mid = dot3(x_high[rows, :], x_low[rows, :], tables[0], tables[1])
            for sub in range(2):
                columns = slice((slot + sub) * size, (slot + sub + 1) * size)
                for ch in range(2):
                    piece = mid[sub * size : (sub + 1) * size, ch * size : (ch + 1) * size]
                    into = slice(ch * size, (ch + 1) * size)
                    y_high[into, columns], y_low[into, columns] = split(piece)
            columns = slice(slot * size, (slot + 2) * size)
            result = dot3(tables[2], tables[3], y_high[:, columns], y_low[:, columns])
            far[:, columns] = result
            for sub in range(2):
                inside = slice(sub * size, (sub + 1) * size)
                re, im = result[:size, inside], result[size:, inside]
                power[slot + sub] = re * re + im * im


def add_patch(total, channel, y, tile, shift, value, lane):
    moved = pltpu.roll(value, shift, 1)
    rows = pl.ds(y, value.shape[0])
    total[channel, tile, rows, :] += jnp.where(lane >= shift, moved, 0.0)
    total[channel, tile + 1, rows, :] += jnp.where(lane < shift, moved, 0.0)


def write_sides(total, side_l, side_r):
    channels, tiles, rows, size = total.shape
    half = size // 2
    low = lanes(rows, size) < half
    if channels == 1:
        side_l[...] = total[0, 0]
        side_r[...] = turn(total[0, tiles - 1])
    else:
        side_l[...] = jnp.where(low, total[0, 0], turn(total[1, 0]))
        side_r[...] = jnp.where(low, turn(total[0, tiles - 1]), total[1, tiles - 1])


def own_columns(total, channel, rows, low):
    tiles = total.shape[1]
    turned = [turn(total[channel, t, rows, :]) for t in range(tiles)]
    return [jnp.where(low, turned[t], turned[t + 1]) for t in range(tiles - 1)]


def write_rims(total, rim_top, rim_bot):
    channels, _, rows, size = total.shape
    half = size // 2
    low = lanes(half, size) < half
    for ch in range(channels):
        for start, out in ((0, rim_top), (rows - half, rim_bot)):
            for t, value in enumerate(own_columns(total, ch, pl.ds(start, half), low)):
                out[ch, :, t * size : (t + 1) * size] = value


def backward_kernel(parts, fresh, last, *refs):
    metas, beams, probe, tables = refs[:4]
    inputs, refs = refs[4 : 4 + 3 * len(parts)], refs[4 + 3 * len(parts) :]
    if not fresh:
        refs = refs[1:]
    total, refs = refs[0], refs[1:]
    if last:
        (side_l, side_r, rim_top, rim_bot), refs = refs[:4], refs[4:]
    x_high, x_low, y_high, y_low = refs
    size = probe.shape[-1]
    scans = beams.shape[1]
    lane = lanes(size, size)
    if fresh:
        total[...] = jnp.zeros_like(total)
    for at, (which, start, slots) in enumerate(parts):
        far, wave, factor = inputs[3 * at : 3 * at + 3]
        for slot in range(0, slots, 2):
            for sub in range(2):
                columns = slice((slot + sub) * size, (slot + sub + 1) * size)
                scale = factor[slot + sub]
                for ch in range(2):
                    into = slice(ch * size, (ch + 1) * size)
                    y_high[into, columns], y_low[into, columns] = split(far[into, columns] * scale)
            columns = slice(slot * size, (slot + 2) * size)
            mid = dot3(tables[0], tables[1], y_high[:, columns], y_low[:, columns])
            for sub in range(2):
                rows = slice((slot + sub) * size, (slot + sub + 1) * size)
                for ch in range(2):
                    piece = mid[ch * size : (ch + 1) * size, sub * size : (sub + 1) * size]
                    into = slice(ch * size, (ch + 1) * size)
                    x_high[rows, into], x_low[rows, into] = split(piece)
            rows = slice(slot * size, (slot + 2) * size)
            result = dot3(x_high[rows, :], x_low[rows, :], tables[2], tables[3])
            for sub in range(2):
                true_slot = start + slot + sub
                live = (true_slot < metas[which, 2 * scans]).astype(F32)
                beam = beams[which, true_slot]
                probe_re, probe_im = probe[beam, 0], probe[beam, 1]
                inside = slice(sub * size, (sub + 1) * size)
                change_re = (result[inside, :size] - wave[slot + sub, 0]) * live
                change_im = (result[inside, size:] - wave[slot + sub, 1]) * live
                grad_re = probe_re * change_re + probe_im * change_im
                grad_im = probe_re * change_im - probe_im * change_re
                spot = place(metas, which, true_slot, size)
                add_patch(total, 0, *spot, grad_re, lane)
                add_patch(total, 1, *spot, grad_im, lane)
    if last:
        write_sides(total, side_l, side_r)
        write_rims(total, rim_top, rim_bot)


def weight_kernel(steps, spans, fresh, *refs):
    metas, (inside, beams, probe) = refs[: len(spans)], refs[len(spans) : len(spans) + 3]
    total = refs[-1]
    _, tiles, rows, size = total.shape
    half, scans = size // 2, beams.shape[1]
    own_rows, own_columns = rows - 2 * size, (tiles - 2) * size
    lane = lanes(size, size)
    if fresh:
        total[...] = jnp.zeros_like(total)
    else:
        total[...] = refs[-2][...]
    for meta, across in zip(metas, spans):
        for row, down, which in steps:

            def add(slot, carry, meta=meta, across=across, row=row, down=down, which=which):
                y = meta[row, 2 * slot] + (down * own_rows + half)
                x = meta[row, 2 * slot + 1] + (across * own_columns + half)
                near = (y > 0) & (y < rows - size) & (x > 0) & (x < (tiles - 1) * size)
                live = (slot < meta[row, 2 * scans]) & (inside[down + 1] > 0)

                @pl.when(near & live)
                def _():
                    beam = beams[which, slot]
                    probe_re, probe_im = probe[beam, 0], probe[beam, 1]
                    value = probe_re * probe_re + probe_im * probe_im
                    add_patch(total, 0, y, x // size, x % size, value, lane)

                return carry

            lax.fori_loop(0, scans, add, 0)


def gathered(total, side_l, side_r, in_top, in_bot, in_ctop, in_cbot, channel, chunk, half):
    _, tiles, rows, size = total.shape
    chunks = (rows - size) // half
    low = lanes(half, size) < half
    ext = pl.ds((chunk + 1) * half, half)
    values = own_columns(total, channel, ext, low)

    def add_sides(from_l, from_r):
        from_l = from_l if channel == 0 else turn(from_l)
        from_r = turn(from_r) if channel == 0 else from_r
        values[0] += jnp.where(low, from_l, 0.0)
        values[-1] += jnp.where(low, 0.0, from_r)

    add_sides(side_l[ext, :], side_r[ext, :])
    for at, rim, corner in ((0, in_top, in_ctop), (chunks - 1, in_bot, in_cbot)):
        if chunk == at:
            for t in range(tiles - 1):
                values[t] += rim[channel, :, t * size : (t + 1) * size]
            add_sides(corner[0], corner[1])
    return values


def final_kernel(*refs):
    obj, weight, out = refs[0], refs[1], refs[-1]
    grads = refs[2:9]
    size = grads[0].shape[-1]
    half = size // 2
    tiles = obj.shape[2] // size
    for chunk in range(obj.shape[1] // half):
        wide = pl.ds(size + chunk * half, half)
        scale = [1.0 / (weight[0, t + 1, wide, :] + DAMPING) for t in range(tiles)]
        rows = slice(chunk * half, (chunk + 1) * half)
        for ch in range(2):
            for t, value in enumerate(gathered(*grads, ch, chunk, half)):
                columns = slice(t * size, (t + 1) * size)
                out[ch, rows, columns] = obj[ch, rows, columns] + value * scale[t]


def line(axis, by):
    count = lax.axis_size(axis)
    return [(i, i + by) for i in range(count) if 0 <= i + by < count]


def ring(axis, by):
    count = lax.axis_size(axis)
    return [(i, (i + by) % count) for i in range(count)]


def send_rims(side_l, side_r, rim_top, rim_bot):
    rows, size = side_l.shape
    half = size // 2
    in_r = lax.ppermute(side_l, "col", line("col", -1))
    in_l = lax.ppermute(side_r, "col", line("col", 1))
    in_bot = lax.ppermute(rim_top, "row", line("row", -1))
    in_top = lax.ppermute(rim_bot, "row", line("row", 1))
    corner_top = jnp.stack([in_l[:half], in_r[:half]])
    corner_bot = jnp.stack([in_l[rows - half :], in_r[rows - half :]])
    in_cbot = lax.ppermute(corner_top, "row", line("row", -1))
    in_ctop = lax.ppermute(corner_bot, "row", line("row", 1))
    return in_l, in_r, in_top, in_bot, in_ctop, in_cbot


def on_device(obj, probe, positions, counts, offsets, measured):
    offsets_count, _, size, _ = probe.shape
    scans = positions.shape[2]
    half = size // 2
    tile_rows, tile_columns = obj.shape[1:]
    rows, tiles = tile_rows + size, tile_columns // size + 1
    row_count = lax.axis_size("row")
    tables = dft_tables(size)

    def packed(x):
        return jnp.concatenate([x[0], x[1]], axis=1)

    up, down, edge_l, edge_r = call(
        edge_kernel, [(2, half, tile_columns)] * 2 + [(tile_rows, size)] * 2, [VMEM], (obj,), 10**6
    )
    top = lax.ppermute(up, "row", line("row", 1))
    bot = lax.ppermute(down, "row", line("row", -1))

    meta = jnp.concatenate([positions.reshape(1, -1), counts.reshape(1, -1)], axis=1)
    kept = min(row_count, offsets_count + 2)
    shifts = [k if k <= offsets_count else k - kept for k in range(kept)]
    metas = [meta] + [lax.ppermute(meta, "row", ring("row", k)) for k in shifts[1:]]
    metas = jnp.concatenate(metas)
    beams = jnp.argmax(offsets[None] == jnp.arange(offsets_count)[:, None, None], axis=2).astype(jnp.int32)
    most = offsets_count - 1

    edge_l, edge_r = (
        jnp.concatenate([packed(top[:, :, part]), edge, packed(bot[:, :, part])])
        for part, edge in ((slice(0, half), edge_l), (slice(tile_columns - half, None), edge_r))
    )
    left = lax.ppermute(edge_r, "col", line("col", 1))
    right = lax.ppermute(edge_l, "col", line("col", -1))
    (frame,) = call(
        frame_kernel, [(2, tiles, rows, size)], [VMEM] * 5, (obj, top, bot, left, right), 10**6
    )

    slots = scans // 2
    halves = ((0, slots), (slots, scans - slots))
    work = [
        pltpu.VMEM((slots * size, 2 * size), BF16),
        pltpu.VMEM((slots * size, 2 * size), BF16),
        pltpu.VMEM((2 * size, slots * size), BF16),
        pltpu.VMEM((2 * size, slots * size), BF16),
    ]
    flops = slots * 2 * 3 * 2 * size * (2 * size) ** 2

    far, wave, power = {}, {}, {}

    def forward(parts):
        outs = []
        for _, _, count in parts:
            outs += [(2 * size, count * size), (count, 2, size, size), (count, size, size)]
        results = call(
            functools.partial(forward_kernel, parts),
            outs,
            [SMEM, SMEM, VMEM, VMEM, VMEM],
            (metas, beams, frame, probe, tables),
            flops * len(parts),
            work,
        )
        for at, (which, start, _) in enumerate(parts):
            far[which, start], wave[which, start], power[which, start] = results[3 * at : 3 * at + 3]

    at_row = lax.axis_index("row")
    inside = jnp.stack([at_row > 0, at_row >= 0, at_row < row_count - 1]).astype(jnp.int32)
    spans = {
        0: metas,
        -1: lax.ppermute(metas, "col", line("col", 1)),
        1: lax.ppermute(metas, "col", line("col", -1)),
    }
    everything = [(which, down) for down in (-1, 0, 1) for which in range(offsets_count)]
    pieces = [(0, everything[::2]), (0, everything[1::2]), (-1, everything), (1, everything)]
    weight = None

    def add_weight(after):
        nonlocal weight
        across, chosen = pieces.pop(0)
        steps = [((which - down) % kept, down, which) for which, down in chosen]
        span, _ = lax.optimization_barrier((spans[across], after))
        (weight,) = call(
            functools.partial(weight_kernel, steps, (across,), weight is None),
            [(1, tiles + 1, tile_rows + 2 * size, size)],
            [SMEM, SMEM, SMEM, VMEM] + ([] if weight is None else [VMEM]),
            (span, inside, beams, probe) + (() if weight is None else (weight,)),
            flops,
            aliases={} if weight is None else {4: 0},
        )

    forward([(most, *halves[0])])
    forward([(most, *halves[1])])
    sums = {start: power[most, start] for start, _ in halves}
    for which in reversed(range(most)):
        for start, _ in halves:
            arrived = lax.ppermute(sums[start], "row", ring("row", -1))
            if which == most - 1 and start == halves[-1][0]:
                forward([(w, *part) for w in reversed(range(most)) for part in halves])
            if which < most - 1 and pieces:
                add_weight(sums[start])
                arrived, weight = lax.optimization_barrier((arrived, weight))
            sums[start] = arrived
        for start, _ in halves:
            sums[start] = sums[start] + power[which, start]
    factors = {
        start: measured[0, 0, start : start + count] / jnp.sqrt(sums[start] + EPSILON) for start, count in halves
    }
    while pieces:
        add_weight(factors[0])

    total = None
    for which in range(offsets_count):
        if which:
            for start, _ in halves:
                value = lax.ppermute(factors[start], "row", ring("row", 1))
                if start == halves[-1][0] and which < most:
                    value, total = lax.optimization_barrier((value, total))
                factors[start] = value
        groups = [[part] for part in halves] if which == most else [list(halves)]
        for group in groups:
            fresh, last = total is None, which == most and group[-1] == halves[-1]
            outs = [(2, tiles, rows, size)]
            if last:
                outs += [(rows, size), (rows, size), (2, half, tile_columns), (2, half, tile_columns)]
            args = [metas, beams, probe, tables]
            for start, _ in group:
                args += [far[which, start], wave[which, start], factors[start]]
            specs = [SMEM, SMEM] + [VMEM] * (len(args) - 2)
            if not fresh:
                args, specs = args + [total], specs + [VMEM]
            total, *sides = call(
                functools.partial(backward_kernel, [(which, *part) for part in group], fresh, last),
                outs,
                specs,
                args,
                flops * len(group),
                work,
                {} if fresh else {len(args) - 1: 0},
            )
    grad_in = send_rims(*sides)

    (new_object,) = call(
        final_kernel, [obj.shape], [VMEM] * 9, (obj, weight, total, *grad_in), 10**6
    )
    return new_object


def solution(mesh):
    return jax.shard_map(
        on_device,
        mesh=mesh,
        in_specs=(
            P(None, "row", "col"),
            P(),
            P("row", "col", None, None),
            P("row", "col"),
            P(),
            P("row", "col", None, None, None),
        ),
        out_specs=P(None, "row", "col"),
        check_vma=False,
    )
```

```python
import functools
import math

import jax
import jax.numpy as jnp
import numpy as np
from jax import lax
from jax.experimental import pallas as pl
from jax.experimental.pallas import tpu as pltpu
from jax.sharding import PartitionSpec as P

EPSILON = 0.5
DAMPING = 0.5


SMEM = pl.BlockSpec(memory_space=pltpu.SMEM)
VMEM = pl.BlockSpec(memory_space=pltpu.VMEM)
F32 = jnp.float32
BF16 = jnp.bfloat16


def call(kernel, outs, specs, args, flops, scratch=(), aliases=None):
    return pl.pallas_call(
        kernel,
        out_shape=[s if hasattr(s, "dtype") else jax.ShapeDtypeStruct(s, F32) for s in outs],
        in_specs=specs,
        out_specs=[VMEM] * len(outs),
        scratch_shapes=list(scratch),
        input_output_aliases=aliases or {},
        compiler_params=pltpu.CompilerParams(vmem_limit_bytes=16 * 2**20),
        cost_estimate=pl.CostEstimate(flops=flops, bytes_accessed=2**20, transcendentals=0),
    )(*args)


def dft_tables(length):
    index = np.arange(length)
    angle = (index[:, None] * index[None, :] % length) * (2.0 * math.pi / length)
    cos, sin = np.cos(angle) / math.sqrt(length), np.sin(angle) / math.sqrt(length)
    right = np.block([[cos, -sin], [sin, cos]])
    tables = []
    for table in (right, right.T):
        high = table.astype(BF16)
        tables += [high, (table - high.astype(np.float64)).astype(BF16)]
    return jnp.asarray(np.stack(tables))


def split(x):
    high = x.astype(BF16)
    return high, (x - high.astype(F32)).astype(BF16)


def dot3(a_high, a_low, b_high, b_low):
    dot = functools.partial(jnp.dot, preferred_element_type=F32)
    return dot(a_high, b_high) + (dot(a_low, b_high) + dot(a_high, b_low))


def lanes(rows, size):
    return lax.broadcasted_iota(jnp.int32, (rows, size), 1)


def turn(x):
    return pltpu.roll(x, x.shape[-1] // 2, 1)


def beam_of(offsets, which, slot):
    beam = jnp.int32(0)
    for index in range(1, offsets.shape[1]):
        beam = jnp.where(offsets[slot, index] == which, index, beam)
    return beam


def place(metas, which, slot, size):
    y, x = metas[which, 2 * slot], metas[which, 2 * slot + 1]
    return y, x // size, x % size


def edge_kernel(obj, positions, counts, place_of, up, down, edge_l, edge_r, meta):
    scans = positions.shape[2]
    values = [positions[0, 0, slot, axis] for slot in range(scans) for axis in range(2)]
    values += [counts[0, 0], place_of[0]]
    lane = lax.broadcasted_iota(jnp.int32, meta.shape, 1)
    row = jnp.zeros(meta.shape, jnp.int32)
    for at, value in enumerate(values):
        row = jnp.where(lane == at, value, row)
    meta[...] = row
    _, rows, columns = obj.shape
    half, size = up.shape[1], edge_l.shape[1]
    low = lanes(rows, size) < half
    for ch in range(2):
        down[ch] = obj[ch, :half, :]
        up[ch] = obj[ch, rows - half :, :]
    near, far = slice(0, size), slice(columns - size, columns)
    edge_l[...] = jnp.where(low, obj[0, :, near], turn(obj[1, :, near]))
    edge_r[...] = jnp.where(low, turn(obj[0, :, far]), obj[1, :, far])


def frame_kernel(obj, top, bot, left, right, out):
    tiles, rows, size = out.shape[1:]
    half = size // 2
    low = lanes(half, size) < half
    for at in range(0, rows, half):
        body, src = obj, pl.ds(at - half, half)
        if at == 0:
            body, src = top, pl.ds(0, half)
        elif at == rows - half:
            body, src = bot, pl.ds(0, half)
        here = pl.ds(at, half)
        for ch in range(2):
            parts = [turn(body[ch, src, t * size : (t + 1) * size]) for t in range(tiles - 1)]
            edge_l, edge_r = left[here, :], right[here, :]
            edge_l = edge_l if ch == 0 else turn(edge_l)
            edge_r = turn(edge_r) if ch == 0 else edge_r
            parts = [edge_l, *parts, edge_r]
            for t in range(tiles):
                out[ch, t, here, :] = jnp.where(low, parts[t], parts[t + 1])


def forward_kernel(parts, *refs):
    metas, offsets, frame, probe, tables = refs[:5]
    outs, (x_high, x_low, y_high, y_low) = refs[5:-4], refs[-4:]
    size = probe.shape[-1]
    lane = lanes(size, size)
    for at, (which, start, slots) in enumerate(parts):
        far, wave, power = outs[3 * at : 3 * at + 3]
        for index in range(slots):
            slot = start + index
            y, tile, shift = place(metas, which, slot, size)
            beam = beam_of(offsets, which, slot)
            back = lax.rem(size - shift, size)
            patch = []
            for ch in range(2):
                near = pltpu.roll(frame[ch, tile, pl.ds(y, size), :], back, 1)
                rest = pltpu.roll(frame[ch, tile + 1, pl.ds(y, size), :], back, 1)
                patch.append(jnp.where(lane < size - shift, near, rest))
            probe_re, probe_im = probe[beam, 0], probe[beam, 1]
            waves = (
                probe_re * patch[0] - probe_im * patch[1],
                probe_re * patch[1] + probe_im * patch[0],
            )
            rows = slice(index * size, (index + 1) * size)
            for ch in range(2):
                wave[index, ch] = waves[ch]
                columns = slice(ch * size, (ch + 1) * size)
                x_high[rows, columns], x_low[rows, columns] = split(waves[ch])
        for slot in range(0, slots, 2):
            rows = slice(slot * size, (slot + 2) * size)
            mid = dot3(x_high[rows, :], x_low[rows, :], tables[0], tables[1])
            for sub in range(2):
                columns = slice((slot + sub) * size, (slot + sub + 1) * size)
                for ch in range(2):
                    piece = mid[sub * size : (sub + 1) * size, ch * size : (ch + 1) * size]
                    into = slice(ch * size, (ch + 1) * size)
                    y_high[into, columns], y_low[into, columns] = split(piece)
            columns = slice(slot * size, (slot + 2) * size)
            result = dot3(tables[2], tables[3], y_high[:, columns], y_low[:, columns])
            far[:, columns] = result
            for sub in range(2):
                inside = slice(sub * size, (sub + 1) * size)
                re, im = result[:size, inside], result[size:, inside]
                power[slot + sub] = re * re + im * im


def add_patch(total, channel, y, tile, shift, value, lane):
    moved = pltpu.roll(value, shift, 1)
    rows = pl.ds(y, value.shape[0])
    total[channel, tile, rows, :] += jnp.where(lane >= shift, moved, 0.0)
    total[channel, tile + 1, rows, :] += jnp.where(lane < shift, moved, 0.0)


def write_sides(total, side_l, side_r):
    channels, tiles, rows, size = total.shape
    half = size // 2
    low = lanes(rows, size) < half
    if channels == 1:
        side_l[...] = total[0, 0]
        side_r[...] = turn(total[0, tiles - 1])
    else:
        side_l[...] = jnp.where(low, total[0, 0], turn(total[1, 0]))
        side_r[...] = jnp.where(low, turn(total[0, tiles - 1]), total[1, tiles - 1])


def own_columns(total, channel, rows, low):
    tiles = total.shape[1]
    turned = [turn(total[channel, t, rows, :]) for t in range(tiles)]
    return [jnp.where(low, turned[t], turned[t + 1]) for t in range(tiles - 1)]


def write_rims(total, rim_top, rim_bot):
    channels, _, rows, size = total.shape
    half = size // 2
    low = lanes(half, size) < half
    for ch in range(channels):
        for start, out in ((0, rim_top), (rows - half, rim_bot)):
            for t, value in enumerate(own_columns(total, ch, pl.ds(start, half), low)):
                out[ch, :, t * size : (t + 1) * size] = value


def backward_kernel(parts, fresh, last, *refs):
    metas, offsets, probe, tables = refs[:4]
    inputs, refs = refs[4 : 4 + 3 * len(parts)], refs[4 + 3 * len(parts) :]
    if not fresh:
        refs = refs[1:]
    total, refs = refs[0], refs[1:]
    if last:
        (side_l, side_r, rim_top, rim_bot), refs = refs[:4], refs[4:]
    x_high, x_low, y_high, y_low = refs
    size = probe.shape[-1]
    scans = offsets.shape[0]
    lane = lanes(size, size)
    if fresh:
        total[...] = jnp.zeros_like(total)
    for at, (which, start, slots) in enumerate(parts):
        far, wave, factor = inputs[3 * at : 3 * at + 3]
        for slot in range(0, slots, 2):
            for sub in range(2):
                columns = slice((slot + sub) * size, (slot + sub + 1) * size)
                scale = factor[slot + sub]
                for ch in range(2):
                    into = slice(ch * size, (ch + 1) * size)
                    y_high[into, columns], y_low[into, columns] = split(far[into, columns] * scale)
            columns = slice(slot * size, (slot + 2) * size)
            mid = dot3(tables[0], tables[1], y_high[:, columns], y_low[:, columns])
            for sub in range(2):
                rows = slice((slot + sub) * size, (slot + sub + 1) * size)
                for ch in range(2):
                    piece = mid[ch * size : (ch + 1) * size, sub * size : (sub + 1) * size]
                    into = slice(ch * size, (ch + 1) * size)
                    x_high[rows, into], x_low[rows, into] = split(piece)
            rows = slice(slot * size, (slot + 2) * size)
            result = dot3(x_high[rows, :], x_low[rows, :], tables[2], tables[3])
            for sub in range(2):
                true_slot = start + slot + sub
                live = (true_slot < metas[which, 2 * scans]).astype(F32)
                beam = beam_of(offsets, which, true_slot)
                probe_re, probe_im = probe[beam, 0], probe[beam, 1]
                inside = slice(sub * size, (sub + 1) * size)
                change_re = (result[inside, :size] - wave[slot + sub, 0]) * live
                change_im = (result[inside, size:] - wave[slot + sub, 1]) * live
                grad_re = probe_re * change_re + probe_im * change_im
                grad_im = probe_re * change_im - probe_im * change_re
                spot = place(metas, which, true_slot, size)
                add_patch(total, 0, *spot, grad_re, lane)
                add_patch(total, 1, *spot, grad_im, lane)
    if last:
        write_sides(total, side_l, side_r)
        write_rims(total, rim_top, rim_bot)


def weight_kernel(steps, spans, row_count, fresh, *refs):
    metas, (offsets, probe) = refs[: len(spans)], refs[len(spans) : len(spans) + 2]
    total = refs[-1]
    _, tiles, rows, size = total.shape
    half, scans = size // 2, offsets.shape[0]
    own_rows, own_columns = rows - 2 * size, (tiles - 2) * size
    lane = lanes(size, size)
    if fresh:
        total[...] = jnp.zeros_like(total)
    else:
        total[...] = refs[-2][...]
    for meta, across in zip(metas, spans):
        for row, down, which in steps:

            def add(slot, carry, meta=meta, across=across, row=row, down=down, which=which):
                y = meta[row, 2 * slot] + (down * own_rows + half)
                x = meta[row, 2 * slot + 1] + (across * own_columns + half)
                near = (y > 0) & (y < rows - size) & (x > 0) & (x < (tiles - 1) * size)
                below = meta[0, 2 * scans + 1] + down
                live = (slot < meta[row, 2 * scans]) & (below >= 0) & (below < row_count)

                @pl.when(near & live)
                def _():
                    beam = beam_of(offsets, which, slot)
                    probe_re, probe_im = probe[beam, 0], probe[beam, 1]
                    value = probe_re * probe_re + probe_im * probe_im
                    add_patch(total, 0, y, x // size, x % size, value, lane)

                return carry

            lax.fori_loop(0, scans, add, 0)


def gathered(total, side_l, side_r, in_top, in_bot, in_ctop, in_cbot, channel, chunk, half):
    _, tiles, rows, size = total.shape
    chunks = (rows - size) // half
    low = lanes(half, size) < half
    ext = pl.ds((chunk + 1) * half, half)
    values = own_columns(total, channel, ext, low)

    def add_sides(from_l, from_r):
        from_l = from_l if channel == 0 else turn(from_l)
        from_r = turn(from_r) if channel == 0 else from_r
        values[0] += jnp.where(low, from_l, 0.0)
        values[-1] += jnp.where(low, 0.0, from_r)

    add_sides(side_l[ext, :], side_r[ext, :])
    for at, rim, corner in ((0, in_top, in_ctop), (chunks - 1, in_bot, in_cbot)):
        if chunk == at:
            for t in range(tiles - 1):
                values[t] += rim[channel, :, t * size : (t + 1) * size]
            add_sides(corner[0], corner[1])
    return values


def final_kernel(*refs):
    obj, weight, out = refs[0], refs[1], refs[-1]
    grads = refs[2:9]
    size = grads[0].shape[-1]
    half = size // 2
    tiles = obj.shape[2] // size
    for chunk in range(obj.shape[1] // half):
        wide = pl.ds(size + chunk * half, half)
        scale = [1.0 / (weight[0, t + 1, wide, :] + DAMPING) for t in range(tiles)]
        rows = slice(chunk * half, (chunk + 1) * half)
        for ch in range(2):
            for t, value in enumerate(gathered(*grads, ch, chunk, half)):
                columns = slice(t * size, (t + 1) * size)
                out[ch, rows, columns] = obj[ch, rows, columns] + value * scale[t]


def line(axis, by):
    count = lax.axis_size(axis)
    return [(i, i + by) for i in range(count) if 0 <= i + by < count]


def ring(axis, by):
    count = lax.axis_size(axis)
    return [(i, (i + by) % count) for i in range(count)]


def send_rims(side_l, side_r, rim_top, rim_bot):
    rows, size = side_l.shape
    half = size // 2
    in_r = lax.ppermute(side_l, "col", line("col", -1))
    in_l = lax.ppermute(side_r, "col", line("col", 1))
    in_bot = lax.ppermute(rim_top, "row", line("row", -1))
    in_top = lax.ppermute(rim_bot, "row", line("row", 1))
    corner_top = jnp.stack([in_l[:half], in_r[:half]])
    corner_bot = jnp.stack([in_l[rows - half :], in_r[rows - half :]])
    in_cbot = lax.ppermute(corner_top, "row", line("row", -1))
    in_ctop = lax.ppermute(corner_bot, "row", line("row", 1))
    return in_l, in_r, in_top, in_bot, in_ctop, in_cbot


def on_device(obj, probe, positions, counts, offsets, measured):
    offsets_count, _, size, _ = probe.shape
    scans = positions.shape[2]
    half = size // 2
    tile_rows, tile_columns = obj.shape[1:]
    rows, tiles = tile_rows + size, tile_columns // size + 1
    row_count = lax.axis_size("row")
    tables = dft_tables(size)

    def packed(x):
        return jnp.concatenate([x[0], x[1]], axis=1)

    up, down, edge_l, edge_r, meta = call(
        edge_kernel,
        [(2, half, tile_columns)] * 2 + [(tile_rows, size)] * 2 + [jax.ShapeDtypeStruct((1, size), jnp.int32)],
        [VMEM, SMEM, SMEM, SMEM],
        (obj, positions, counts, lax.axis_index("row").astype(jnp.int32).reshape(1)),
        10**6,
    )
    top = lax.ppermute(up, "row", line("row", 1))
    bot = lax.ppermute(down, "row", line("row", -1))

    kept = min(row_count, offsets_count + 2)
    shifts = [k if k <= offsets_count else k - kept for k in range(kept)]
    metas = [meta] + [lax.ppermute(meta, "row", ring("row", k)) for k in shifts[1:]]
    metas = jnp.concatenate(metas)
    most = offsets_count - 1

    edge_l, edge_r = (
        jnp.concatenate([packed(top[:, :, part]), edge, packed(bot[:, :, part])])
        for part, edge in ((slice(0, half), edge_l), (slice(tile_columns - half, None), edge_r))
    )
    left = lax.ppermute(edge_r, "col", line("col", 1))
    right = lax.ppermute(edge_l, "col", line("col", -1))
    (frame,) = call(
        frame_kernel, [(2, tiles, rows, size)], [VMEM] * 5, (obj, top, bot, left, right), 10**6
    )

    slots = scans // 2
    halves = ((0, slots), (slots, scans - slots))
    work = [
        pltpu.VMEM((slots * size, 2 * size), BF16),
        pltpu.VMEM((slots * size, 2 * size), BF16),
        pltpu.VMEM((2 * size, slots * size), BF16),
        pltpu.VMEM((2 * size, slots * size), BF16),
    ]
    flops = slots * 2 * 3 * 2 * size * (2 * size) ** 2

    far, wave, power = {}, {}, {}

    def forward(parts):
        outs = []
        for _, _, count in parts:
            outs += [(2 * size, count * size), (count, 2, size, size), (count, size, size)]
        results = call(
            functools.partial(forward_kernel, parts),
            outs,
            [SMEM, SMEM, VMEM, VMEM, VMEM],
            (metas, offsets, frame, probe, tables),
            flops * len(parts),
            work,
        )
        for at, (which, start, _) in enumerate(parts):
            far[which, start], wave[which, start], power[which, start] = results[3 * at : 3 * at + 3]

    spans = {
        0: metas,
        -1: lax.ppermute(metas, "col", line("col", 1)),
        1: lax.ppermute(metas, "col", line("col", -1)),
    }
    everything = [(which, down) for down in (-1, 0, 1) for which in range(offsets_count)]
    pieces = [(0, everything[::2]), (0, everything[1::2]), (-1, everything), (1, everything)]
    weight = None

    def add_weight(after):
        nonlocal weight
        across, chosen = pieces.pop(0)
        steps = [((which - down) % kept, down, which) for which, down in chosen]
        span, _ = lax.optimization_barrier((spans[across], after))
        (weight,) = call(
            functools.partial(weight_kernel, steps, (across,), row_count, weight is None),
            [(1, tiles + 1, tile_rows + 2 * size, size)],
            [SMEM, SMEM, VMEM] + ([] if weight is None else [VMEM]),
            (span, offsets, probe) + (() if weight is None else (weight,)),
            flops,
            aliases={} if weight is None else {3: 0},
        )

    forward([(most, *halves[0])])
    forward([(most, *halves[1])])
    sums = {start: power[most, start] for start, _ in halves}
    for which in reversed(range(most)):
        for start, _ in halves:
            arrived = lax.ppermute(sums[start], "row", ring("row", -1))
            if which == most - 1 and start == halves[-1][0]:
                forward([(w, *part) for w in reversed(range(most)) for part in halves])
            if which < most - 1 and pieces:
                add_weight(sums[start])
                arrived, weight = lax.optimization_barrier((arrived, weight))
            sums[start] = arrived
        for start, _ in halves:
            sums[start] = sums[start] + power[which, start]
    factors = {
        start: measured[0, 0, start : start + count] / jnp.sqrt(sums[start] + EPSILON) for start, count in halves
    }
    while pieces:
        add_weight(factors[0])

    total = None
    for which in range(offsets_count):
        if which:
            for start, _ in halves:
                value = lax.ppermute(factors[start], "row", ring("row", 1))
                if start == halves[-1][0] and which < most:
                    value, total = lax.optimization_barrier((value, total))
                factors[start] = value
        groups = [[part] for part in halves] if which == most else [list(halves)]
        for group in groups:
            fresh, last = total is None, which == most and group[-1] == halves[-1]
            outs = [(2, tiles, rows, size)]
            if last:
                outs += [(rows, size), (rows, size), (2, half, tile_columns), (2, half, tile_columns)]
            args = [metas, offsets, probe, tables]
            for start, _ in group:
                args += [far[which, start], wave[which, start], factors[start]]
            specs = [SMEM, SMEM] + [VMEM] * (len(args) - 2)
            if not fresh:
                args, specs = args + [total], specs + [VMEM]
            total, *sides = call(
                functools.partial(backward_kernel, [(which, *part) for part in group], fresh, last),
                outs,
                specs,
                args,
                flops * len(group),
                work,
                {} if fresh else {len(args) - 1: 0},
            )
    grad_in = send_rims(*sides)

    (new_object,) = call(
        final_kernel, [obj.shape], [VMEM] * 9, (obj, weight, total, *grad_in), 10**6
    )
    return new_object


def solution(mesh):
    return jax.shard_map(
        on_device,
        mesh=mesh,
        in_specs=(
            P(None, "row", "col"),
            P(),
            P("row", "col", None, None),
            P("row", "col"),
            P(),
            P("row", "col", None, None, None),
        ),
        out_specs=P(None, "row", "col"),
        check_vma=False,
    )
```

```python
import functools
import math

import jax
import jax.numpy as jnp
import numpy as np
from jax import lax
from jax.experimental import pallas as pl
from jax.experimental.pallas import tpu as pltpu
from jax.sharding import PartitionSpec as P

EPSILON = 0.5
DAMPING = 0.5


SMEM = pl.BlockSpec(memory_space=pltpu.SMEM)
VMEM = pl.BlockSpec(memory_space=pltpu.VMEM)
F32 = jnp.float32
BF16 = jnp.bfloat16


def call(kernel, outs, specs, args, flops, scratch=(), aliases=None):
    return pl.pallas_call(
        kernel,
        out_shape=[s if hasattr(s, "dtype") else jax.ShapeDtypeStruct(s, F32) for s in outs],
        in_specs=specs,
        out_specs=[VMEM] * len(outs),
        scratch_shapes=list(scratch),
        input_output_aliases=aliases or {},
        compiler_params=pltpu.CompilerParams(vmem_limit_bytes=16 * 2**20),
        cost_estimate=pl.CostEstimate(flops=flops, bytes_accessed=2**20, transcendentals=0),
    )(*args)


def dft_tables(length):
    index = np.arange(length)
    angle = (index[:, None] * index[None, :] % length) * (2.0 * math.pi / length)
    cos, sin = np.cos(angle) / math.sqrt(length), np.sin(angle) / math.sqrt(length)
    right = np.block([[cos, -sin], [sin, cos]])
    tables = []
    for table in (right, right.T):
        high = table.astype(BF16)
        tables += [high, (table - high.astype(np.float64)).astype(BF16)]
    return jnp.asarray(np.stack(tables))


def split(x):
    high = x.astype(BF16)
    return high, (x - high.astype(F32)).astype(BF16)


def dot3(a_high, a_low, b_high, b_low):
    dot = functools.partial(jnp.dot, preferred_element_type=F32)
    return dot(a_high, b_high) + (dot(a_low, b_high) + dot(a_high, b_low))


def lanes(rows, size):
    return lax.broadcasted_iota(jnp.int32, (rows, size), 1)


def turn(x):
    return pltpu.roll(x, x.shape[-1] // 2, 1)


def beam_of(offsets, which, slot):
    beam = jnp.int32(0)
    for index in range(1, offsets.shape[1]):
        beam = jnp.where(offsets[slot, index] == which, index, beam)
    return beam


def place(metas, which, slot, size):
    y, x = metas[which, 2 * slot], metas[which, 2 * slot + 1]
    return y, x // size, x % size


def edge_kernel(obj, positions, counts, place_of, edge_l, edge_r, meta):
    scans = positions.shape[2]
    values = [positions[0, 0, slot, axis] for slot in range(scans) for axis in range(2)]
    values += [counts[0, 0], place_of[0]]
    lane = lax.broadcasted_iota(jnp.int32, meta.shape, 1)
    row = jnp.zeros(meta.shape, jnp.int32)
    for at, value in enumerate(values):
        row = jnp.where(lane == at, value, row)
    meta[...] = row
    _, rows, columns = obj.shape
    size = edge_l.shape[1]
    low = lanes(rows, size) < size // 2
    near, far = slice(0, size), slice(columns - size, columns)
    edge_l[...] = jnp.where(low, obj[0, :, near], turn(obj[1, :, near]))
    edge_r[...] = jnp.where(low, turn(obj[0, :, far]), obj[1, :, far])


def frame_kernel(obj, top, bot, left, right, out):
    tiles, rows, size = out.shape[1:]
    half = size // 2
    low = lanes(half, size) < half
    for at in range(0, rows, half):
        body, src = obj, pl.ds(at - half, half)
        if at == 0:
            body, src = top, pl.ds(0, half)
        elif at == rows - half:
            body, src = bot, pl.ds(0, half)
        here = pl.ds(at, half)
        for ch in range(2):
            parts = [turn(body[ch, src, t * size : (t + 1) * size]) for t in range(tiles - 1)]
            edge_l, edge_r = left[here, :], right[here, :]
            edge_l = edge_l if ch == 0 else turn(edge_l)
            edge_r = turn(edge_r) if ch == 0 else edge_r
            parts = [edge_l, *parts, edge_r]
            for t in range(tiles):
                out[ch, t, here, :] = jnp.where(low, parts[t], parts[t + 1])


def forward_kernel(parts, *refs):
    metas, offsets, frame, probe, tables = refs[:5]
    outs, (x_high, x_low, y_high, y_low) = refs[5:-4], refs[-4:]
    size = probe.shape[-1]
    lane = lanes(size, size)
    for at, (which, start, slots) in enumerate(parts):
        far, wave, power = outs[3 * at : 3 * at + 3]
        for index in range(slots):
            slot = start + index
            y, tile, shift = place(metas, which, slot, size)
            beam = beam_of(offsets, which, slot)
            back = lax.rem(size - shift, size)
            patch = []
            for ch in range(2):
                near = pltpu.roll(frame[ch, tile, pl.ds(y, size), :], back, 1)
                rest = pltpu.roll(frame[ch, tile + 1, pl.ds(y, size), :], back, 1)
                patch.append(jnp.where(lane < size - shift, near, rest))
            probe_re, probe_im = probe[beam, 0], probe[beam, 1]
            waves = (
                probe_re * patch[0] - probe_im * patch[1],
                probe_re * patch[1] + probe_im * patch[0],
            )
            rows = slice(index * size, (index + 1) * size)
            for ch in range(2):
                wave[index, ch] = waves[ch]
                columns = slice(ch * size, (ch + 1) * size)
                x_high[rows, columns], x_low[rows, columns] = split(waves[ch])
        for slot in range(0, slots, 2):
            rows = slice(slot * size, (slot + 2) * size)
            mid = dot3(x_high[rows, :], x_low[rows, :], tables[0], tables[1])
            for sub in range(2):
                columns = slice((slot + sub) * size, (slot + sub + 1) * size)
                for ch in range(2):
                    piece = mid[sub * size : (sub + 1) * size, ch * size : (ch + 1) * size]
                    into = slice(ch * size, (ch + 1) * size)
                    y_high[into, columns], y_low[into, columns] = split(piece)
            columns = slice(slot * size, (slot + 2) * size)
            result = dot3(tables[2], tables[3], y_high[:, columns], y_low[:, columns])
            far[:, columns] = result
            for sub in range(2):
                inside = slice(sub * size, (sub + 1) * size)
                re, im = result[:size, inside], result[size:, inside]
                power[slot + sub] = re * re + im * im


def add_patch(total, channel, y, tile, shift, value, lane):
    moved = pltpu.roll(value, shift, 1)
    rows = pl.ds(y, value.shape[0])
    total[channel, tile, rows, :] += jnp.where(lane >= shift, moved, 0.0)
    total[channel, tile + 1, rows, :] += jnp.where(lane < shift, moved, 0.0)


def write_sides(total, side_l, side_r):
    channels, tiles, rows, size = total.shape
    half = size // 2
    low = lanes(rows, size) < half
    if channels == 1:
        side_l[...] = total[0, 0]
        side_r[...] = turn(total[0, tiles - 1])
    else:
        side_l[...] = jnp.where(low, total[0, 0], turn(total[1, 0]))
        side_r[...] = jnp.where(low, turn(total[0, tiles - 1]), total[1, tiles - 1])


def own_columns(total, channel, rows, low):
    tiles = total.shape[1]
    turned = [turn(total[channel, t, rows, :]) for t in range(tiles)]
    return [jnp.where(low, turned[t], turned[t + 1]) for t in range(tiles - 1)]


def write_rims(total, rim_top, rim_bot):
    channels, _, rows, size = total.shape
    half = size // 2
    low = lanes(half, size) < half
    for ch in range(channels):
        for start, out in ((0, rim_top), (rows - half, rim_bot)):
            for t, value in enumerate(own_columns(total, ch, pl.ds(start, half), low)):
                out[ch, :, t * size : (t + 1) * size] = value


def backward_kernel(parts, fresh, last, *refs):
    metas, offsets, probe, tables = refs[:4]
    inputs, refs = refs[4 : 4 + 3 * len(parts)], refs[4 + 3 * len(parts) :]
    if not fresh:
        refs = refs[1:]
    total, refs = refs[0], refs[1:]
    if last:
        (side_l, side_r, rim_top, rim_bot), refs = refs[:4], refs[4:]
    x_high, x_low, y_high, y_low = refs
    size = probe.shape[-1]
    scans = offsets.shape[0]
    lane = lanes(size, size)
    if fresh:
        total[...] = jnp.zeros_like(total)
    for at, (which, start, slots) in enumerate(parts):
        far, wave, factor = inputs[3 * at : 3 * at + 3]
        for slot in range(0, slots, 2):
            for sub in range(2):
                columns = slice((slot + sub) * size, (slot + sub + 1) * size)
                scale = factor[slot + sub]
                for ch in range(2):
                    into = slice(ch * size, (ch + 1) * size)
                    y_high[into, columns], y_low[into, columns] = split(far[into, columns] * scale)
            columns = slice(slot * size, (slot + 2) * size)
            mid = dot3(tables[0], tables[1], y_high[:, columns], y_low[:, columns])
            for sub in range(2):
                rows = slice((slot + sub) * size, (slot + sub + 1) * size)
                for ch in range(2):
                    piece = mid[ch * size : (ch + 1) * size, sub * size : (sub + 1) * size]
                    into = slice(ch * size, (ch + 1) * size)
                    x_high[rows, into], x_low[rows, into] = split(piece)
            rows = slice(slot * size, (slot + 2) * size)
            result = dot3(x_high[rows, :], x_low[rows, :], tables[2], tables[3])
            for sub in range(2):
                true_slot = start + slot + sub
                live = (true_slot < metas[which, 2 * scans]).astype(F32)
                beam = beam_of(offsets, which, true_slot)
                probe_re, probe_im = probe[beam, 0], probe[beam, 1]
                inside = slice(sub * size, (sub + 1) * size)
                change_re = (result[inside, :size] - wave[slot + sub, 0]) * live
                change_im = (result[inside, size:] - wave[slot + sub, 1]) * live
                grad_re = probe_re * change_re + probe_im * change_im
                grad_im = probe_re * change_im - probe_im * change_re
                spot = place(metas, which, true_slot, size)
                add_patch(total, 0, *spot, grad_re, lane)
                add_patch(total, 1, *spot, grad_im, lane)
    if last:
        write_sides(total, side_l, side_r)
        write_rims(total, rim_top, rim_bot)


def weight_kernel(steps, spans, row_count, fresh, *refs):
    metas, (offsets, probe) = refs[: len(spans)], refs[len(spans) : len(spans) + 2]
    total = refs[-1]
    _, tiles, rows, size = total.shape
    half, scans = size // 2, offsets.shape[0]
    own_rows, own_columns = rows - 2 * size, (tiles - 2) * size
    lane = lanes(size, size)
    if fresh:
        total[...] = jnp.zeros_like(total)
    else:
        total[...] = refs[-2][...]
    for meta, across in zip(metas, spans):
        for row, down, which in steps:

            def add(slot, carry, meta=meta, across=across, row=row, down=down, which=which):
                y = meta[row, 2 * slot] + (down * own_rows + half)
                x = meta[row, 2 * slot + 1] + (across * own_columns + half)
                near = (y > 0) & (y < rows - size) & (x > 0) & (x < (tiles - 1) * size)
                below = meta[0, 2 * scans + 1] + down
                live = (slot < meta[row, 2 * scans]) & (below >= 0) & (below < row_count)

                @pl.when(near & live)
                def _():
                    beam = beam_of(offsets, which, slot)
                    probe_re, probe_im = probe[beam, 0], probe[beam, 1]
                    value = probe_re * probe_re + probe_im * probe_im
                    add_patch(total, 0, y, x // size, x % size, value, lane)

                return carry

            lax.fori_loop(0, scans, add, 0)


def gathered(total, side_l, side_r, in_top, in_bot, in_ctop, in_cbot, channel, chunk, half):
    _, tiles, rows, size = total.shape
    chunks = (rows - size) // half
    low = lanes(half, size) < half
    ext = pl.ds((chunk + 1) * half, half)
    values = own_columns(total, channel, ext, low)

    def add_sides(from_l, from_r):
        from_l = from_l if channel == 0 else turn(from_l)
        from_r = turn(from_r) if channel == 0 else from_r
        values[0] += jnp.where(low, from_l, 0.0)
        values[-1] += jnp.where(low, 0.0, from_r)

    add_sides(side_l[ext, :], side_r[ext, :])
    for at, rim, corner in ((0, in_top, in_ctop), (chunks - 1, in_bot, in_cbot)):
        if chunk == at:
            for t in range(tiles - 1):
                values[t] += rim[channel, :, t * size : (t + 1) * size]
            add_sides(corner[0], corner[1])
    return values


def final_kernel(*refs):
    obj, weight, out = refs[0], refs[1], refs[-1]
    grads = refs[2:9]
    size = grads[0].shape[-1]
    half = size // 2
    tiles = obj.shape[2] // size
    for chunk in range(obj.shape[1] // half):
        wide = pl.ds(size + chunk * half, half)
        scale = [1.0 / (weight[0, t + 1, wide, :] + DAMPING) for t in range(tiles)]
        rows = slice(chunk * half, (chunk + 1) * half)
        for ch in range(2):
            for t, value in enumerate(gathered(*grads, ch, chunk, half)):
                columns = slice(t * size, (t + 1) * size)
                out[ch, rows, columns] = obj[ch, rows, columns] + value * scale[t]


def line(axis, by):
    count = lax.axis_size(axis)
    return [(i, i + by) for i in range(count) if 0 <= i + by < count]


def ring(axis, by):
    count = lax.axis_size(axis)
    return [(i, (i + by) % count) for i in range(count)]


def send_rims(side_l, side_r, rim_top, rim_bot):
    rows, size = side_l.shape
    half = size // 2
    in_r = lax.ppermute(side_l, "col", line("col", -1))
    in_l = lax.ppermute(side_r, "col", line("col", 1))
    in_bot = lax.ppermute(rim_top, "row", line("row", -1))
    in_top = lax.ppermute(rim_bot, "row", line("row", 1))
    corner_top = jnp.stack([in_l[:half], in_r[:half]])
    corner_bot = jnp.stack([in_l[rows - half :], in_r[rows - half :]])
    in_cbot = lax.ppermute(corner_top, "row", line("row", -1))
    in_ctop = lax.ppermute(corner_bot, "row", line("row", 1))
    return in_l, in_r, in_top, in_bot, in_ctop, in_cbot


def on_device(obj, probe, positions, counts, offsets, measured):
    offsets_count, _, size, _ = probe.shape
    scans = positions.shape[2]
    half = size // 2
    tile_rows, tile_columns = obj.shape[1:]
    rows, tiles = tile_rows + size, tile_columns // size + 1
    row_count = lax.axis_size("row")
    tables = dft_tables(size)

    def packed(x):
        return jnp.concatenate([x[0], x[1]], axis=1)

    edge_l, edge_r, meta = call(
        edge_kernel,
        [(tile_rows, size)] * 2 + [jax.ShapeDtypeStruct((1, size), jnp.int32)],
        [VMEM, SMEM, SMEM, SMEM],
        (obj, positions, counts, lax.axis_index("row").astype(jnp.int32).reshape(1)),
        10**6,
    )
    top = lax.ppermute(obj[:, tile_rows - half :], "row", line("row", 1))
    bot = lax.ppermute(obj[:, :half], "row", line("row", -1))

    kept = min(row_count, offsets_count + 2)
    shifts = [k if k <= offsets_count else k - kept for k in range(kept)]
    metas = [meta] + [lax.ppermute(meta, "row", ring("row", k)) for k in shifts[1:]]
    metas = jnp.concatenate(metas)
    most = offsets_count - 1

    extra = metas.astype(F32)
    edge_l, edge_r = (
        jnp.concatenate([packed(top[:, :, part]), edge, packed(bot[:, :, part]), extra])
        for part, edge in ((slice(0, half), edge_l), (slice(tile_columns - half, None), edge_r))
    )
    left = lax.ppermute(edge_r, "col", line("col", 1))
    right = lax.ppermute(edge_l, "col", line("col", -1))
    (frame,) = call(
        frame_kernel, [(2, tiles, rows, size)], [VMEM] * 5, (obj, top, bot, left, right), 10**6
    )

    slots = scans // 2
    halves = ((0, slots), (slots, scans - slots))
    work = [
        pltpu.VMEM((slots * size, 2 * size), BF16),
        pltpu.VMEM((slots * size, 2 * size), BF16),
        pltpu.VMEM((2 * size, slots * size), BF16),
        pltpu.VMEM((2 * size, slots * size), BF16),
    ]
    flops = slots * 2 * 3 * 2 * size * (2 * size) ** 2

    far, wave, power = {}, {}, {}

    def forward(parts):
        outs = []
        for _, _, count in parts:
            outs += [(2 * size, count * size), (count, 2, size, size), (count, size, size)]
        results = call(
            functools.partial(forward_kernel, parts),
            outs,
            [SMEM, SMEM, VMEM, VMEM, VMEM],
            (metas, offsets, frame, probe, tables),
            flops * len(parts),
            work,
        )
        for at, (which, start, _) in enumerate(parts):
            far[which, start], wave[which, start], power[which, start] = results[3 * at : 3 * at + 3]

    spans = {
        0: metas,
        -1: left[rows : rows + kept].astype(jnp.int32),
        1: right[rows : rows + kept].astype(jnp.int32),
    }
    everything = [(which, down) for down in (-1, 0, 1) for which in range(offsets_count)]
    pieces = [(0, everything[::2]), (0, everything[1::2]), (-1, everything), (1, everything)]
    weight = None

    def add_weight(after):
        nonlocal weight
        across, chosen = pieces.pop(0)
        steps = [((which - down) % kept, down, which) for which, down in chosen]
        span, _ = lax.optimization_barrier((spans[across], after))
        (weight,) = call(
            functools.partial(weight_kernel, steps, (across,), row_count, weight is None),
            [(1, tiles + 1, tile_rows + 2 * size, size)],
            [SMEM, SMEM, VMEM] + ([] if weight is None else [VMEM]),
            (span, offsets, probe) + (() if weight is None else (weight,)),
            flops,
            aliases={} if weight is None else {3: 0},
        )

    forward([(most, *halves[0])])
    forward([(most, *halves[1])])
    sums = {start: power[most, start] for start, _ in halves}
    for which in reversed(range(most)):
        for start, _ in halves:
            arrived = lax.ppermute(sums[start], "row", ring("row", -1))
            if which == most - 1 and start == halves[-1][0]:
                forward([(w, *part) for w in reversed(range(most)) for part in halves])
            if which < most - 1 and pieces:
                add_weight(sums[start])
                arrived, weight = lax.optimization_barrier((arrived, weight))
            sums[start] = arrived
        for start, _ in halves:
            sums[start] = sums[start] + power[which, start]
    factors = {
        start: measured[0, 0, start : start + count] / jnp.sqrt(sums[start] + EPSILON) for start, count in halves
    }
    while pieces:
        add_weight(factors[0])

    total = None
    for which in range(offsets_count):
        if which:
            for start, _ in halves:
                value = lax.ppermute(factors[start], "row", ring("row", 1))
                if start == halves[-1][0] and which < most:
                    value, total = lax.optimization_barrier((value, total))
                factors[start] = value
        groups = [[part] for part in halves] if which == most else [list(halves)]
        for group in groups:
            fresh, last = total is None, which == most and group[-1] == halves[-1]
            outs = [(2, tiles, rows, size)]
            if last:
                outs += [(rows, size), (rows, size), (2, half, tile_columns), (2, half, tile_columns)]
            args = [metas, offsets, probe, tables]
            for start, _ in group:
                args += [far[which, start], wave[which, start], factors[start]]
            specs = [SMEM, SMEM] + [VMEM] * (len(args) - 2)
            if not fresh:
                args, specs = args + [total], specs + [VMEM]
            total, *sides = call(
                functools.partial(backward_kernel, [(which, *part) for part in group], fresh, last),
                outs,
                specs,
                args,
                flops * len(group),
                work,
                {} if fresh else {len(args) - 1: 0},
            )
    grad_in = send_rims(*sides)

    (new_object,) = call(
        final_kernel, [obj.shape], [VMEM] * 9, (obj, weight, total, *grad_in), 10**6
    )
    return new_object


def solution(mesh):
    return jax.shard_map(
        on_device,
        mesh=mesh,
        in_specs=(
            P(None, "row", "col"),
            P(),
            P("row", "col", None, None),
            P("row", "col"),
            P(),
            P("row", "col", None, None, None),
        ),
        out_specs=P(None, "row", "col"),
        check_vma=False,
    )
```

```python
import functools
import math

import jax
import jax.numpy as jnp
import numpy as np
from jax import lax
from jax.experimental import pallas as pl
from jax.experimental.pallas import tpu as pltpu
from jax.sharding import PartitionSpec as P

EPSILON = 0.5
DAMPING = 0.5


SMEM = pl.BlockSpec(memory_space=pltpu.SMEM)
VMEM = pl.BlockSpec(memory_space=pltpu.VMEM)
F32 = jnp.float32
BF16 = jnp.bfloat16


def call(kernel, outs, specs, args, flops, scratch=(), aliases=None):
    return pl.pallas_call(
        kernel,
        out_shape=[s if hasattr(s, "dtype") else jax.ShapeDtypeStruct(s, F32) for s in outs],
        in_specs=specs,
        out_specs=[VMEM] * len(outs),
        scratch_shapes=list(scratch),
        input_output_aliases=aliases or {},
        compiler_params=pltpu.CompilerParams(vmem_limit_bytes=16 * 2**20),
        cost_estimate=pl.CostEstimate(flops=flops, bytes_accessed=2**20, transcendentals=0),
    )(*args)


def dft_tables(length):
    index = np.arange(length)
    angle = (index[:, None] * index[None, :] % length) * (2.0 * math.pi / length)
    cos, sin = np.cos(angle) / math.sqrt(length), np.sin(angle) / math.sqrt(length)
    right = np.block([[cos, -sin], [sin, cos]])
    tables = []
    for table in (right, right.T):
        high = table.astype(BF16)
        tables += [high, (table - high.astype(np.float64)).astype(BF16)]
    return jnp.asarray(np.stack(tables))


def split(x):
    high = x.astype(BF16)
    return high, (x - high.astype(F32)).astype(BF16)


def dot3(a_high, a_low, b_high, b_low):
    dot = functools.partial(jnp.dot, preferred_element_type=F32)
    return dot(a_high, b_high) + (dot(a_low, b_high) + dot(a_high, b_low))


def lanes(rows, size):
    return lax.broadcasted_iota(jnp.int32, (rows, size), 1)


def turn(x):
    return pltpu.roll(x, x.shape[-1] // 2, 1)


def beam_of(offsets, which, slot):
    beam = jnp.int32(0)
    for index in range(1, offsets.shape[1]):
        beam = jnp.where(offsets[slot, index] == which, index, beam)
    return beam


def place(meta, slot, size):
    y, x = meta[0, 2 * slot], meta[0, 2 * slot + 1]
    return y, x // size, x % size


def edge_kernel(obj, positions, counts, place_of, edge_l, edge_r, meta):
    scans = positions.shape[2]
    values = [positions[0, 0, slot, axis] for slot in range(scans) for axis in range(2)]
    values += [counts[0, 0], place_of[0]]
    lane = lax.broadcasted_iota(jnp.int32, meta.shape, 1)
    row = jnp.zeros(meta.shape, jnp.int32)
    for at, value in enumerate(values):
        row = jnp.where(lane == at, value, row)
    meta[...] = row
    _, rows, columns = obj.shape
    size = edge_l.shape[1]
    low = lanes(rows, size) < size // 2
    near, far = slice(0, size), slice(columns - size, columns)
    edge_l[...] = jnp.where(low, obj[0, :, near], turn(obj[1, :, near]))
    edge_r[...] = jnp.where(low, turn(obj[0, :, far]), obj[1, :, far])


def frame_kernel(obj, top, bot, left, right, out):
    tiles, rows, size = out.shape[1:]
    half = size // 2
    low = lanes(half, size) < half
    for at in range(0, rows, half):
        body, src = obj, pl.ds(at - half, half)
        if at == 0:
            body, src = top, pl.ds(0, half)
        elif at == rows - half:
            body, src = bot, pl.ds(0, half)
        here = pl.ds(at, half)
        for ch in range(2):
            parts = [turn(body[ch, src, t * size : (t + 1) * size]) for t in range(tiles - 1)]
            edge_l, edge_r = left[here, :], right[here, :]
            edge_l = edge_l if ch == 0 else turn(edge_l)
            edge_r = turn(edge_r) if ch == 0 else edge_r
            parts = [edge_l, *parts, edge_r]
            for t in range(tiles):
                out[ch, t, here, :] = jnp.where(low, parts[t], parts[t + 1])


def forward_kernel(parts, adds, *refs):
    meta, offsets, frame, probe, tables = refs[:5]
    refs = refs[5:]
    if adds:
        arrived, refs = refs[0], refs[1:]
    outs, (x_high, x_low, y_high, y_low) = refs[:-4], refs[-4:]
    size = probe.shape[-1]
    lane = lanes(size, size)
    for at, (which, start, slots) in enumerate(parts):
        far, wave, power = outs[3 * at : 3 * at + 3]
        for index in range(slots):
            slot = start + index
            y, tile, shift = place(meta, slot, size)
            beam = beam_of(offsets, which, slot)
            back = lax.rem(size - shift, size)
            patch = []
            for ch in range(2):
                near = pltpu.roll(frame[ch, tile, pl.ds(y, size), :], back, 1)
                rest = pltpu.roll(frame[ch, tile + 1, pl.ds(y, size), :], back, 1)
                patch.append(jnp.where(lane < size - shift, near, rest))
            probe_re, probe_im = probe[beam, 0], probe[beam, 1]
            waves = (
                probe_re * patch[0] - probe_im * patch[1],
                probe_re * patch[1] + probe_im * patch[0],
            )
            rows = slice(index * size, (index + 1) * size)
            for ch in range(2):
                wave[index, ch] = waves[ch]
                columns = slice(ch * size, (ch + 1) * size)
                x_high[rows, columns], x_low[rows, columns] = split(waves[ch])
        for slot in range(0, slots, 2):
            rows = slice(slot * size, (slot + 2) * size)
            mid = dot3(x_high[rows, :], x_low[rows, :], tables[0], tables[1])
            for sub in range(2):
                columns = slice((slot + sub) * size, (slot + sub + 1) * size)
                for ch in range(2):
                    piece = mid[sub * size : (sub + 1) * size, ch * size : (ch + 1) * size]
                    into = slice(ch * size, (ch + 1) * size)
                    y_high[into, columns], y_low[into, columns] = split(piece)
            columns = slice(slot * size, (slot + 2) * size)
            result = dot3(tables[2], tables[3], y_high[:, columns], y_low[:, columns])
            far[:, columns] = result
            for sub in range(2):
                inside = slice(sub * size, (sub + 1) * size)
                re, im = result[:size, inside], result[size:, inside]
                rows = slice((slot + sub) * size, (slot + sub + 1) * size)
                own = re * re + im * im
                power[rows, :] = own + arrived[rows, :] if adds else own
        if power.shape[0] > slots * size:
            scans = offsets.shape[0]
            lane = lanes(power.shape[0] - slots * size, size)
            row = jnp.zeros(lane.shape, jnp.int32)
            for index in range(2 * scans + 1):
                row = jnp.where(lane == index, meta[0, index], row)
            power[slots * size :, :] = row.astype(F32)


def add_patch(total, channel, y, tile, shift, value, lane):
    moved = pltpu.roll(value, shift, 1)
    rows = pl.ds(y, value.shape[0])
    total[channel, tile, rows, :] += jnp.where(lane >= shift, moved, 0.0)
    total[channel, tile + 1, rows, :] += jnp.where(lane < shift, moved, 0.0)


def write_sides(total, weight, side_l, side_r):
    _, tiles, rows, size = total.shape
    last, middle = tiles - 1, rows // 2
    low = lanes(rows, size) < size // 2
    side_l[:rows, :] = jnp.where(low, total[0, 0], turn(total[1, 0]))
    side_r[:rows, :] = jnp.where(low, turn(total[0, last]), total[1, last])
    low = lanes(middle, size) < size // 2
    side_l[rows:, :] = jnp.where(low, weight[0, 0, :middle, :], turn(weight[0, 0, middle:, :]))
    side_r[rows:, :] = jnp.where(low, turn(weight[0, last, :middle, :]), weight[0, last, middle:, :])


def own_columns(total, channel, rows, low):
    tiles = total.shape[1]
    turned = [turn(total[channel, t, rows, :]) for t in range(tiles)]
    return [jnp.where(low, turned[t], turned[t + 1]) for t in range(tiles - 1)]


def write_rims(total, weight, rim_top, rim_bot):
    channels, _, rows, size = total.shape
    half = size // 2
    low = lanes(half, size) < half
    for ch in range(channels + 1):
        source, at = (weight, 0) if ch == channels else (total, ch)
        for start, out in ((0, rim_top), (rows - half, rim_bot)):
            for t, value in enumerate(own_columns(source, at, pl.ds(start, half), low)):
                out[ch, :, t * size : (t + 1) * size] = value


def backward_kernel(parts, fresh, last, *refs):
    meta, offsets, probe, tables = refs[:4]
    inputs, refs = refs[4 : 4 + 3 * len(parts)], refs[4 + 3 * len(parts) :]
    if last:
        weight, refs = refs[0], refs[1:]
    if not fresh:
        refs = refs[1:]
    total, refs = refs[0], refs[1:]
    if last:
        (side_l, side_r, rim_top, rim_bot), refs = refs[:4], refs[4:]
    x_high, x_low, y_high, y_low = refs
    size = probe.shape[-1]
    scans = offsets.shape[0]
    lane = lanes(size, size)
    if fresh:
        total[...] = jnp.zeros_like(total)
    for at, (which, start, slots) in enumerate(parts):
        far, wave, factor = inputs[3 * at : 3 * at + 3]
        for slot in range(0, slots, 2):
            for sub in range(2):
                columns = slice((slot + sub) * size, (slot + sub + 1) * size)
                scale = factor[slot + sub]
                for ch in range(2):
                    into = slice(ch * size, (ch + 1) * size)
                    y_high[into, columns], y_low[into, columns] = split(far[into, columns] * scale)
            columns = slice(slot * size, (slot + 2) * size)
            mid = dot3(tables[0], tables[1], y_high[:, columns], y_low[:, columns])
            for sub in range(2):
                rows = slice((slot + sub) * size, (slot + sub + 1) * size)
                for ch in range(2):
                    piece = mid[ch * size : (ch + 1) * size, sub * size : (sub + 1) * size]
                    into = slice(ch * size, (ch + 1) * size)
                    x_high[rows, into], x_low[rows, into] = split(piece)
            rows = slice(slot * size, (slot + 2) * size)
            result = dot3(x_high[rows, :], x_low[rows, :], tables[2], tables[3])
            for sub in range(2):
                true_slot = start + slot + sub
                live = (true_slot < meta[0, 2 * scans]).astype(F32)
                beam = beam_of(offsets, which, true_slot)
                probe_re, probe_im = probe[beam, 0], probe[beam, 1]
                inside = slice(sub * size, (sub + 1) * size)
                change_re = (result[inside, :size] - wave[slot + sub, 0]) * live
                change_im = (result[inside, size:] - wave[slot + sub, 1]) * live
                grad_re = probe_re * change_re + probe_im * change_im
                grad_im = probe_re * change_im - probe_im * change_re
                spot = place(meta, true_slot, size)
                add_patch(total, 0, *spot, grad_re, lane)
                add_patch(total, 1, *spot, grad_im, lane)
    if last:
        write_sides(total, weight, side_l, side_r)
        write_rims(total, weight, rim_top, rim_bot)


def weight_kernel(*refs):
    metas, (offsets, probe, total) = refs[:-3], refs[-3:]
    size = probe.shape[-1]
    scans = offsets.shape[0]
    lane = lanes(size, size)
    total[...] = jnp.zeros_like(total)
    for which, meta in enumerate(metas):

        def add(slot, carry, which=which, meta=meta):
            @pl.when(slot < meta[0, 2 * scans])
            def _():
                beam = beam_of(offsets, which, slot)
                probe_re, probe_im = probe[beam, 0], probe[beam, 1]
                value = probe_re * probe_re + probe_im * probe_im
                add_patch(total, 0, *place(meta, slot, size), value, lane)

            return carry

        lax.fori_loop(0, scans, add, 0)


def gathered(total, weight, side_l, side_r, in_top, in_bot, in_ctop, in_cbot, channel, chunk, half):
    _, tiles, rows, size = total.shape
    chunks = (rows - size) // half
    low = lanes(half, size) < half
    start = (chunk + 1) * half
    at, of_upper = pl.ds(start, half), channel == 0
    if channel == 2:
        values = own_columns(weight, 0, at, low)
        of_upper = start < rows // 2
        at = pl.ds(rows + start % (rows // 2), half)
    else:
        values = own_columns(total, channel, at, low)

    def add_sides(from_l, from_r, of_upper):
        from_l = from_l if of_upper else turn(from_l)
        from_r = turn(from_r) if of_upper else from_r
        values[0] += jnp.where(low, from_l, 0.0)
        values[-1] += jnp.where(low, 0.0, from_r)

    add_sides(side_l[at, :], side_r[at, :], of_upper)
    for where, rim, corner in ((0, in_top, in_ctop), (chunks - 1, in_bot, in_cbot)):
        if chunk == where:
            for t in range(tiles - 1):
                values[t] += rim[channel, :, t * size : (t + 1) * size]
            if channel == 2:
                values[0] += jnp.where(low, corner[2], 0.0)
                values[-1] += jnp.where(low, 0.0, corner[2])
            else:
                add_sides(corner[0], corner[1], of_upper)
    return values


def final_kernel(*refs):
    obj, out = refs[0], refs[-1]
    grads = refs[1:9]
    size = grads[0].shape[-1]
    half = size // 2
    for chunk in range(obj.shape[1] // half):
        scale = [1.0 / (w + DAMPING) for w in gathered(*grads, 2, chunk, half)]
        rows = slice(chunk * half, (chunk + 1) * half)
        for ch in range(2):
            for t, value in enumerate(gathered(*grads, ch, chunk, half)):
                columns = slice(t * size, (t + 1) * size)
                out[ch, rows, columns] = obj[ch, rows, columns] + value * scale[t]


def line(axis, by):
    count = lax.axis_size(axis)
    return [(i, i + by) for i in range(count) if 0 <= i + by < count]


def ring(axis, by):
    count = lax.axis_size(axis)
    return [(i, (i + by) % count) for i in range(count)]


def send_rims(side_l, side_r, rim_top, rim_bot):
    _, half, _ = rim_top.shape
    size = side_l.shape[1]
    rows = side_l.shape[0] * 2 // 3
    in_r = lax.ppermute(side_l, "col", line("col", -1))
    in_l = lax.ppermute(side_r, "col", line("col", 1))
    in_bot = lax.ppermute(rim_top, "row", line("row", -1))
    in_top = lax.ppermute(rim_bot, "row", line("row", 1))

    def corner(start, columns):
        at = rows + start % (rows // 2)
        weight = jnp.concatenate([x[at : at + half, columns] for x in (in_l, in_r)], axis=1)
        return jnp.stack([in_l[start : start + half], in_r[start : start + half], weight])

    in_cbot = lax.ppermute(corner(0, slice(0, half)), "row", line("row", -1))
    in_ctop = lax.ppermute(corner(rows - half, slice(half, size)), "row", line("row", 1))
    return in_l, in_r, in_top, in_bot, in_ctop, in_cbot


def on_device(obj, probe, positions, counts, offsets, measured):
    offsets_count, _, size, _ = probe.shape
    scans = positions.shape[2]
    half = size // 2
    tile_rows, tile_columns = obj.shape[1:]
    rows, tiles = tile_rows + size, tile_columns // size + 1
    tables = dft_tables(size)

    def packed(x):
        return jnp.concatenate([x[0], x[1]], axis=1)

    edge_l, edge_r, meta = call(
        edge_kernel,
        [(tile_rows, size)] * 2 + [jax.ShapeDtypeStruct((1, size), jnp.int32)],
        [VMEM, SMEM, SMEM, SMEM],
        (obj, positions, counts, lax.axis_index("row").astype(jnp.int32).reshape(1)),
        10**6,
    )
    top = lax.ppermute(obj[:, tile_rows - half :], "row", line("row", 1))
    bot = lax.ppermute(obj[:, :half], "row", line("row", -1))

    most = offsets_count - 1
    metas = {0: meta, most: lax.ppermute(meta, "row", ring("row", most))}

    edge_l, edge_r = (
        jnp.concatenate([packed(top[:, :, part]), edge, packed(bot[:, :, part])])
        for part, edge in ((slice(0, half), edge_l), (slice(tile_columns - half, None), edge_r))
    )
    left = lax.ppermute(edge_r, "col", line("col", 1))
    right = lax.ppermute(edge_l, "col", line("col", -1))
    (frame,) = call(
        frame_kernel, [(2, tiles, rows, size)], [VMEM] * 5, (obj, top, bot, left, right), 10**6
    )

    slots = scans // 2
    halves = ((0, slots), (slots, scans - slots))
    work = [
        pltpu.VMEM((slots * size, 2 * size), BF16),
        pltpu.VMEM((slots * size, 2 * size), BF16),
        pltpu.VMEM((2 * size, slots * size), BF16),
        pltpu.VMEM((2 * size, slots * size), BF16),
    ]
    flops = slots * 2 * 3 * 2 * size * (2 * size) ** 2

    far, wave, power = {}, {}, {}

    def forward(which, parts, arrived=None):
        outs = []
        for start, count in parts:
            tail = 8 if which and start == 0 else 0
            outs += [(2 * size, count * size), (count, 2, size, size), (count * size + tail, size)]
        adds = arrived is not None
        results = call(
            functools.partial(forward_kernel, [(which, *part) for part in parts], adds),
            outs,
            [SMEM, SMEM, VMEM, VMEM, VMEM] + [VMEM] * adds,
            (metas[which], offsets, frame, probe, tables) + ((arrived,) if adds else ()),
            flops * len(parts),
            work,
        )
        for at, (start, _) in enumerate(parts):
            far[which, start], wave[which, start], power[which, start] = results[3 * at : 3 * at + 3]

    forward(most, [halves[0]])
    forward(most, [halves[1]])
    forward(0, list(halves))
    for which in reversed(range(most)):
        for start, count in halves:
            arrived = lax.ppermute(power[which + 1, start], "row", ring("row", -1))
            if which:
                if start == 0:
                    metas[which] = arrived[count * size : count * size + 1].astype(jnp.int32)
                forward(which, [(start, count)], arrived)
            else:
                power[0, start] += arrived[: count * size]
    factors = {
        start: measured[0, 0, start : start + count]
        / jnp.sqrt(power[0, start].reshape(count, size, size) + EPSILON)
        for start, count in halves
    }
    (weight,) = call(
        weight_kernel,
        [(1, tiles, rows, size)],
        [SMEM] * (offsets_count + 1) + [VMEM],
        (*(metas[which] for which in range(offsets_count)), offsets, probe),
        flops,
    )

    total = None
    for which in range(offsets_count):
        if which:
            for start, _ in halves:
                value = lax.ppermute(factors[start], "row", ring("row", 1))
                if start == halves[-1][0] and which < most:
                    if which == 1:
                        value, weight = lax.optimization_barrier((value, weight))
                    value, total = lax.optimization_barrier((value, total))
                factors[start] = value
        groups = [[part] for part in halves] if which == most else [list(halves)]
        for group in groups:
            fresh, last = total is None, which == most and group[-1] == halves[-1]
            outs = [(2, tiles, rows, size)]
            if last:
                outs += [(rows + rows // 2, size)] * 2 + [(3, half, tile_columns)] * 2
            args = [metas[which], offsets, probe, tables]
            for start, _ in group:
                args += [far[which, start], wave[which, start], factors[start]]
            args += [weight] if last else []
            specs = [SMEM, SMEM] + [VMEM] * (len(args) - 2)
            if not fresh:
                args, specs = args + [total], specs + [VMEM]
            total, *sides = call(
                functools.partial(backward_kernel, [(which, *part) for part in group], fresh, last),
                outs,
                specs,
                args,
                flops * len(group),
                work,
                {} if fresh else {len(args) - 1: 0},
            )
    grad_in = send_rims(*sides)

    (new_object,) = call(
        final_kernel, [obj.shape], [VMEM] * 9, (obj, total, weight, *grad_in), 10**6
    )
    return new_object


def solution(mesh):
    return jax.shard_map(
        on_device,
        mesh=mesh,
        in_specs=(
            P(None, "row", "col"),
            P(),
            P("row", "col", None, None),
            P("row", "col"),
            P(),
            P("row", "col", None, None, None),
        ),
        out_specs=P(None, "row", "col"),
        check_vma=False,
    )
```

```python
import functools
import math

import jax
import jax.numpy as jnp
import numpy as np
from jax import lax
from jax.experimental import pallas as pl
from jax.experimental.pallas import tpu as pltpu
from jax.sharding import PartitionSpec as P

EPSILON = 0.5
DAMPING = 0.5


SMEM = pl.BlockSpec(memory_space=pltpu.SMEM)
VMEM = pl.BlockSpec(memory_space=pltpu.VMEM)
F32 = jnp.float32
BF16 = jnp.bfloat16


def call(kernel, outs, specs, args, flops, scratch=(), aliases=None):
    return pl.pallas_call(
        kernel,
        out_shape=[s if hasattr(s, "dtype") else jax.ShapeDtypeStruct(s, F32) for s in outs],
        in_specs=specs,
        out_specs=[VMEM] * len(outs),
        scratch_shapes=list(scratch),
        input_output_aliases=aliases or {},
        compiler_params=pltpu.CompilerParams(vmem_limit_bytes=16 * 2**20),
        cost_estimate=pl.CostEstimate(flops=flops, bytes_accessed=2**20, transcendentals=0),
    )(*args)


def dft_tables(length):
    index = np.arange(length)
    angle = (index[:, None] * index[None, :] % length) * (2.0 * math.pi / length)
    cos, sin = np.cos(angle) / math.sqrt(length), np.sin(angle) / math.sqrt(length)
    right = np.block([[cos, -sin], [sin, cos]])
    tables = []
    for table in (right, right.T):
        high = table.astype(BF16)
        tables += [high, (table - high.astype(np.float64)).astype(BF16)]
    return jnp.asarray(np.stack(tables))


def split(x):
    high = x.astype(BF16)
    return high, (x - high.astype(F32)).astype(BF16)


def dot3(a_high, a_low, b_high, b_low):
    dot = functools.partial(jnp.dot, preferred_element_type=F32)
    return dot(a_high, b_high) + (dot(a_low, b_high) + dot(a_high, b_low))


def lanes(rows, size):
    return lax.broadcasted_iota(jnp.int32, (rows, size), 1)


def turn(x):
    return pltpu.roll(x, x.shape[-1] // 2, 1)


def beam_of(meta, which, slot, scans, beams):
    beam = jnp.int32(0)
    for index in range(1, beams):
        beam = jnp.where(meta[0, 2 * scans + 2 + slot * beams + index] == which, index, beam)
    return beam


def place(meta, slot, size):
    y, x = meta[0, 2 * slot], meta[0, 2 * slot + 1]
    return y, x // size, x % size


def edge_kernel(obj, positions, counts, offsets, place_of, edge_l, edge_r, meta):
    scans = positions.shape[2]
    values = [positions[0, 0, slot, axis] for slot in range(scans) for axis in range(2)]
    values += [counts[0, 0], place_of[0]]
    values += [offsets[slot, beam] for slot in range(scans) for beam in range(offsets.shape[1])]
    assert len(values) <= meta.shape[1]
    lane = lax.broadcasted_iota(jnp.int32, meta.shape, 1)
    row = jnp.zeros(meta.shape, jnp.int32)
    for at, value in enumerate(values):
        row = jnp.where(lane == at, value, row)
    meta[...] = row
    _, rows, columns = obj.shape
    size = edge_l.shape[1]
    low = lanes(rows, size) < size // 2
    near, far = slice(0, size), slice(columns - size, columns)
    edge_l[...] = jnp.where(low, obj[0, :, near], turn(obj[1, :, near]))
    edge_r[...] = jnp.where(low, turn(obj[0, :, far]), obj[1, :, far])


def frame_kernel(obj, top, bot, left, right, out):
    tiles, rows, size = out.shape[1:]
    half = size // 2
    low = lanes(half, size) < half
    for at in range(0, rows, half):
        body, src = obj, pl.ds(at - half, half)
        if at == 0:
            body, src = top, pl.ds(0, half)
        elif at == rows - half:
            body, src = bot, pl.ds(0, half)
        here = pl.ds(at, half)
        for ch in range(2):
            parts = [turn(body[ch, src, t * size : (t + 1) * size]) for t in range(tiles - 1)]
            edge_l, edge_r = left[here, :], right[here, :]
            edge_l = edge_l if ch == 0 else turn(edge_l)
            edge_r = turn(edge_r) if ch == 0 else edge_r
            parts = [edge_l, *parts, edge_r]
            for t in range(tiles):
                out[ch, t, here, :] = jnp.where(low, parts[t], parts[t + 1])


def forward_kernel(parts, scans, adds, *refs):
    meta, frame, probe, tables = refs[:4]
    refs = refs[4:]
    if adds:
        arrived, refs = refs[0], refs[1:]
    outs, (x_high, x_low, y_high, y_low) = refs[:-4], refs[-4:]
    size = probe.shape[-1]
    lane = lanes(size, size)
    for at, (which, start, slots) in enumerate(parts):
        far, wave, power = outs[3 * at : 3 * at + 3]
        for index in range(slots):
            slot = start + index
            y, tile, shift = place(meta, slot, size)
            beam = beam_of(meta, which, slot, scans, probe.shape[0])
            back = lax.rem(size - shift, size)
            patch = []
            for ch in range(2):
                near = pltpu.roll(frame[ch, tile, pl.ds(y, size), :], back, 1)
                rest = pltpu.roll(frame[ch, tile + 1, pl.ds(y, size), :], back, 1)
                patch.append(jnp.where(lane < size - shift, near, rest))
            probe_re, probe_im = probe[beam, 0], probe[beam, 1]
            waves = (
                probe_re * patch[0] - probe_im * patch[1],
                probe_re * patch[1] + probe_im * patch[0],
            )
            rows = slice(index * size, (index + 1) * size)
            for ch in range(2):
                wave[index, ch] = waves[ch]
                columns = slice(ch * size, (ch + 1) * size)
                x_high[rows, columns], x_low[rows, columns] = split(waves[ch])
        for slot in range(0, slots, 2):
            rows = slice(slot * size, (slot + 2) * size)
            mid = dot3(x_high[rows, :], x_low[rows, :], tables[0], tables[1])
            for sub in range(2):
                columns = slice((slot + sub) * size, (slot + sub + 1) * size)
                for ch in range(2):
                    piece = mid[sub * size : (sub + 1) * size, ch * size : (ch + 1) * size]
                    into = slice(ch * size, (ch + 1) * size)
                    y_high[into, columns], y_low[into, columns] = split(piece)
            columns = slice(slot * size, (slot + 2) * size)
            result = dot3(tables[2], tables[3], y_high[:, columns], y_low[:, columns])
            far[:, columns] = result
            for sub in range(2):
                inside = slice(sub * size, (sub + 1) * size)
                re, im = result[:size, inside], result[size:, inside]
                rows = slice((slot + sub) * size, (slot + sub + 1) * size)
                own = re * re + im * im
                power[rows, :] = own + arrived[rows, :] if adds else own
        if power.shape[0] > slots * size:
            lane = lanes(power.shape[0] - slots * size, size)
            row = jnp.zeros(lane.shape, jnp.int32)
            for index in range(2 * scans + 2 + scans * probe.shape[0]):
                row = jnp.where(lane == index, meta[0, index], row)
            power[slots * size :, :] = row.astype(F32)


def add_patch(total, channel, y, tile, shift, value, lane):
    moved = pltpu.roll(value, shift, 1)
    rows = pl.ds(y, value.shape[0])
    total[channel, tile, rows, :] += jnp.where(lane >= shift, moved, 0.0)
    total[channel, tile + 1, rows, :] += jnp.where(lane < shift, moved, 0.0)


def write_sides(total, side_l, side_r):
    _, tiles, rows, size = total.shape
    low = lanes(rows, size) < size // 2
    side_l[...] = jnp.where(low, total[0, 0], turn(total[1, 0]))
    side_r[...] = jnp.where(low, turn(total[0, tiles - 1]), total[1, tiles - 1])


def own_columns(total, channel, rows, low):
    tiles = total.shape[1]
    turned = [turn(total[channel, t, rows, :]) for t in range(tiles)]
    return [jnp.where(low, turned[t], turned[t + 1]) for t in range(tiles - 1)]


def write_rims(total, rim_top, rim_bot):
    channels, _, rows, size = total.shape
    half = size // 2
    low = lanes(half, size) < half
    for ch in range(channels):
        for start, out in ((0, rim_top), (rows - half, rim_bot)):
            for t, value in enumerate(own_columns(total, ch, pl.ds(start, half), low)):
                out[ch, :, t * size : (t + 1) * size] = value


def backward_kernel(parts, scans, fresh, last, *refs):
    meta, probe, tables = refs[:3]
    inputs, refs = refs[3 : 3 + 3 * len(parts)], refs[3 + 3 * len(parts) :]
    if not fresh:
        refs = refs[1:]
    total, refs = refs[0], refs[1:]
    if last:
        (side_l, side_r, rim_top, rim_bot), refs = refs[:4], refs[4:]
    x_high, x_low, y_high, y_low = refs
    size = probe.shape[-1]
    lane = lanes(size, size)
    if fresh:
        total[...] = jnp.zeros_like(total)
    for at, (which, start, slots) in enumerate(parts):
        far, wave, factor = inputs[3 * at : 3 * at + 3]
        for slot in range(0, slots, 2):
            for sub in range(2):
                columns = slice((slot + sub) * size, (slot + sub + 1) * size)
                scale = factor[(slot + sub) * size : (slot + sub + 1) * size, :]
                for ch in range(2):
                    into = slice(ch * size, (ch + 1) * size)
                    y_high[into, columns], y_low[into, columns] = split(far[into, columns] * scale)
            columns = slice(slot * size, (slot + 2) * size)
            mid = dot3(tables[0], tables[1], y_high[:, columns], y_low[:, columns])
            for sub in range(2):
                rows = slice((slot + sub) * size, (slot + sub + 1) * size)
                for ch in range(2):
                    piece = mid[ch * size : (ch + 1) * size, sub * size : (sub + 1) * size]
                    into = slice(ch * size, (ch + 1) * size)
                    x_high[rows, into], x_low[rows, into] = split(piece)
            rows = slice(slot * size, (slot + 2) * size)
            result = dot3(x_high[rows, :], x_low[rows, :], tables[2], tables[3])
            for sub in range(2):
                true_slot = start + slot + sub
                live = (true_slot < meta[0, 2 * scans]).astype(F32)
                beam = beam_of(meta, which, true_slot, scans, probe.shape[0])
                probe_re, probe_im = probe[beam, 0], probe[beam, 1]
                inside = slice(sub * size, (sub + 1) * size)
                change_re = (result[inside, :size] - wave[slot + sub, 0]) * live
                change_im = (result[inside, size:] - wave[slot + sub, 1]) * live
                grad_re = probe_re * change_re + probe_im * change_im
                grad_im = probe_re * change_im - probe_im * change_re
                spot = place(meta, true_slot, size)
                add_patch(total, 0, *spot, grad_re, lane)
                add_patch(total, 1, *spot, grad_im, lane)
    if last:
        write_sides(total, side_l, side_r)
        write_rims(total, rim_top, rim_bot)


def weight_kernel(steps, scans, which_tile, row_count, fresh, *refs):
    metas, probe, total = refs[0], refs[1], refs[-1]
    _, tiles, rows, size = total.shape
    half = size // 2
    own_rows, own_columns = rows - 2 * size, (tiles - 2) * size
    lane = lanes(size, size)
    if fresh:
        total[...] = jnp.zeros_like(total)
    at_row = lax.rem(metas[0, 2 * scans + 1] + which_tile + row_count, row_count)
    for row, across in enumerate((0, -1, 1)):
        for down, which in steps:

            def add(slot, carry, row=row, across=across, down=down, which=which):
                y = metas[row, 2 * slot] + (down * own_rows + half)
                x = metas[row, 2 * slot + 1] + (across * own_columns + half)
                near = (y > 0) & (y < rows - size) & (x > 0) & (x < (tiles - 1) * size)
                below = at_row + down
                live = (slot < metas[row, 2 * scans]) & (below >= 0) & (below < row_count)

                @pl.when(near & live)
                def _():
                    beam = beam_of(metas, which, slot, scans, probe.shape[0])
                    probe_re, probe_im = probe[beam, 0], probe[beam, 1]
                    value = probe_re * probe_re + probe_im * probe_im
                    add_patch(total, 0, y, x // size, x % size, value, lane)

                return carry

            lax.fori_loop(0, scans, add, 0)


def gathered(total, side_l, side_r, in_top, in_bot, in_ctop, in_cbot, channel, chunk, half):
    _, tiles, rows, size = total.shape
    chunks = (rows - size) // half
    low = lanes(half, size) < half
    ext = pl.ds((chunk + 1) * half, half)
    values = own_columns(total, channel, ext, low)

    def add_sides(from_l, from_r):
        from_l = from_l if channel == 0 else turn(from_l)
        from_r = turn(from_r) if channel == 0 else from_r
        values[0] += jnp.where(low, from_l, 0.0)
        values[-1] += jnp.where(low, 0.0, from_r)

    add_sides(side_l[ext, :], side_r[ext, :])
    for at, rim, corner in ((0, in_top, in_ctop), (chunks - 1, in_bot, in_cbot)):
        if chunk == at:
            for t in range(tiles - 1):
                values[t] += rim[channel, :, t * size : (t + 1) * size]
            add_sides(corner[0], corner[1])
    return values


def final_kernel(*refs):
    obj, weight, out = refs[0], refs[1], refs[-1]
    grads = refs[2:9]
    size = grads[0].shape[-1]
    half = size // 2
    tiles = obj.shape[2] // size
    for chunk in range(obj.shape[1] // half):
        wide = pl.ds(size + chunk * half, half)
        scale = [1.0 / (weight[0, t + 1, wide, :] + DAMPING) for t in range(tiles)]
        rows = slice(chunk * half, (chunk + 1) * half)
        for ch in range(2):
            for t, value in enumerate(gathered(*grads, ch, chunk, half)):
                columns = slice(t * size, (t + 1) * size)
                out[ch, rows, columns] = obj[ch, rows, columns] + value * scale[t]


def line(axis, by):
    count = lax.axis_size(axis)
    return [(i, i + by) for i in range(count) if 0 <= i + by < count]


def ring(axis, by):
    count = lax.axis_size(axis)
    return [(i, (i + by) % count) for i in range(count)]


def move(x, axis, pairs):
    return lax.ppermute(x, axis, pairs)


def send_rims(side_l, side_r, rim_top, rim_bot):
    rows, size = side_l.shape
    half = size // 2
    in_r = move(side_l, "col", line("col", -1))
    in_l = move(side_r, "col", line("col", 1))
    in_bot = move(rim_top, "row", line("row", -1))
    in_top = move(rim_bot, "row", line("row", 1))
    corner_top = jnp.stack([in_l[:half], in_r[:half]])
    corner_bot = jnp.stack([in_l[rows - half :], in_r[rows - half :]])
    in_cbot = move(corner_top, "row", line("row", -1))
    in_ctop = move(corner_bot, "row", line("row", 1))
    return in_l, in_r, in_top, in_bot, in_ctop, in_cbot


def on_device(obj, probe, positions, counts, offsets, measured):
    offsets_count, _, size, _ = probe.shape
    scans = positions.shape[2]
    half = size // 2
    tile_rows, tile_columns = obj.shape[1:]
    rows, tiles = tile_rows + size, tile_columns // size + 1
    row_count = lax.axis_size("row")
    tables = dft_tables(size)

    def packed(x):
        return jnp.concatenate([x[0], x[1]], axis=1)

    edge_l, edge_r, meta = call(
        edge_kernel,
        [(tile_rows, size)] * 2 + [jax.ShapeDtypeStruct((1, size), jnp.int32)],
        [VMEM, SMEM, SMEM, SMEM, SMEM],
        (obj, positions, counts, offsets, lax.axis_index("row").astype(jnp.int32).reshape(1)),
        10**6,
    )
    top = move(obj[:, tile_rows - half :], "row", line("row", 1))
    bot = move(obj[:, :half], "row", line("row", -1))

    most = offsets_count - 1
    metas = {0: meta, most: move(meta, "row", ring("row", most))}

    own_meta = jnp.broadcast_to(meta.astype(F32), (8, size))
    edge_l, edge_r = (
        jnp.concatenate([packed(top[:, :, part]), edge, packed(bot[:, :, part]), own_meta])
        for part, edge in ((slice(0, half), edge_l), (slice(tile_columns - half, None), edge_r))
    )
    left = move(edge_r, "col", line("col", 1))
    right = move(edge_l, "col", line("col", -1))
    (frame,) = call(
        frame_kernel, [(2, tiles, rows, size)], [VMEM] * 5, (obj, top, bot, left, right), 10**6
    )

    slots = scans // 2
    halves = ((0, slots), (slots, scans - slots))
    work = [
        pltpu.VMEM((slots * size, 2 * size), BF16),
        pltpu.VMEM((slots * size, 2 * size), BF16),
        pltpu.VMEM((2 * size, slots * size), BF16),
        pltpu.VMEM((2 * size, slots * size), BF16),
    ]
    flops = slots * 2 * 3 * 2 * size * (2 * size) ** 2

    far, wave, power = {}, {}, {}

    def forward(which, parts, arrived=None):
        outs = []
        for start, count in parts:
            tail = 8 if which and start == 0 else 0
            outs += [(2 * size, count * size), (count, 2, size, size), (count * size + tail, size)]
        adds = arrived is not None
        results = call(
            functools.partial(forward_kernel, [(which, *part) for part in parts], scans, adds),
            outs,
            [SMEM, VMEM, VMEM, VMEM] + [VMEM] * adds,
            (metas[which], frame, probe, tables) + ((arrived,) if adds else ()),
            flops * len(parts),
            work,
        )
        for at, (start, _) in enumerate(parts):
            far[which, start], wave[which, start], power[which, start] = results[3 * at : 3 * at + 3]

    forward(most, [halves[0]])
    forward(most, [halves[1]])
    forward(0, list(halves))
    for which in reversed(range(most)):
        for start, count in halves:
            arrived = move(power[which + 1, start], "row", ring("row", -1))
            if which:
                if start == 0:
                    metas[which] = arrived[count * size : count * size + 1].astype(jnp.int32)
                forward(which, [(start, count)], arrived)
            else:
                power[0, start] += arrived[: count * size]
    factors = {
        start: measured[0, 0, start : start + count].reshape(count * size, size) / jnp.sqrt(power[0, start] + EPSILON)
        for start, count in halves
    }
    beside = jnp.concatenate([left[rows : rows + 1], right[rows : rows + 1], jnp.zeros((6, size), F32)])
    factors[0] = jnp.concatenate([factors[0], beside])

    row_count = lax.axis_size("row")
    kept = min(row_count, offsets_count + 2)
    weight = None

    def add_weight(index, shift, beside):
        nonlocal weight
        own = metas[shift] if shift in metas else None
        if own is None:
            span = move(jnp.concatenate([meta.astype(F32), beside[:2]]), "row", ring("row", shift))
            span = span.astype(jnp.int32)
        else:
            span = jnp.concatenate([own, beside[:2].astype(jnp.int32)])
        steps = [(d, w) for d in (-1, 0, 1) for w in range(offsets_count) if (w - d) % kept == index]
        (weight,) = call(
            functools.partial(weight_kernel, steps, scans, shift, row_count, weight is None),
            [(1, tiles + 1, tile_rows + 2 * size, size)],
            [SMEM, VMEM] + ([] if weight is None else [VMEM]),
            (span, probe) + (() if weight is None else (weight,)),
            flops,
            aliases={} if weight is None else {2: 0},
        )

    for index in range(offsets_count, kept):
        add_weight(index, index if index <= offsets_count else index - kept, beside)

    total = None
    for which in range(offsets_count):
        if which:
            for start, _ in halves:
                value = move(factors[start], "row", ring("row", 1))
                if start == halves[-1][0]:
                    value, weight = lax.optimization_barrier((value, weight))
                    if which < most:
                        value, total = lax.optimization_barrier((value, total))
                factors[start] = value
                if start == halves[-1][0]:
                    add_weight(which, which, factors[0][slots * size :])
        else:
            add_weight(0, 0, beside)
        groups = [[part] for part in halves] if which == most else [list(halves)]
        for group in groups:
            fresh, last = total is None, which == most and group[-1] == halves[-1]
            outs = [(2, tiles, rows, size)]
            if last:
                outs += [(rows, size)] * 2 + [(2, half, tile_columns)] * 2
            args = [metas[which], probe, tables]
            for start, _ in group:
                args += [far[which, start], wave[which, start], factors[start]]
            specs = [SMEM] + [VMEM] * (len(args) - 1)
            if not fresh:
                args, specs = args + [total], specs + [VMEM]
            total, *sides = call(
                functools.partial(backward_kernel, [(which, *part) for part in group], scans, fresh, last),
                outs,
                specs,
                args,
                flops * len(group),
                work,
                {} if fresh else {len(args) - 1: 0},
            )
    grad_in = send_rims(*sides)

    (new_object,) = call(
        final_kernel, [obj.shape], [VMEM] * 9, (obj, weight, total, *grad_in), 10**6
    )
    return new_object


def solution(mesh):
    return jax.shard_map(
        on_device,
        mesh=mesh,
        in_specs=(
            P(None, "row", "col"),
            P(),
            P("row", "col", None, None),
            P("row", "col"),
            P(),
            P("row", "col", None, None, None),
        ),
        out_specs=P(None, "row", "col"),
        check_vma=False,
    )
```

```python
import functools
import math

import jax
import jax.numpy as jnp
import numpy as np
from jax import lax
from jax.experimental import pallas as pl
from jax.experimental.pallas import tpu as pltpu
from jax.sharding import PartitionSpec as P

EPSILON = 0.5
DAMPING = 0.5


SMEM = pl.BlockSpec(memory_space=pltpu.SMEM)
VMEM = pl.BlockSpec(memory_space=pltpu.VMEM)
F32 = jnp.float32
BF16 = jnp.bfloat16


def call(kernel, outs, specs, args, flops, scratch=(), aliases=None):
    return pl.pallas_call(
        kernel,
        out_shape=[s if hasattr(s, "dtype") else jax.ShapeDtypeStruct(s, F32) for s in outs],
        in_specs=specs,
        out_specs=[VMEM] * len(outs),
        scratch_shapes=list(scratch),
        input_output_aliases=aliases or {},
        compiler_params=pltpu.CompilerParams(vmem_limit_bytes=16 * 2**20),
        cost_estimate=pl.CostEstimate(flops=flops, bytes_accessed=2**20, transcendentals=0),
    )(*args)


def dft_tables(length):
    index = np.arange(length)
    angle = (index[:, None] * index[None, :] % length) * (2.0 * math.pi / length)
    cos, sin = np.cos(angle) / math.sqrt(length), np.sin(angle) / math.sqrt(length)
    right = np.block([[cos, -sin], [sin, cos]])
    tables = []
    for table in (right, right.T):
        high = table.astype(BF16)
        tables += [high, (table - high.astype(np.float64)).astype(BF16)]
    return jnp.asarray(np.stack(tables))


def split(x):
    high = x.astype(BF16)
    return high, (x - high.astype(F32)).astype(BF16)


def dot3(a_high, a_low, b_high, b_low):
    dot = functools.partial(jnp.dot, preferred_element_type=F32)
    return dot(a_high, b_high) + (dot(a_low, b_high) + dot(a_high, b_low))


def lanes(rows, size):
    return lax.broadcasted_iota(jnp.int32, (rows, size), 1)


def turn(x):
    return pltpu.roll(x, x.shape[-1] // 2, 1)


def beam_of(meta, which, slot, scans, beams):
    beam = jnp.int32(0)
    for index in range(1, beams):
        beam = jnp.where(meta[0, 2 * scans + 2 + slot * beams + index] == which, index, beam)
    return beam


def place(meta, slot, size):
    y, x = meta[0, 2 * slot], meta[0, 2 * slot + 1]
    return y, x // size, x % size


def edge_kernel(obj, positions, counts, offsets, place_of, edge_l, edge_r, meta):
    scans = positions.shape[2]
    values = [positions[0, 0, slot, axis] for slot in range(scans) for axis in range(2)]
    values += [counts[0, 0], place_of[0]]
    values += [offsets[slot, beam] for slot in range(scans) for beam in range(offsets.shape[1])]
    assert len(values) <= meta.shape[1]
    lane = lax.broadcasted_iota(jnp.int32, meta.shape, 1)
    row = jnp.zeros(meta.shape, jnp.int32)
    for at, value in enumerate(values):
        row = jnp.where(lane == at, value, row)
    meta[...] = row
    _, rows, columns = obj.shape
    size = edge_l.shape[1]
    low = lanes(rows, size) < size // 2
    near, far = slice(0, size), slice(columns - size, columns)
    edge_l[...] = jnp.where(low, obj[0, :, near], turn(obj[1, :, near]))
    edge_r[...] = jnp.where(low, turn(obj[0, :, far]), obj[1, :, far])


def frame_kernel(obj, top, bot, left, right, out):
    tiles, rows, size = out.shape[1:]
    half = size // 2
    low = lanes(half, size) < half
    for at in range(0, rows, half):
        body, src = obj, pl.ds(at - half, half)
        if at == 0:
            body, src = top, pl.ds(0, half)
        elif at == rows - half:
            body, src = bot, pl.ds(0, half)
        here = pl.ds(at, half)
        for ch in range(2):
            parts = [turn(body[ch, src, t * size : (t + 1) * size]) for t in range(tiles - 1)]
            edge_l, edge_r = left[here, :], right[here, :]
            edge_l = edge_l if ch == 0 else turn(edge_l)
            edge_r = turn(edge_r) if ch == 0 else edge_r
            parts = [edge_l, *parts, edge_r]
            for t in range(tiles):
                out[ch, t, here, :] = jnp.where(low, parts[t], parts[t + 1])


def forward_kernel(parts, scans, adds, *refs):
    meta, frame, probe, tables = refs[:4]
    refs = refs[4:]
    if adds:
        arrived, refs = refs[0], refs[1:]
    outs, (x_high, x_low, y_high, y_low) = refs[:-4], refs[-4:]
    size = probe.shape[-1]
    lane = lanes(size, size)
    for at, (which, start, slots) in enumerate(parts):
        far, wave, power = outs[3 * at : 3 * at + 3]
        for index in range(slots):
            slot = start + index
            y, tile, shift = place(meta, slot, size)
            beam = beam_of(meta, which, slot, scans, probe.shape[0])
            back = lax.rem(size - shift, size)
            patch = []
            for ch in range(2):
                near = pltpu.roll(frame[ch, tile, pl.ds(y, size), :], back, 1)
                rest = pltpu.roll(frame[ch, tile + 1, pl.ds(y, size), :], back, 1)
                patch.append(jnp.where(lane < size - shift, near, rest))
            probe_re, probe_im = probe[beam, 0], probe[beam, 1]
            waves = (
                probe_re * patch[0] - probe_im * patch[1],
                probe_re * patch[1] + probe_im * patch[0],
            )
            rows = slice(index * size, (index + 1) * size)
            for ch in range(2):
                wave[index, ch] = waves[ch]
                columns = slice(ch * size, (ch + 1) * size)
                x_high[rows, columns], x_low[rows, columns] = split(waves[ch])
        for slot in range(0, slots, 2):
            rows = slice(slot * size, (slot + 2) * size)
            mid = dot3(x_high[rows, :], x_low[rows, :], tables[0], tables[1])
            for sub in range(2):
                columns = slice((slot + sub) * size, (slot + sub + 1) * size)
                for ch in range(2):
                    piece = mid[sub * size : (sub + 1) * size, ch * size : (ch + 1) * size]
                    into = slice(ch * size, (ch + 1) * size)
                    y_high[into, columns], y_low[into, columns] = split(piece)
            columns = slice(slot * size, (slot + 2) * size)
            result = dot3(tables[2], tables[3], y_high[:, columns], y_low[:, columns])
            far[:, columns] = result
            for sub in range(2):
                inside = slice(sub * size, (sub + 1) * size)
                re, im = result[:size, inside], result[size:, inside]
                rows = slice((slot + sub) * size, (slot + sub + 1) * size)
                own = re * re + im * im
                power[rows, :] = own + arrived[rows, :] if adds else own
        if power.shape[0] > slots * size:
            lane = lanes(power.shape[0] - slots * size, size)
            row = jnp.zeros(lane.shape, jnp.int32)
            for index in range(2 * scans + 2 + scans * probe.shape[0]):
                row = jnp.where(lane == index, meta[0, index], row)
            power[slots * size :, :] = row.astype(F32)


def factor_kernel(arrived, own, measured, *refs):
    out = refs[-1]
    count = own.shape[0]
    total = own[...] + arrived[:count, :]
    out[:count, :] = measured[...] / jnp.sqrt(total + EPSILON)
    if len(refs) > 1:
        out[count:, :] = refs[0][...]


def add_patch(total, channel, y, tile, shift, value, lane):
    moved = pltpu.roll(value, shift, 1)
    rows = pl.ds(y, value.shape[0])
    total[channel, tile, rows, :] += jnp.where(lane >= shift, moved, 0.0)
    total[channel, tile + 1, rows, :] += jnp.where(lane < shift, moved, 0.0)


def write_sides(total, side_l, side_r):
    _, tiles, rows, size = total.shape
    low = lanes(rows, size) < size // 2
    side_l[...] = jnp.where(low, total[0, 0], turn(total[1, 0]))
    side_r[...] = jnp.where(low, turn(total[0, tiles - 1]), total[1, tiles - 1])


def own_columns(total, channel, rows, low):
    tiles = total.shape[1]
    turned = [turn(total[channel, t, rows, :]) for t in range(tiles)]
    return [jnp.where(low, turned[t], turned[t + 1]) for t in range(tiles - 1)]


def write_rims(total, rim_top, rim_bot):
    channels, _, rows, size = total.shape
    half = size // 2
    low = lanes(half, size) < half
    for ch in range(channels):
        for start, out in ((0, rim_top), (rows - half, rim_bot)):
            for t, value in enumerate(own_columns(total, ch, pl.ds(start, half), low)):
                out[ch, :, t * size : (t + 1) * size] = value


def backward_kernel(parts, scans, fresh, last, *refs):
    meta, probe, tables = refs[:3]
    inputs, refs = refs[3 : 3 + 3 * len(parts)], refs[3 + 3 * len(parts) :]
    if not fresh:
        refs = refs[1:]
    total, refs = refs[0], refs[1:]
    if last:
        (side_l, side_r, rim_top, rim_bot), refs = refs[:4], refs[4:]
    x_high, x_low, y_high, y_low = refs
    size = probe.shape[-1]
    lane = lanes(size, size)
    if fresh:
        total[...] = jnp.zeros_like(total)
    for at, (which, start, slots) in enumerate(parts):
        far, wave, factor = inputs[3 * at : 3 * at + 3]
        for slot in range(0, slots, 2):
            for sub in range(2):
                columns = slice((slot + sub) * size, (slot + sub + 1) * size)
                scale = factor[(slot + sub) * size : (slot + sub + 1) * size, :]
                for ch in range(2):
                    into = slice(ch * size, (ch + 1) * size)
                    y_high[into, columns], y_low[into, columns] = split(far[into, columns] * scale)
            columns = slice(slot * size, (slot + 2) * size)
            mid = dot3(tables[0], tables[1], y_high[:, columns], y_low[:, columns])
            for sub in range(2):
                rows = slice((slot + sub) * size, (slot + sub + 1) * size)
                for ch in range(2):
                    piece = mid[ch * size : (ch + 1) * size, sub * size : (sub + 1) * size]
                    into = slice(ch * size, (ch + 1) * size)
                    x_high[rows, into], x_low[rows, into] = split(piece)
            rows = slice(slot * size, (slot + 2) * size)
            result = dot3(x_high[rows, :], x_low[rows, :], tables[2], tables[3])
            for sub in range(2):
                true_slot = start + slot + sub
                live = (true_slot < meta[0, 2 * scans]).astype(F32)
                beam = beam_of(meta, which, true_slot, scans, probe.shape[0])
                probe_re, probe_im = probe[beam, 0], probe[beam, 1]
                inside = slice(sub * size, (sub + 1) * size)
                change_re = (result[inside, :size] - wave[slot + sub, 0]) * live
                change_im = (result[inside, size:] - wave[slot + sub, 1]) * live
                grad_re = probe_re * change_re + probe_im * change_im
                grad_im = probe_re * change_im - probe_im * change_re
                spot = place(meta, true_slot, size)
                add_patch(total, 0, *spot, grad_re, lane)
                add_patch(total, 1, *spot, grad_im, lane)
    if last:
        write_sides(total, side_l, side_r)
        write_rims(total, rim_top, rim_bot)


def weight_kernel(steps, scans, which_tile, row_count, fresh, *refs):
    metas, probe, total = refs[0], refs[1], refs[-1]
    _, tiles, rows, size = total.shape
    half = size // 2
    own_rows, own_columns = rows - 2 * size, (tiles - 2) * size
    lane = lanes(size, size)
    if fresh:
        total[...] = jnp.zeros_like(total)
    at_row = lax.rem(metas[0, 2 * scans + 1] + which_tile + row_count, row_count)
    for row, across in enumerate((0, -1, 1)):
        for down, which in steps:

            def add(slot, carry, row=row, across=across, down=down, which=which):
                y = metas[row, 2 * slot] + (down * own_rows + half)
                x = metas[row, 2 * slot + 1] + (across * own_columns + half)
                near = (y > 0) & (y < rows - size) & (x > 0) & (x < (tiles - 1) * size)
                below = at_row + down
                live = (slot < metas[row, 2 * scans]) & (below >= 0) & (below < row_count)

                @pl.when(near & live)
                def _():
                    beam = beam_of(metas, which, slot, scans, probe.shape[0])
                    probe_re, probe_im = probe[beam, 0], probe[beam, 1]
                    value = probe_re * probe_re + probe_im * probe_im
                    add_patch(total, 0, y, x // size, x % size, value, lane)

                return carry

            lax.fori_loop(0, scans, add, 0)


def gathered(total, side_l, side_r, in_top, in_bot, in_ctop, in_cbot, channel, chunk, half):
    _, tiles, rows, size = total.shape
    chunks = (rows - size) // half
    low = lanes(half, size) < half
    ext = pl.ds((chunk + 1) * half, half)
    values = own_columns(total, channel, ext, low)

    def add_sides(from_l, from_r):
        from_l = from_l if channel == 0 else turn(from_l)
        from_r = turn(from_r) if channel == 0 else from_r
        values[0] += jnp.where(low, from_l, 0.0)
        values[-1] += jnp.where(low, 0.0, from_r)

    add_sides(side_l[ext, :], side_r[ext, :])
    for at, rim, corner in ((0, in_top, in_ctop), (chunks - 1, in_bot, in_cbot)):
        if chunk == at:
            for t in range(tiles - 1):
                values[t] += rim[channel, :, t * size : (t + 1) * size]
            add_sides(corner[0], corner[1])
    return values


def final_kernel(*refs):
    obj, weight, out = refs[0], refs[1], refs[-1]
    grads = refs[2:9]
    size = grads[0].shape[-1]
    half = size // 2
    tiles = obj.shape[2] // size
    for chunk in range(obj.shape[1] // half):
        wide = pl.ds(size + chunk * half, half)
        scale = [1.0 / (weight[0, t + 1, wide, :] + DAMPING) for t in range(tiles)]
        rows = slice(chunk * half, (chunk + 1) * half)
        for ch in range(2):
            for t, value in enumerate(gathered(*grads, ch, chunk, half)):
                columns = slice(t * size, (t + 1) * size)
                out[ch, rows, columns] = obj[ch, rows, columns] + value * scale[t]


def line(axis, by):
    count = lax.axis_size(axis)
    return [(i, i + by) for i in range(count) if 0 <= i + by < count]


def ring(axis, by):
    count = lax.axis_size(axis)
    return [(i, (i + by) % count) for i in range(count)]


def move(x, axis, pairs):
    return lax.ppermute(x, axis, pairs)


def send_rims(side_l, side_r, rim_top, rim_bot):
    rows, size = side_l.shape
    half = size // 2
    in_r = move(side_l, "col", line("col", -1))
    in_l = move(side_r, "col", line("col", 1))
    in_bot = move(rim_top, "row", line("row", -1))
    in_top = move(rim_bot, "row", line("row", 1))
    corner_top = jnp.stack([in_l[:half], in_r[:half]])
    corner_bot = jnp.stack([in_l[rows - half :], in_r[rows - half :]])
    in_cbot = move(corner_top, "row", line("row", -1))
    in_ctop = move(corner_bot, "row", line("row", 1))
    return in_l, in_r, in_top, in_bot, in_ctop, in_cbot


def on_device(obj, probe, positions, counts, offsets, measured):
    offsets_count, _, size, _ = probe.shape
    scans = positions.shape[2]
    half = size // 2
    tile_rows, tile_columns = obj.shape[1:]
    rows, tiles = tile_rows + size, tile_columns // size + 1
    row_count = lax.axis_size("row")
    tables = dft_tables(size)

    def packed(x):
        return jnp.concatenate([x[0], x[1]], axis=1)

    edge_l, edge_r, meta = call(
        edge_kernel,
        [(tile_rows, size)] * 2 + [jax.ShapeDtypeStruct((1, size), jnp.int32)],
        [VMEM, SMEM, SMEM, SMEM, SMEM],
        (obj, positions, counts, offsets, lax.axis_index("row").astype(jnp.int32).reshape(1)),
        10**6,
    )
    top = move(obj[:, tile_rows - half :], "row", line("row", 1))
    bot = move(obj[:, :half], "row", line("row", -1))

    most = offsets_count - 1
    metas = {0: meta, most: move(meta, "row", ring("row", most))}

    own_meta = jnp.broadcast_to(meta.astype(F32), (8, size))
    edge_l, edge_r = (
        jnp.concatenate([packed(top[:, :, part]), edge, packed(bot[:, :, part]), own_meta])
        for part, edge in ((slice(0, half), edge_l), (slice(tile_columns - half, None), edge_r))
    )
    left = move(edge_r, "col", line("col", 1))
    right = move(edge_l, "col", line("col", -1))
    (frame,) = call(frame_kernel, [(2, tiles, rows, size)], [VMEM] * 5, (obj, top, bot, left, right), 10**6)

    slots = scans // 2
    halves = ((0, slots), (slots, scans - slots))
    work = [
        pltpu.VMEM((slots * size, 2 * size), BF16),
        pltpu.VMEM((slots * size, 2 * size), BF16),
        pltpu.VMEM((2 * size, slots * size), BF16),
        pltpu.VMEM((2 * size, slots * size), BF16),
    ]
    flops = slots * 2 * 3 * 2 * size * (2 * size) ** 2

    far, wave, power = {}, {}, {}

    def forward(which, parts, arrived=None):
        outs = []
        for start, count in parts:
            tail = 8 if which and start == 0 else 0
            outs += [(2 * size, count * size), (count, 2, size, size), (count * size + tail, size)]
        adds = arrived is not None
        results = call(
            functools.partial(forward_kernel, [(which, *part) for part in parts], scans, adds),
            outs,
            [SMEM, VMEM, VMEM, VMEM] + [VMEM] * adds,
            (metas[which], frame, probe, tables) + ((arrived,) if adds else ()),
            flops * len(parts),
            work,
        )
        for at, (start, _) in enumerate(parts):
            far[which, start], wave[which, start], power[which, start] = results[3 * at : 3 * at + 3]

    forward(most, [halves[0]])
    forward(most, [halves[1]])
    forward(0, list(halves))
    for which in reversed(range(most)):
        for start, count in halves:
            arrived = move(power[which + 1, start], "row", ring("row", -1))
            if which:
                if start == 0:
                    metas[which] = arrived[count * size : count * size + 1].astype(jnp.int32)
                forward(which, [(start, count)], arrived)
            else:
                power[1, start] = arrived
    beside = jnp.concatenate([left[rows : rows + 1], right[rows : rows + 1], jnp.zeros((6, size), F32)])
    factors = {}
    for start, count in halves:
        args = [power[1, start], power[0, start], measured[0, 0, start : start + count].reshape(-1, size)]
        args += [beside] if start == 0 else []
        height = count * size + (beside.shape[0] if start == 0 else 0)
        (factors[start],) = call(factor_kernel, [(height, size)], [VMEM] * len(args), args, 10**6)

    row_count = lax.axis_size("row")
    kept = min(row_count, offsets_count + 2)
    weight = None

    def add_weight(index, shift, beside):
        nonlocal weight
        own = metas[shift] if shift in metas else None
        if own is None:
            span = move(jnp.concatenate([meta.astype(F32), beside[:2]]), "row", ring("row", shift))
            span = span.astype(jnp.int32)
        else:
            span = jnp.concatenate([own, beside[:2].astype(jnp.int32)])
        steps = [(d, w) for d in (-1, 0, 1) for w in range(offsets_count) if (w - d) % kept == index]
        (weight,) = call(
            functools.partial(weight_kernel, steps, scans, shift, row_count, weight is None),
            [(1, tiles + 1, tile_rows + 2 * size, size)],
            [SMEM, VMEM] + ([] if weight is None else [VMEM]),
            (span, probe) + (() if weight is None else (weight,)),
            flops,
            aliases={} if weight is None else {2: 0},
        )

    for index in range(offsets_count, kept):
        add_weight(index, index if index <= offsets_count else index - kept, beside)

    total = None
    for which in range(offsets_count):
        if which:
            for start, _ in halves:
                value = move(factors[start], "row", ring("row", 1))
                if start == 0 and which < most:
                    value, total = lax.optimization_barrier((value, total))
                factors[start] = value
            add_weight(which, which, factors[0][slots * size :])
        else:
            add_weight(0, 0, beside)
        groups = [[part] for part in halves] if which == most else [list(halves)]
        for group in groups:
            fresh, last = total is None, which == most and group[-1] == halves[-1]
            outs = [(2, tiles, rows, size)]
            if last:
                outs += [(rows, size)] * 2 + [(2, half, tile_columns)] * 2
            args = [metas[which], probe, tables]
            for start, _ in group:
                args += [far[which, start], wave[which, start], factors[start]]
            specs = [SMEM] + [VMEM] * (len(args) - 1)
            if not fresh:
                args, specs = args + [total], specs + [VMEM]
            total, *sides = call(
                functools.partial(backward_kernel, [(which, *part) for part in group], scans, fresh, last),
                outs,
                specs,
                args,
                flops * len(group),
                work,
                {} if fresh else {len(args) - 1: 0},
            )
    grad_in = send_rims(*sides)

    (new_object,) = call(final_kernel, [obj.shape], [VMEM] * 9, (obj, weight, total, *grad_in), 10**6)
    return new_object


def solution(mesh):
    return jax.shard_map(
        on_device,
        mesh=mesh,
        in_specs=(
            P(None, "row", "col"),
            P(),
            P("row", "col", None, None),
            P("row", "col"),
            P(),
            P("row", "col", None, None, None),
        ),
        out_specs=P(None, "row", "col"),
        check_vma=False,
    )
```

```python
import functools
import math

import jax
import jax.numpy as jnp
import numpy as np
from jax import lax
from jax.experimental import pallas as pl
from jax.experimental.pallas import tpu as pltpu
from jax.sharding import PartitionSpec as P

EPSILON = 0.5
DAMPING = 0.5


SMEM = pl.BlockSpec(memory_space=pltpu.SMEM)
VMEM = pl.BlockSpec(memory_space=pltpu.VMEM)
F32 = jnp.float32
BF16 = jnp.bfloat16


def call(kernel, outs, specs, args, flops, scratch=(), aliases=None):
    return pl.pallas_call(
        kernel,
        out_shape=[s if hasattr(s, "dtype") else jax.ShapeDtypeStruct(s, F32) for s in outs],
        in_specs=specs,
        out_specs=[VMEM] * len(outs),
        scratch_shapes=list(scratch),
        input_output_aliases=aliases or {},
        compiler_params=pltpu.CompilerParams(vmem_limit_bytes=16 * 2**20),
        cost_estimate=pl.CostEstimate(flops=flops, bytes_accessed=2**20, transcendentals=0),
    )(*args)


def dft_tables(length):
    index = np.arange(length)
    angle = (index[:, None] * index[None, :] % length) * (2.0 * math.pi / length)
    cos, sin = np.cos(angle) / math.sqrt(length), np.sin(angle) / math.sqrt(length)
    right = np.block([[cos, -sin], [sin, cos]])
    tables = []
    for table in (right, right.T):
        high = table.astype(BF16)
        tables += [high, (table - high.astype(np.float64)).astype(BF16)]
    return jnp.asarray(np.stack(tables))


def split(x):
    high = x.astype(BF16)
    return high, (x - high.astype(F32)).astype(BF16)


def dot3(a_high, a_low, b_high, b_low):
    dot = functools.partial(jnp.dot, preferred_element_type=F32)
    return dot(a_high, b_high) + (dot(a_low, b_high) + dot(a_high, b_low))


def lanes(rows, size):
    return lax.broadcasted_iota(jnp.int32, (rows, size), 1)


def turn(x):
    return pltpu.roll(x, x.shape[-1] // 2, 1)


def beam_of(meta, which, slot, scans, beams):
    beam = jnp.int32(0)
    for index in range(1, beams):
        beam = jnp.where(meta[0, 2 * scans + 3 + slot * beams + index] == which, index, beam)
    return beam


def place(meta, slot, size):
    y, x = meta[0, 2 * slot], meta[0, 2 * slot + 1]
    return y, x // size, x % size


def edge_kernel(obj, positions, counts, offsets, place_of, edge_l, edge_r, meta):
    scans = positions.shape[2]
    values = [positions[0, 0, slot, axis] for slot in range(scans) for axis in range(2)]
    values += [counts[0, 0], place_of[0], place_of[1]]
    values += [offsets[slot, beam] for slot in range(scans) for beam in range(offsets.shape[1])]
    assert len(values) <= meta.shape[1]
    lane = lax.broadcasted_iota(jnp.int32, meta.shape, 1)
    row = jnp.zeros(meta.shape, jnp.int32)
    for at, value in enumerate(values):
        row = jnp.where(lane == at, value, row)
    meta[...] = row
    _, rows, columns = obj.shape
    size = edge_l.shape[1]
    low = lanes(rows, size) < size // 2
    near, far = slice(0, size), slice(columns - size, columns)
    edge_l[...] = jnp.where(low, obj[0, :, near], turn(obj[1, :, near]))
    edge_r[...] = jnp.where(low, turn(obj[0, :, far]), obj[1, :, far])


def frame_kernel(obj, top, bot, left, right, out):
    tiles, rows, size = out.shape[1:]
    half = size // 2
    low = lanes(half, size) < half
    for at in range(0, rows, half):
        body, src = obj, pl.ds(at - half, half)
        if at == 0:
            body, src = top, pl.ds(0, half)
        elif at == rows - half:
            body, src = bot, pl.ds(0, half)
        here = pl.ds(at, half)
        for ch in range(2):
            parts = [turn(body[ch, src, t * size : (t + 1) * size]) for t in range(tiles - 1)]
            edge_l, edge_r = left[here, :], right[here, :]
            edge_l = edge_l if ch == 0 else turn(edge_l)
            edge_r = turn(edge_r) if ch == 0 else edge_r
            parts = [edge_l, *parts, edge_r]
            for t in range(tiles):
                out[ch, t, here, :] = jnp.where(low, parts[t], parts[t + 1])


def forward_kernel(parts, scans, adds, *refs):
    meta, frame, probe, tables = refs[:4]
    refs = refs[4:]
    if adds:
        arrived, refs = refs[0], refs[1:]
    outs, (x_high, x_low, y_high, y_low) = refs[:-4], refs[-4:]
    size = probe.shape[-1]
    lane = lanes(size, size)
    for at, (which, start, slots) in enumerate(parts):
        far, wave, power = outs[3 * at : 3 * at + 3]
        for index in range(slots):
            slot = start + index
            y, tile, shift = place(meta, slot, size)
            beam = beam_of(meta, which, slot, scans, probe.shape[0])
            back = lax.rem(size - shift, size)
            patch = []
            for ch in range(2):
                near = pltpu.roll(frame[ch, tile, pl.ds(y, size), :], back, 1)
                rest = pltpu.roll(frame[ch, tile + 1, pl.ds(y, size), :], back, 1)
                patch.append(jnp.where(lane < size - shift, near, rest))
            probe_re, probe_im = probe[beam, 0], probe[beam, 1]
            waves = (
                probe_re * patch[0] - probe_im * patch[1],
                probe_re * patch[1] + probe_im * patch[0],
            )
            rows = slice(index * size, (index + 1) * size)
            for ch in range(2):
                wave[index, ch] = waves[ch]
                columns = slice(ch * size, (ch + 1) * size)
                x_high[rows, columns], x_low[rows, columns] = split(waves[ch])
        for slot in range(0, slots, 2):
            rows = slice(slot * size, (slot + 2) * size)
            mid = dot3(x_high[rows, :], x_low[rows, :], tables[0], tables[1])
            for sub in range(2):
                columns = slice((slot + sub) * size, (slot + sub + 1) * size)
                for ch in range(2):
                    piece = mid[sub * size : (sub + 1) * size, ch * size : (ch + 1) * size]
                    into = slice(ch * size, (ch + 1) * size)
                    y_high[into, columns], y_low[into, columns] = split(piece)
            columns = slice(slot * size, (slot + 2) * size)
            result = dot3(tables[2], tables[3], y_high[:, columns], y_low[:, columns])
            far[:, columns] = result
            for sub in range(2):
                inside = slice(sub * size, (sub + 1) * size)
                re, im = result[:size, inside], result[size:, inside]
                rows = slice((slot + sub) * size, (slot + sub + 1) * size)
                own = re * re + im * im
                power[rows, :] = own + arrived[rows, :] if adds else own
        if power.shape[0] > slots * size:
            lane = lanes(power.shape[0] - slots * size, size)
            row = jnp.zeros(lane.shape, jnp.int32)
            for index in range(2 * scans + 3 + scans * probe.shape[0]):
                row = jnp.where(lane == index, meta[0, index], row)
            power[slots * size :, :] = row.astype(F32)


def factor_kernel(arrived, own, measured, *refs):
    out = refs[-1]
    count = own.shape[0]
    total = own[...] + arrived[:count, :]
    out[:count, :] = measured[...] / jnp.sqrt(total + EPSILON)
    if len(refs) > 1:
        out[count:, :] = refs[0][...]


def add_patch(total, channel, y, tile, shift, value, lane):
    moved = pltpu.roll(value, shift, 1)
    rows = pl.ds(y, value.shape[0])
    total[channel, tile, rows, :] += jnp.where(lane >= shift, moved, 0.0)
    total[channel, tile + 1, rows, :] += jnp.where(lane < shift, moved, 0.0)


def write_sides(total, odd, side_1, side_2):
    _, tiles, rows, size = total.shape
    low = lanes(rows, size) < size // 2
    left = jnp.where(low, total[0, 0], turn(total[1, 0]))
    right = jnp.where(low, turn(total[0, tiles - 1]), total[1, tiles - 1])
    side_1[...] = jnp.where(odd == 1, left, right)
    side_2[...] = jnp.where(odd == 1, right, left)


def own_columns(total, channel, rows, low):
    tiles = total.shape[1]
    turned = [turn(total[channel, t, rows, :]) for t in range(tiles)]
    return [jnp.where(low, turned[t], turned[t + 1]) for t in range(tiles - 1)]


def write_rims(total, odd, rim_1, rim_2):
    channels, _, rows, size = total.shape
    half = size // 2
    low = lanes(half, size) < half
    for ch in range(channels):
        tops = own_columns(total, ch, pl.ds(0, half), low)
        bottoms = own_columns(total, ch, pl.ds(rows - half, half), low)
        for t, (top, bottom) in enumerate(zip(tops, bottoms)):
            columns = slice(t * size, (t + 1) * size)
            rim_1[ch, :, columns] = jnp.where(odd == 1, top, bottom)
            rim_2[ch, :, columns] = jnp.where(odd == 1, bottom, top)


def backward_kernel(parts, scans, row_count, fresh, last, *refs):
    meta, probe, tables = refs[:3]
    inputs, refs = refs[3 : 3 + 3 * len(parts)], refs[3 + 3 * len(parts) :]
    if not fresh:
        refs = refs[1:]
    total, refs = refs[0], refs[1:]
    if last:
        (side_1, side_2, rim_1, rim_2), refs = refs[:4], refs[4:]
    x_high, x_low, y_high, y_low = refs
    size = probe.shape[-1]
    lane = lanes(size, size)
    if fresh:
        total[...] = jnp.zeros_like(total)
    for at, (which, start, slots) in enumerate(parts):
        far, wave, factor = inputs[3 * at : 3 * at + 3]
        for slot in range(0, slots, 2):
            for sub in range(2):
                columns = slice((slot + sub) * size, (slot + sub + 1) * size)
                scale = factor[(slot + sub) * size : (slot + sub + 1) * size, :]
                for ch in range(2):
                    into = slice(ch * size, (ch + 1) * size)
                    y_high[into, columns], y_low[into, columns] = split(far[into, columns] * scale)
            columns = slice(slot * size, (slot + 2) * size)
            mid = dot3(tables[0], tables[1], y_high[:, columns], y_low[:, columns])
            for sub in range(2):
                rows = slice((slot + sub) * size, (slot + sub + 1) * size)
                for ch in range(2):
                    piece = mid[ch * size : (ch + 1) * size, sub * size : (sub + 1) * size]
                    into = slice(ch * size, (ch + 1) * size)
                    x_high[rows, into], x_low[rows, into] = split(piece)
            rows = slice(slot * size, (slot + 2) * size)
            result = dot3(x_high[rows, :], x_low[rows, :], tables[2], tables[3])
            for sub in range(2):
                true_slot = start + slot + sub
                live = (true_slot < meta[0, 2 * scans]).astype(F32)
                beam = beam_of(meta, which, true_slot, scans, probe.shape[0])
                probe_re, probe_im = probe[beam, 0], probe[beam, 1]
                inside = slice(sub * size, (sub + 1) * size)
                change_re = (result[inside, :size] - wave[slot + sub, 0]) * live
                change_im = (result[inside, size:] - wave[slot + sub, 1]) * live
                grad_re = probe_re * change_re + probe_im * change_im
                grad_im = probe_re * change_im - probe_im * change_re
                spot = place(meta, true_slot, size)
                add_patch(total, 0, *spot, grad_re, lane)
                add_patch(total, 1, *spot, grad_im, lane)
    if last:
        odd = lax.rem(meta[0, 2 * scans + 2], 2)
        write_sides(total, odd, side_1, side_2)
        odd = lax.rem(lax.rem(meta[0, 2 * scans + 1] + parts[0][0], row_count), 2)
        write_rims(total, odd, rim_1, rim_2)


def weight_kernel(steps, scans, which_tile, row_count, fresh, *refs):
    metas, probe, total = refs[0], refs[1], refs[-1]
    _, tiles, rows, size = total.shape
    half = size // 2
    own_rows, own_columns = rows - 2 * size, (tiles - 2) * size
    lane = lanes(size, size)
    if fresh:
        total[...] = jnp.zeros_like(total)
    at_row = lax.rem(metas[0, 2 * scans + 1] + which_tile + row_count, row_count)
    for row, across in enumerate((0, -1, 1)):
        for down, which in steps:

            def add(slot, carry, row=row, across=across, down=down, which=which):
                y = metas[row, 2 * slot] + (down * own_rows + half)
                x = metas[row, 2 * slot + 1] + (across * own_columns + half)
                near = (y > 0) & (y < rows - size) & (x > 0) & (x < (tiles - 1) * size)
                below = at_row + down
                live = (slot < metas[row, 2 * scans]) & (below >= 0) & (below < row_count)

                @pl.when(near & live)
                def _():
                    beam = beam_of(metas, which, slot, scans, probe.shape[0])
                    probe_re, probe_im = probe[beam, 0], probe[beam, 1]
                    value = probe_re * probe_re + probe_im * probe_im
                    add_patch(total, 0, y, x // size, x % size, value, lane)

                return carry

            lax.fori_loop(0, scans, add, 0)


def gathered(total, side_l, side_r, in_top, in_bot, in_ctop, in_cbot, channel, chunk, half):
    _, tiles, rows, size = total.shape
    chunks = (rows - size) // half
    low = lanes(half, size) < half
    ext = pl.ds((chunk + 1) * half, half)
    values = own_columns(total, channel, ext, low)

    def add_sides(from_l, from_r):
        from_l = from_l if channel == 0 else turn(from_l)
        from_r = turn(from_r) if channel == 0 else from_r
        values[0] += jnp.where(low, from_l, 0.0)
        values[-1] += jnp.where(low, 0.0, from_r)

    add_sides(side_l[ext, :], side_r[ext, :])
    for at, rim, corner in ((0, in_top, in_ctop), (chunks - 1, in_bot, in_cbot)):
        if chunk == at:
            for t in range(tiles - 1):
                values[t] += rim[channel, :, t * size : (t + 1) * size]
            add_sides(corner[0], corner[1])
    return values


def final_kernel(*refs):
    obj, weight, out = refs[0], refs[1], refs[-1]
    grads = refs[2:9]
    size = grads[0].shape[-1]
    half = size // 2
    tiles = obj.shape[2] // size
    for chunk in range(obj.shape[1] // half):
        wide = pl.ds(size + chunk * half, half)
        scale = [1.0 / (weight[0, t + 1, wide, :] + DAMPING) for t in range(tiles)]
        rows = slice(chunk * half, (chunk + 1) * half)
        for ch in range(2):
            for t, value in enumerate(gathered(*grads, ch, chunk, half)):
                columns = slice(t * size, (t + 1) * size)
                out[ch, rows, columns] = obj[ch, rows, columns] + value * scale[t]


def swap(axis, first):
    lower = range(first, lax.axis_size(axis) - 1, 2)
    return [(i, i + 1) for i in lower] + [(i + 1, i) for i in lower]


def ring(axis, by):
    count = lax.axis_size(axis)
    return [(i, (i + by) % count) for i in range(count)]


def move(x, axis, pairs):
    return lax.ppermute(x, axis, pairs)


def send_rims(side_1, side_2, rim_1, rim_2, odd_row, odd_col):
    rows, size = side_1.shape
    half = size // 2
    in_2 = move(side_2, "col", swap("col", 1))
    in_1 = move(side_1, "col", swap("col", 0))
    rim_1 = move(rim_1, "row", swap("row", 0))
    rim_2 = move(rim_2, "row", swap("row", 1))
    in_l, in_r = jnp.where(odd_col, in_1, in_2), jnp.where(odd_col, in_2, in_1)
    tops = jnp.where(odd_col, jnp.stack([in_1[:half], in_2[:half]]), jnp.stack([in_2[:half], in_1[:half]]))
    low = rows - half
    bottoms = jnp.where(odd_col, jnp.stack([in_1[low:], in_2[low:]]), jnp.stack([in_2[low:], in_1[low:]]))
    corner_1 = move(jnp.where(odd_row, tops, bottoms), "row", swap("row", 0))
    corner_2 = move(jnp.where(odd_row, bottoms, tops), "row", swap("row", 1))
    in_top, in_bot = jnp.where(odd_row, rim_1, rim_2), jnp.where(odd_row, rim_2, rim_1)
    in_ctop, in_cbot = jnp.where(odd_row, corner_1, corner_2), jnp.where(odd_row, corner_2, corner_1)
    return in_l, in_r, in_top, in_bot, in_ctop, in_cbot


def on_device(obj, probe, positions, counts, offsets, measured):
    offsets_count, _, size, _ = probe.shape
    scans = positions.shape[2]
    half = size // 2
    tile_rows, tile_columns = obj.shape[1:]
    rows, tiles = tile_rows + size, tile_columns // size + 1
    row_count = lax.axis_size("row")
    tables = dft_tables(size)

    def packed(x):
        return jnp.concatenate([x[0], x[1]], axis=1)

    at_row, at_col = lax.axis_index("row").astype(jnp.int32), lax.axis_index("col").astype(jnp.int32)
    odd_row, odd_col = lax.rem(at_row, 2) == 1, lax.rem(at_col, 2) == 1
    ends = jnp.where(odd_row, 0, tile_rows - half), jnp.where(odd_row, tile_rows - half, 0)
    rows_1, rows_2 = (
        move(lax.dynamic_slice_in_dim(obj, ends[i], half, axis=1), "row", swap("row", i))
        for i in range(2)
    )
    top, bot = jnp.where(odd_row, rows_1, rows_2), jnp.where(odd_row, rows_2, rows_1)
    edge_l, edge_r, meta = call(
        edge_kernel,
        [(tile_rows, size)] * 2 + [jax.ShapeDtypeStruct((1, size), jnp.int32)],
        [VMEM, SMEM, SMEM, SMEM, SMEM],
        (obj, positions, counts, offsets, jnp.stack([at_row, at_col])),
        10**6,
    )

    most = offsets_count - 1
    metas = {0: meta, most: move(meta, "row", ring("row", most))}

    own_meta = jnp.broadcast_to(meta.astype(F32), (8, size))
    edge_l, edge_r = (
        jnp.concatenate([packed(top[:, :, part]), edge, packed(bot[:, :, part]), own_meta])
        for part, edge in ((slice(0, half), edge_l), (slice(tile_columns - half, None), edge_r))
    )
    columns_2 = move(jnp.where(odd_col, edge_r, edge_l), "col", swap("col", 1))
    columns_1 = move(jnp.where(odd_col, edge_l, edge_r), "col", swap("col", 0))
    left, right = jnp.where(odd_col, columns_1, columns_2), jnp.where(odd_col, columns_2, columns_1)
    (frame,) = call(frame_kernel, [(2, tiles, rows, size)], [VMEM] * 5, (obj, top, bot, left, right), 10**6)

    slots = scans // 2
    halves = ((0, slots), (slots, scans - slots))
    work = [
        pltpu.VMEM((slots * size, 2 * size), BF16),
        pltpu.VMEM((slots * size, 2 * size), BF16),
        pltpu.VMEM((2 * size, slots * size), BF16),
        pltpu.VMEM((2 * size, slots * size), BF16),
    ]
    flops = slots * 2 * 3 * 2 * size * (2 * size) ** 2

    far, wave, power = {}, {}, {}

    def forward(which, parts, arrived=None):
        outs = []
        for start, count in parts:
            tail = 8 if which and start == 0 else 0
            outs += [(2 * size, count * size), (count, 2, size, size), (count * size + tail, size)]
        adds = arrived is not None
        results = call(
            functools.partial(forward_kernel, [(which, *part) for part in parts], scans, adds),
            outs,
            [SMEM, VMEM, VMEM, VMEM] + [VMEM] * adds,
            (metas[which], frame, probe, tables) + ((arrived,) if adds else ()),
            flops * len(parts),
            work,
        )
        for at, (start, _) in enumerate(parts):
            far[which, start], wave[which, start], power[which, start] = results[3 * at : 3 * at + 3]

    forward(most, [halves[0]])
    forward(most, [halves[1]])
    forward(0, list(halves))
    for which in reversed(range(most)):
        for start, count in halves:
            arrived = move(power[which + 1, start], "row", ring("row", -1))
            if which:
                if start == 0:
                    metas[which] = arrived[count * size : count * size + 1].astype(jnp.int32)
                forward(which, [(start, count)], arrived)
            else:
                power[1, start] = arrived
    beside = jnp.concatenate([left[rows : rows + 1], right[rows : rows + 1], jnp.zeros((6, size), F32)])
    factors = {}
    for start, count in halves:
        args = [power[1, start], power[0, start], measured[0, 0, start : start + count].reshape(-1, size)]
        args += [beside] if start == 0 else []
        height = count * size + (beside.shape[0] if start == 0 else 0)
        (factors[start],) = call(factor_kernel, [(height, size)], [VMEM] * len(args), args, 10**6)

    row_count = lax.axis_size("row")
    kept = min(row_count, offsets_count + 2)
    weight = None

    def add_weight(index, shift, beside):
        nonlocal weight
        own = metas[shift] if shift in metas else None
        if own is None:
            span = move(jnp.concatenate([meta.astype(F32), beside[:2]]), "row", ring("row", shift))
            span = span.astype(jnp.int32)
        else:
            span = jnp.concatenate([own, beside[:2].astype(jnp.int32)])
        steps = [(d, w) for d in (-1, 0, 1) for w in range(offsets_count) if (w - d) % kept == index]
        (weight,) = call(
            functools.partial(weight_kernel, steps, scans, shift, row_count, weight is None),
            [(1, tiles + 1, tile_rows + 2 * size, size)],
            [SMEM, VMEM] + ([] if weight is None else [VMEM]),
            (span, probe) + (() if weight is None else (weight,)),
            flops,
            aliases={} if weight is None else {2: 0},
        )

    for index in range(offsets_count, kept):
        add_weight(index, index if index <= offsets_count else index - kept, beside)

    total = None
    for which in range(offsets_count):
        if which:
            for start, _ in halves:
                value = move(factors[start], "row", ring("row", 1))
                if start == 0 and which < most:
                    value, total = lax.optimization_barrier((value, total))
                factors[start] = value
            add_weight(which, which, factors[0][slots * size :])
        else:
            add_weight(0, 0, beside)
        groups = [[part] for part in halves] if which == most else [list(halves)]
        for group in groups:
            fresh, last = total is None, which == most and group[-1] == halves[-1]
            outs = [(2, tiles, rows, size)]
            if last:
                outs += [(rows, size)] * 2 + [(2, half, tile_columns)] * 2
            args = [metas[which], probe, tables]
            for start, _ in group:
                args += [far[which, start], wave[which, start], factors[start]]
            specs = [SMEM] + [VMEM] * (len(args) - 1)
            if not fresh:
                args, specs = args + [total], specs + [VMEM]
            total, *sides = call(
                functools.partial(backward_kernel, [(which, *part) for part in group], scans, row_count, fresh, last),
                outs,
                specs,
                args,
                flops * len(group),
                work,
                {} if fresh else {len(args) - 1: 0},
            )
    grad_in = send_rims(*sides, odd_row, odd_col)

    (new_object,) = call(final_kernel, [obj.shape], [VMEM] * 9, (obj, weight, total, *grad_in), 10**6)
    return new_object


def solution(mesh):
    return jax.shard_map(
        on_device,
        mesh=mesh,
        in_specs=(
            P(None, "row", "col"),
            P(),
            P("row", "col", None, None),
            P("row", "col"),
            P(),
            P("row", "col", None, None, None),
        ),
        out_specs=P(None, "row", "col"),
        check_vma=False,
    )
```

```python
import functools
import math

import jax
import jax.numpy as jnp
import numpy as np
from jax import lax
from jax.experimental import pallas as pl
from jax.experimental.pallas import tpu as pltpu
from jax.sharding import PartitionSpec as P

EPSILON = 0.5
DAMPING = 0.5


SMEM = pl.BlockSpec(memory_space=pltpu.SMEM)
VMEM = pl.BlockSpec(memory_space=pltpu.VMEM)
F32 = jnp.float32
BF16 = jnp.bfloat16


def call(kernel, outs, specs, args, flops, scratch=(), aliases=None):
    return pl.pallas_call(
        kernel,
        out_shape=[s if hasattr(s, "dtype") else jax.ShapeDtypeStruct(s, F32) for s in outs],
        in_specs=specs,
        out_specs=[VMEM] * len(outs),
        scratch_shapes=list(scratch),
        input_output_aliases=aliases or {},
        compiler_params=pltpu.CompilerParams(vmem_limit_bytes=16 * 2**20),
        cost_estimate=pl.CostEstimate(flops=flops, bytes_accessed=2**20, transcendentals=0),
    )(*args)


def dft_tables(length):
    index = np.arange(length)
    angle = (index[:, None] * index[None, :] % length) * (2.0 * math.pi / length)
    cos, sin = np.cos(angle) / math.sqrt(length), np.sin(angle) / math.sqrt(length)
    right = np.block([[cos, -sin], [sin, cos]])
    tables = []
    for table in (right, right.T):
        high = table.astype(BF16)
        tables += [high, (table - high.astype(np.float64)).astype(BF16)]
    return jnp.asarray(np.stack(tables))


def split(x):
    high = x.astype(BF16)
    return high, (x - high.astype(F32)).astype(BF16)


def dot3(a_high, a_low, b_high, b_low):
    dot = functools.partial(jnp.dot, preferred_element_type=F32)
    return dot(a_high, b_high) + (dot(a_low, b_high) + dot(a_high, b_low))


def lanes(rows, size):
    return lax.broadcasted_iota(jnp.int32, (rows, size), 1)


def turn(x):
    return pltpu.roll(x, x.shape[-1] // 2, 1)


def beam_of(meta, which, slot, scans, beams):
    beam = jnp.int32(0)
    for index in range(1, beams):
        beam = jnp.where(meta[0, 2 * scans + 3 + slot * beams + index] == which, index, beam)
    return beam


def place(meta, slot, size):
    y, x = meta[0, 2 * slot], meta[0, 2 * slot + 1]
    return y, x // size, x % size


def edge_kernel(obj, positions, counts, offsets, place_of, edge_l, edge_r, meta):
    scans = positions.shape[1]
    values = [positions[axis, slot] for slot in range(scans) for axis in range(2)]
    values += [counts[0, 0], place_of[0], place_of[1]]
    values += [offsets[beam, slot] for slot in range(scans) for beam in range(offsets.shape[0])]
    assert len(values) <= meta.shape[1]
    lane = lax.broadcasted_iota(jnp.int32, meta.shape, 1)
    row = jnp.zeros(meta.shape, jnp.int32)
    for at, value in enumerate(values):
        row = jnp.where(lane == at, value, row)
    meta[...] = row
    _, rows, columns = obj.shape
    size = edge_l.shape[1]
    low = lanes(rows, size) < size // 2
    near, far = slice(0, size), slice(columns - size, columns)
    edge_l[...] = jnp.where(low, obj[0, :, near], turn(obj[1, :, near]))
    edge_r[...] = jnp.where(low, turn(obj[0, :, far]), obj[1, :, far])


def frame_kernel(obj, top, bot, left, right, out):
    tiles, rows, size = out.shape[1:]
    half = size // 2
    low = lanes(half, size) < half
    for at in range(0, rows, half):
        body, src = obj, pl.ds(at - half, half)
        if at == 0:
            body, src = top, pl.ds(0, half)
        elif at == rows - half:
            body, src = bot, pl.ds(0, half)
        here = pl.ds(at, half)
        for ch in range(2):
            parts = [turn(body[ch, src, t * size : (t + 1) * size]) for t in range(tiles - 1)]
            edge_l, edge_r = left[here, :], right[here, :]
            edge_l = edge_l if ch == 0 else turn(edge_l)
            edge_r = turn(edge_r) if ch == 0 else edge_r
            parts = [edge_l, *parts, edge_r]
            for t in range(tiles):
                out[ch, t, here, :] = jnp.where(low, parts[t], parts[t + 1])


def forward_kernel(parts, scans, adds, *refs):
    meta, frame, probe, tables = refs[:4]
    refs = refs[4:]
    if adds:
        arrived, refs = refs[0], refs[1:]
    outs, (x_high, x_low, y_high, y_low) = refs[:-4], refs[-4:]
    size = probe.shape[-1]
    lane = lanes(size, size)
    for at, (which, start, slots) in enumerate(parts):
        far, wave, power = outs[3 * at : 3 * at + 3]
        for index in range(slots):
            slot = start + index
            y, tile, shift = place(meta, slot, size)
            beam = beam_of(meta, which, slot, scans, probe.shape[0])
            back = lax.rem(size - shift, size)
            patch = []
            for ch in range(2):
                near = pltpu.roll(frame[ch, tile, pl.ds(y, size), :], back, 1)
                rest = pltpu.roll(frame[ch, tile + 1, pl.ds(y, size), :], back, 1)
                patch.append(jnp.where(lane < size - shift, near, rest))
            probe_re, probe_im = probe[beam, 0], probe[beam, 1]
            waves = (
                probe_re * patch[0] - probe_im * patch[1],
                probe_re * patch[1] + probe_im * patch[0],
            )
            rows = slice(index * size, (index + 1) * size)
            for ch in range(2):
                wave[index, ch] = waves[ch]
                columns = slice(ch * size, (ch + 1) * size)
                x_high[rows, columns], x_low[rows, columns] = split(waves[ch])
        for slot in range(0, slots, 2):
            rows = slice(slot * size, (slot + 2) * size)
            mid = dot3(x_high[rows, :], x_low[rows, :], tables[0], tables[1])
            for sub in range(2):
                columns = slice((slot + sub) * size, (slot + sub + 1) * size)
                for ch in range(2):
                    piece = mid[sub * size : (sub + 1) * size, ch * size : (ch + 1) * size]
                    into = slice(ch * size, (ch + 1) * size)
                    y_high[into, columns], y_low[into, columns] = split(piece)
            columns = slice(slot * size, (slot + 2) * size)
            result = dot3(tables[2], tables[3], y_high[:, columns], y_low[:, columns])
            far[:, columns] = result
            for sub in range(2):
                inside = slice(sub * size, (sub + 1) * size)
                re, im = result[:size, inside], result[size:, inside]
                rows = slice((slot + sub) * size, (slot + sub + 1) * size)
                own = re * re + im * im
                power[rows, :] = own + arrived[rows, :] if adds else own
        if power.shape[0] > slots * size:
            lane = lanes(power.shape[0] - slots * size, size)
            row = jnp.zeros(lane.shape, jnp.int32)
            for index in range(2 * scans + 3 + scans * probe.shape[0]):
                row = jnp.where(lane == index, meta[0, index], row)
            power[slots * size :, :] = row.astype(F32)


def factor_kernel(arrived, own, measured, *refs):
    out = refs[-1]
    count = own.shape[0]
    total = own[...] + arrived[:count, :]
    out[:count, :] = measured[...] / jnp.sqrt(total + EPSILON)
    if len(refs) > 1:
        out[count:, :] = refs[0][...]


def add_patch(total, channel, y, tile, shift, value, lane):
    moved = pltpu.roll(value, shift, 1)
    rows = pl.ds(y, value.shape[0])
    total[channel, tile, rows, :] += jnp.where(lane >= shift, moved, 0.0)
    total[channel, tile + 1, rows, :] += jnp.where(lane < shift, moved, 0.0)


def write_sides(total, odd, side_1, side_2):
    _, tiles, rows, size = total.shape
    low = lanes(rows, size) < size // 2
    left = jnp.where(low, total[0, 0], turn(total[1, 0]))
    right = jnp.where(low, turn(total[0, tiles - 1]), total[1, tiles - 1])
    side_1[...] = jnp.where(odd == 1, left, right)
    side_2[...] = jnp.where(odd == 1, right, left)


def own_columns(total, channel, rows, low):
    tiles = total.shape[1]
    turned = [turn(total[channel, t, rows, :]) for t in range(tiles)]
    return [jnp.where(low, turned[t], turned[t + 1]) for t in range(tiles - 1)]


def write_rims(total, odd, rim_1, rim_2):
    channels, _, rows, size = total.shape
    half = size // 2
    low = lanes(half, size) < half
    for ch in range(channels):
        tops = own_columns(total, ch, pl.ds(0, half), low)
        bottoms = own_columns(total, ch, pl.ds(rows - half, half), low)
        for t, (top, bottom) in enumerate(zip(tops, bottoms)):
            columns = slice(t * size, (t + 1) * size)
            rim_1[ch, :, columns] = jnp.where(odd == 1, top, bottom)
            rim_2[ch, :, columns] = jnp.where(odd == 1, bottom, top)


def backward_kernel(parts, scans, row_count, fresh, last, *refs):
    meta, probe, tables = refs[:3]
    inputs, refs = refs[3 : 3 + 3 * len(parts)], refs[3 + 3 * len(parts) :]
    if not fresh:
        refs = refs[1:]
    total, refs = refs[0], refs[1:]
    if last:
        (side_1, side_2, rim_1, rim_2), refs = refs[:4], refs[4:]
    x_high, x_low, y_high, y_low = refs
    size = probe.shape[-1]
    lane = lanes(size, size)
    if fresh:
        total[...] = jnp.zeros_like(total)
    for at, (which, start, slots) in enumerate(parts):
        far, wave, factor = inputs[3 * at : 3 * at + 3]
        for slot in range(0, slots, 2):
            for sub in range(2):
                columns = slice((slot + sub) * size, (slot + sub + 1) * size)
                scale = factor[(slot + sub) * size : (slot + sub + 1) * size, :]
                for ch in range(2):
                    into = slice(ch * size, (ch + 1) * size)
                    y_high[into, columns], y_low[into, columns] = split(far[into, columns] * scale)
            columns = slice(slot * size, (slot + 2) * size)
            mid = dot3(tables[0], tables[1], y_high[:, columns], y_low[:, columns])
            for sub in range(2):
                rows = slice((slot + sub) * size, (slot + sub + 1) * size)
                for ch in range(2):
                    piece = mid[ch * size : (ch + 1) * size, sub * size : (sub + 1) * size]
                    into = slice(ch * size, (ch + 1) * size)
                    x_high[rows, into], x_low[rows, into] = split(piece)
            rows = slice(slot * size, (slot + 2) * size)
            result = dot3(x_high[rows, :], x_low[rows, :], tables[2], tables[3])
            for sub in range(2):
                true_slot = start + slot + sub
                live = (true_slot < meta[0, 2 * scans]).astype(F32)
                beam = beam_of(meta, which, true_slot, scans, probe.shape[0])
                probe_re, probe_im = probe[beam, 0], probe[beam, 1]
                inside = slice(sub * size, (sub + 1) * size)
                change_re = (result[inside, :size] - wave[slot + sub, 0]) * live
                change_im = (result[inside, size:] - wave[slot + sub, 1]) * live
                grad_re = probe_re * change_re + probe_im * change_im
                grad_im = probe_re * change_im - probe_im * change_re
                spot = place(meta, true_slot, size)
                add_patch(total, 0, *spot, grad_re, lane)
                add_patch(total, 1, *spot, grad_im, lane)
    if last:
        odd = lax.rem(meta[0, 2 * scans + 2], 2)
        write_sides(total, odd, side_1, side_2)
        odd = lax.rem(lax.rem(meta[0, 2 * scans + 1] + parts[0][0], row_count), 2)
        write_rims(total, odd, rim_1, rim_2)


def weight_kernel(steps, scans, which_tile, row_count, fresh, *refs):
    metas, probe, total = refs[0], refs[1], refs[-1]
    _, tiles, rows, size = total.shape
    half = size // 2
    own_rows, own_columns = rows - 2 * size, (tiles - 2) * size
    lane = lanes(size, size)
    if fresh:
        total[...] = jnp.zeros_like(total)
    at_row = lax.rem(metas[0, 2 * scans + 1] + which_tile + row_count, row_count)
    for row, across in enumerate((0, -1, 1)):
        for down, which in steps:

            def add(slot, carry, row=row, across=across, down=down, which=which):
                y = metas[row, 2 * slot] + (down * own_rows + half)
                x = metas[row, 2 * slot + 1] + (across * own_columns + half)
                near = (y > 0) & (y < rows - size) & (x > 0) & (x < (tiles - 1) * size)
                below = at_row + down
                live = (slot < metas[row, 2 * scans]) & (below >= 0) & (below < row_count)

                @pl.when(near & live)
                def _():
                    beam = beam_of(metas, which, slot, scans, probe.shape[0])
                    probe_re, probe_im = probe[beam, 0], probe[beam, 1]
                    value = probe_re * probe_re + probe_im * probe_im
                    add_patch(total, 0, y, x // size, x % size, value, lane)

                return carry

            lax.fori_loop(0, scans, add, 0)


def gathered(total, side_l, side_r, in_top, in_bot, in_ctop, in_cbot, channel, chunk, half):
    _, tiles, rows, size = total.shape
    chunks = (rows - size) // half
    low = lanes(half, size) < half
    ext = pl.ds((chunk + 1) * half, half)
    values = own_columns(total, channel, ext, low)

    def add_sides(from_l, from_r):
        from_l = from_l if channel == 0 else turn(from_l)
        from_r = turn(from_r) if channel == 0 else from_r
        values[0] += jnp.where(low, from_l, 0.0)
        values[-1] += jnp.where(low, 0.0, from_r)

    add_sides(side_l[ext, :], side_r[ext, :])
    for at, rim, corner in ((0, in_top, in_ctop), (chunks - 1, in_bot, in_cbot)):
        if chunk == at:
            for t in range(tiles - 1):
                values[t] += rim[channel, :, t * size : (t + 1) * size]
            add_sides(corner[0], corner[1])
    return values


def final_kernel(*refs):
    obj, weight, out = refs[0], refs[1], refs[-1]
    grads = refs[2:9]
    size = grads[0].shape[-1]
    half = size // 2
    tiles = obj.shape[2] // size
    for chunk in range(obj.shape[1] // half):
        wide = pl.ds(size + chunk * half, half)
        scale = [1.0 / (weight[0, t + 1, wide, :] + DAMPING) for t in range(tiles)]
        rows = slice(chunk * half, (chunk + 1) * half)
        for ch in range(2):
            for t, value in enumerate(gathered(*grads, ch, chunk, half)):
                columns = slice(t * size, (t + 1) * size)
                out[ch, rows, columns] = obj[ch, rows, columns] + value * scale[t]


def swap(axis, first):
    lower = range(first, lax.axis_size(axis) - 1, 2)
    return [(i, i + 1) for i in lower] + [(i + 1, i) for i in lower]


def ring(axis, by):
    count = lax.axis_size(axis)
    return [(i, (i + by) % count) for i in range(count)]


def move(x, axis, pairs):
    return lax.ppermute(x, axis, pairs)


def send_rims(side_1, side_2, rim_1, rim_2, odd_row, odd_col):
    rows, size = side_1.shape
    half = size // 2
    in_2 = move(side_2, "col", swap("col", 1))
    in_1 = move(side_1, "col", swap("col", 0))
    rim_1 = move(rim_1, "row", swap("row", 0))
    rim_2 = move(rim_2, "row", swap("row", 1))
    in_l, in_r = jnp.where(odd_col, in_1, in_2), jnp.where(odd_col, in_2, in_1)
    tops = jnp.where(odd_col, jnp.stack([in_1[:half], in_2[:half]]), jnp.stack([in_2[:half], in_1[:half]]))
    low = rows - half
    bottoms = jnp.where(odd_col, jnp.stack([in_1[low:], in_2[low:]]), jnp.stack([in_2[low:], in_1[low:]]))
    corner_1 = move(jnp.where(odd_row, tops, bottoms), "row", swap("row", 0))
    corner_2 = move(jnp.where(odd_row, bottoms, tops), "row", swap("row", 1))
    in_top, in_bot = jnp.where(odd_row, rim_1, rim_2), jnp.where(odd_row, rim_2, rim_1)
    in_ctop, in_cbot = jnp.where(odd_row, corner_1, corner_2), jnp.where(odd_row, corner_2, corner_1)
    return in_l, in_r, in_top, in_bot, in_ctop, in_cbot


def on_device(obj, probe, positions, counts, offsets, measured):
    offsets_count, _, size, _ = probe.shape
    scans = positions.shape[2]
    half = size // 2
    tile_rows, tile_columns = obj.shape[1:]
    rows, tiles = tile_rows + size, tile_columns // size + 1
    row_count = lax.axis_size("row")
    tables = dft_tables(size)

    def packed(x):
        return jnp.concatenate([x[0], x[1]], axis=1)

    at_row, at_col = lax.axis_index("row").astype(jnp.int32), lax.axis_index("col").astype(jnp.int32)
    odd_row, odd_col = lax.rem(at_row, 2) == 1, lax.rem(at_col, 2) == 1
    ends = jnp.where(odd_row, 0, tile_rows - half), jnp.where(odd_row, tile_rows - half, 0)
    here = jnp.stack([at_row, at_col])
    ends, here, odd_row, odd_col = lax.optimization_barrier((ends, here, odd_row, odd_col))
    rows_1, rows_2 = (
        move(lax.dynamic_slice_in_dim(obj, ends[i], half, axis=1), "row", swap("row", i))
        for i in range(2)
    )
    top, bot = jnp.where(odd_row, rows_1, rows_2), jnp.where(odd_row, rows_2, rows_1)
    edge_l, edge_r, meta = call(
        edge_kernel,
        [(tile_rows, size)] * 2 + [jax.ShapeDtypeStruct((1, size), jnp.int32)],
        [VMEM, SMEM, SMEM, SMEM, SMEM],
        (obj, positions[0, 0].T, counts, offsets.T, here),
        10**6,
    )

    most = offsets_count - 1
    metas = {0: meta, most: move(meta, "row", ring("row", most))}

    own_meta = jnp.broadcast_to(meta.astype(F32), (8, size))
    edge_l, edge_r = (
        jnp.concatenate([packed(top[:, :, part]), edge, packed(bot[:, :, part]), own_meta])
        for part, edge in ((slice(0, half), edge_l), (slice(tile_columns - half, None), edge_r))
    )
    columns_2 = move(jnp.where(odd_col, edge_r, edge_l), "col", swap("col", 1))
    columns_1 = move(jnp.where(odd_col, edge_l, edge_r), "col", swap("col", 0))
    left, right = jnp.where(odd_col, columns_1, columns_2), jnp.where(odd_col, columns_2, columns_1)
    (frame,) = call(frame_kernel, [(2, tiles, rows, size)], [VMEM] * 5, (obj, top, bot, left, right), 10**6)

    slots = scans // 2
    halves = ((0, slots), (slots, scans - slots))
    work = [
        pltpu.VMEM((slots * size, 2 * size), BF16),
        pltpu.VMEM((slots * size, 2 * size), BF16),
        pltpu.VMEM((2 * size, slots * size), BF16),
        pltpu.VMEM((2 * size, slots * size), BF16),
    ]
    flops = slots * 2 * 3 * 2 * size * (2 * size) ** 2

    far, wave, power = {}, {}, {}

    def forward(which, parts, arrived=None):
        outs = []
        for start, count in parts:
            tail = 8 if which and start == 0 else 0
            outs += [(2 * size, count * size), (count, 2, size, size), (count * size + tail, size)]
        adds = arrived is not None
        results = call(
            functools.partial(forward_kernel, [(which, *part) for part in parts], scans, adds),
            outs,
            [SMEM, VMEM, VMEM, VMEM] + [VMEM] * adds,
            (metas[which], frame, probe, tables) + ((arrived,) if adds else ()),
            flops * len(parts),
            work,
        )
        for at, (start, _) in enumerate(parts):
            far[which, start], wave[which, start], power[which, start] = results[3 * at : 3 * at + 3]

    forward(most, [halves[0]])
    forward(most, [halves[1]])
    forward(0, list(halves))
    for which in reversed(range(most)):
        for start, count in halves:
            arrived = move(power[which + 1, start], "row", ring("row", -1))
            if which:
                if start == 0:
                    metas[which] = arrived[count * size : count * size + 1].astype(jnp.int32)
                forward(which, [(start, count)], arrived)
            else:
                power[1, start] = arrived
    beside = jnp.concatenate([left[rows : rows + 1], right[rows : rows + 1], jnp.zeros((6, size), F32)])
    factors = {}
    for start, count in halves:
        args = [power[1, start], power[0, start], measured[0, 0, start : start + count].reshape(-1, size)]
        args += [beside] if start == 0 else []
        height = count * size + (beside.shape[0] if start == 0 else 0)
        (factors[start],) = call(factor_kernel, [(height, size)], [VMEM] * len(args), args, 10**6)

    row_count = lax.axis_size("row")
    kept = min(row_count, offsets_count + 2)
    weight = None

    def add_weight(index, shift, beside):
        nonlocal weight
        own = metas[shift] if shift in metas else None
        if own is None:
            span = move(jnp.concatenate([meta.astype(F32), beside[:2]]), "row", ring("row", shift))
            span = span.astype(jnp.int32)
        else:
            span = jnp.concatenate([own, beside[:2].astype(jnp.int32)])
        steps = [(d, w) for d in (-1, 0, 1) for w in range(offsets_count) if (w - d) % kept == index]
        (weight,) = call(
            functools.partial(weight_kernel, steps, scans, shift, row_count, weight is None),
            [(1, tiles + 1, tile_rows + 2 * size, size)],
            [SMEM, VMEM] + ([] if weight is None else [VMEM]),
            (span, probe) + (() if weight is None else (weight,)),
            flops,
            aliases={} if weight is None else {2: 0},
        )

    for index in range(offsets_count, kept):
        add_weight(index, index if index <= offsets_count else index - kept, beside)

    total = None
    for which in range(offsets_count):
        if which:
            for start, _ in halves:
                value = move(factors[start], "row", ring("row", 1))
                if start == 0 and which < most:
                    value, total = lax.optimization_barrier((value, total))
                factors[start] = value
            add_weight(which, which, factors[0][slots * size :])
        else:
            add_weight(0, 0, beside)
        groups = [[part] for part in halves] if which == most else [list(halves)]
        for group in groups:
            fresh, last = total is None, which == most and group[-1] == halves[-1]
            outs = [(2, tiles, rows, size)]
            if last:
                outs += [(rows, size)] * 2 + [(2, half, tile_columns)] * 2
            args = [metas[which], probe, tables]
            for start, _ in group:
                args += [far[which, start], wave[which, start], factors[start]]
            specs = [SMEM] + [VMEM] * (len(args) - 1)
            if not fresh:
                args, specs = args + [total], specs + [VMEM]
            total, *sides = call(
                functools.partial(backward_kernel, [(which, *part) for part in group], scans, row_count, fresh, last),
                outs,
                specs,
                args,
                flops * len(group),
                work,
                {} if fresh else {len(args) - 1: 0},
            )
    grad_in = send_rims(*sides, odd_row, odd_col)

    (new_object,) = call(final_kernel, [obj.shape], [VMEM] * 9, (obj, weight, total, *grad_in), 10**6)
    return new_object


def solution(mesh):
    return jax.shard_map(
        on_device,
        mesh=mesh,
        in_specs=(
            P(None, "row", "col"),
            P(),
            P("row", "col", None, None),
            P("row", "col"),
            P(),
            P("row", "col", None, None, None),
        ),
        out_specs=P(None, "row", "col"),
        check_vma=False,
    )
```

```python
import functools
import math

import jax
import jax.numpy as jnp
import numpy as np
from jax import lax
from jax.experimental import pallas as pl
from jax.experimental.pallas import tpu as pltpu
from jax.sharding import PartitionSpec as P

EPSILON = 0.5
DAMPING = 0.5


SMEM = pl.BlockSpec(memory_space=pltpu.SMEM)
VMEM = pl.BlockSpec(memory_space=pltpu.VMEM)
F32 = jnp.float32
BF16 = jnp.bfloat16


def call(kernel, outs, specs, args, flops, scratch=(), aliases=None):
    return pl.pallas_call(
        kernel,
        out_shape=[s if hasattr(s, "dtype") else jax.ShapeDtypeStruct(s, F32) for s in outs],
        in_specs=specs,
        out_specs=[VMEM] * len(outs),
        scratch_shapes=list(scratch),
        input_output_aliases=aliases or {},
        compiler_params=pltpu.CompilerParams(vmem_limit_bytes=16 * 2**20),
        cost_estimate=pl.CostEstimate(flops=flops, bytes_accessed=2**20, transcendentals=0),
    )(*args)


def dft_tables(length):
    index = np.arange(length)
    angle = (index[:, None] * index[None, :] % length) * (2.0 * math.pi / length)
    cos, sin = np.cos(angle) / math.sqrt(length), np.sin(angle) / math.sqrt(length)
    right = np.block([[cos, -sin], [sin, cos]])
    tables = []
    for table in (right, right.T):
        high = table.astype(BF16)
        tables += [high, (table - high.astype(np.float64)).astype(BF16)]
    return jnp.asarray(np.stack(tables))


def split(x):
    high = x.astype(BF16)
    return high, (x - high.astype(F32)).astype(BF16)


def dot3(a_high, a_low, b_high, b_low):
    dot = functools.partial(jnp.dot, preferred_element_type=F32)
    return dot(a_high, b_high) + (dot(a_low, b_high) + dot(a_high, b_low))


def lanes(rows, size):
    return lax.broadcasted_iota(jnp.int32, (rows, size), 1)


def turn(x):
    return pltpu.roll(x, x.shape[-1] // 2, 1)


def beam_of(meta, which, slot, scans, beams):
    beam = jnp.int32(0)
    for index in range(1, beams):
        beam = jnp.where(meta[0, 2 * scans + 3 + slot * beams + index] == which, index, beam)
    return beam


def place(meta, slot, size):
    y, x = meta[0, 2 * slot], meta[0, 2 * slot + 1]
    return y, x // size, x % size


def edge_kernel(obj, positions, counts, offsets, place_of, edge_l, edge_r, meta):
    scans = positions.shape[2]
    values = [positions[0, 0, slot, axis] for slot in range(scans) for axis in range(2)]
    values += [counts[0, 0], place_of[0], place_of[1]]
    values += [offsets[slot, beam] for slot in range(scans) for beam in range(offsets.shape[1])]
    assert len(values) <= meta.shape[1]
    lane = lax.broadcasted_iota(jnp.int32, meta.shape, 1)
    row = jnp.zeros(meta.shape, jnp.int32)
    for at, value in enumerate(values):
        row = jnp.where(lane == at, value, row)
    meta[...] = row
    _, rows, columns = obj.shape
    size = edge_l.shape[1]
    low = lanes(rows, size) < size // 2
    near, far = slice(0, size), slice(columns - size, columns)
    edge_l[...] = jnp.where(low, obj[0, :, near], turn(obj[1, :, near]))
    edge_r[...] = jnp.where(low, turn(obj[0, :, far]), obj[1, :, far])


def frame_kernel(obj, top, bot, left, right, out):
    tiles, rows, size = out.shape[1:]
    half = size // 2
    low = lanes(half, size) < half
    for at in range(0, rows, half):
        body, src = obj, pl.ds(at - half, half)
        if at == 0:
            body, src = top, pl.ds(0, half)
        elif at == rows - half:
            body, src = bot, pl.ds(0, half)
        here = pl.ds(at, half)
        for ch in range(2):
            parts = [turn(body[ch, src, t * size : (t + 1) * size]) for t in range(tiles - 1)]
            edge_l, edge_r = left[here, :], right[here, :]
            edge_l = edge_l if ch == 0 else turn(edge_l)
            edge_r = turn(edge_r) if ch == 0 else edge_r
            parts = [edge_l, *parts, edge_r]
            for t in range(tiles):
                out[ch, t, here, :] = jnp.where(low, parts[t], parts[t + 1])


def forward_kernel(parts, scans, adds, *refs):
    meta, frame, probe, tables = refs[:4]
    refs = refs[4:]
    if adds:
        arrived, refs = refs[0], refs[1:]
    outs, (x_high, x_low, y_high, y_low) = refs[:-4], refs[-4:]
    size = probe.shape[-1]
    lane = lanes(size, size)
    for at, (which, start, slots) in enumerate(parts):
        far, wave, power = outs[3 * at : 3 * at + 3]
        for index in range(slots):
            slot = start + index
            y, tile, shift = place(meta, slot, size)
            beam = beam_of(meta, which, slot, scans, probe.shape[0])
            back = lax.rem(size - shift, size)
            patch = []
            for ch in range(2):
                near = pltpu.roll(frame[ch, tile, pl.ds(y, size), :], back, 1)
                rest = pltpu.roll(frame[ch, tile + 1, pl.ds(y, size), :], back, 1)
                patch.append(jnp.where(lane < size - shift, near, rest))
            probe_re, probe_im = probe[beam, 0], probe[beam, 1]
            waves = (
                probe_re * patch[0] - probe_im * patch[1],
                probe_re * patch[1] + probe_im * patch[0],
            )
            rows = slice(index * size, (index + 1) * size)
            for ch in range(2):
                wave[index, ch] = waves[ch]
                columns = slice(ch * size, (ch + 1) * size)
                x_high[rows, columns], x_low[rows, columns] = split(waves[ch])
        for slot in range(0, slots, 2):
            rows = slice(slot * size, (slot + 2) * size)
            mid = dot3(x_high[rows, :], x_low[rows, :], tables[0], tables[1])
            for sub in range(2):
                columns = slice((slot + sub) * size, (slot + sub + 1) * size)
                for ch in range(2):
                    piece = mid[sub * size : (sub + 1) * size, ch * size : (ch + 1) * size]
                    into = slice(ch * size, (ch + 1) * size)
                    y_high[into, columns], y_low[into, columns] = split(piece)
            columns = slice(slot * size, (slot + 2) * size)
            result = dot3(tables[2], tables[3], y_high[:, columns], y_low[:, columns])
            far[:, columns] = result
            for sub in range(2):
                inside = slice(sub * size, (sub + 1) * size)
                re, im = result[:size, inside], result[size:, inside]
                rows = slice((slot + sub) * size, (slot + sub + 1) * size)
                own = re * re + im * im
                power[rows, :] = own + arrived[rows, :] if adds else own
        if power.shape[0] > slots * size:
            lane = lanes(power.shape[0] - slots * size, size)
            row = jnp.zeros(lane.shape, jnp.int32)
            for index in range(2 * scans + 3 + scans * probe.shape[0]):
                row = jnp.where(lane == index, meta[0, index], row)
            power[slots * size :, :] = row.astype(F32)


def factor_kernel(arrived, own, measured, *refs):
    out = refs[-1]
    count = own.shape[0]
    total = own[...] + arrived[:count, :]
    out[:count, :] = measured[...] / jnp.sqrt(total + EPSILON)
    if len(refs) > 1:
        out[count:, :] = refs[0][...]


def add_patch(total, channel, y, tile, shift, value, lane):
    moved = pltpu.roll(value, shift, 1)
    rows = pl.ds(y, value.shape[0])
    total[channel, tile, rows, :] += jnp.where(lane >= shift, moved, 0.0)
    total[channel, tile + 1, rows, :] += jnp.where(lane < shift, moved, 0.0)


def write_sides(total, odd, side_1, side_2, ends_2):
    _, tiles, rows, size = total.shape
    low = lanes(rows, size) < size // 2
    left = jnp.where(low, total[0, 0], turn(total[1, 0]))
    right = jnp.where(low, turn(total[0, tiles - 1]), total[1, tiles - 1])
    side_1[...] = jnp.where(odd == 1, left, right)
    second = jnp.where(odd == 1, right, left)
    half = size // 2
    side_2[...] = second[half : rows - half, :]
    ends_2[:half, :] = second[:half, :]
    ends_2[half:, :] = second[rows - half :, :]


def own_columns(total, channel, rows, low):
    tiles = total.shape[1]
    turned = [turn(total[channel, t, rows, :]) for t in range(tiles)]
    return [jnp.where(low, turned[t], turned[t + 1]) for t in range(tiles - 1)]


def write_rims(total, odd, rim_1, rim_2):
    channels, _, rows, size = total.shape
    half = size // 2
    low = lanes(half, size) < half
    for ch in range(channels):
        tops = own_columns(total, ch, pl.ds(0, half), low)
        bottoms = own_columns(total, ch, pl.ds(rows - half, half), low)
        for t, (top, bottom) in enumerate(zip(tops, bottoms)):
            columns = slice(t * size, (t + 1) * size)
            rim_1[ch, :, columns] = jnp.where(odd == 1, top, bottom)
            rim_2[ch, :, columns] = jnp.where(odd == 1, bottom, top)


def backward_kernel(parts, scans, row_count, fresh, last, *refs):
    meta, probe, tables = refs[:3]
    inputs, refs = refs[3 : 3 + 3 * len(parts)], refs[3 + 3 * len(parts) :]
    if not fresh:
        refs = refs[1:]
    total, refs = refs[0], refs[1:]
    if last:
        (side_1, side_2, ends_2, rim_1, rim_2), refs = refs[:5], refs[5:]
    x_high, x_low, y_high, y_low = refs
    size = probe.shape[-1]
    lane = lanes(size, size)
    if fresh:
        total[...] = jnp.zeros_like(total)
    for at, (which, start, slots) in enumerate(parts):
        far, wave, factor = inputs[3 * at : 3 * at + 3]
        for slot in range(0, slots, 2):
            for sub in range(2):
                columns = slice((slot + sub) * size, (slot + sub + 1) * size)
                scale = factor[(slot + sub) * size : (slot + sub + 1) * size, :]
                for ch in range(2):
                    into = slice(ch * size, (ch + 1) * size)
                    y_high[into, columns], y_low[into, columns] = split(far[into, columns] * scale)
            columns = slice(slot * size, (slot + 2) * size)
            mid = dot3(tables[0], tables[1], y_high[:, columns], y_low[:, columns])
            for sub in range(2):
                rows = slice((slot + sub) * size, (slot + sub + 1) * size)
                for ch in range(2):
                    piece = mid[ch * size : (ch + 1) * size, sub * size : (sub + 1) * size]
                    into = slice(ch * size, (ch + 1) * size)
                    x_high[rows, into], x_low[rows, into] = split(piece)
            rows = slice(slot * size, (slot + 2) * size)
            result = dot3(x_high[rows, :], x_low[rows, :], tables[2], tables[3])
            for sub in range(2):
                true_slot = start + slot + sub
                live = (true_slot < meta[0, 2 * scans]).astype(F32)
                beam = beam_of(meta, which, true_slot, scans, probe.shape[0])
                probe_re, probe_im = probe[beam, 0], probe[beam, 1]
                inside = slice(sub * size, (sub + 1) * size)
                change_re = (result[inside, :size] - wave[slot + sub, 0]) * live
                change_im = (result[inside, size:] - wave[slot + sub, 1]) * live
                grad_re = probe_re * change_re + probe_im * change_im
                grad_im = probe_re * change_im - probe_im * change_re
                spot = place(meta, true_slot, size)
                add_patch(total, 0, *spot, grad_re, lane)
                add_patch(total, 1, *spot, grad_im, lane)
    if last:
        odd = lax.rem(meta[0, 2 * scans + 2], 2)
        write_sides(total, odd, side_1, side_2, ends_2)
        odd = lax.rem(lax.rem(meta[0, 2 * scans + 1] + parts[0][0], row_count), 2)
        write_rims(total, odd, rim_1, rim_2)


def weight_kernel(steps, scans, which_tile, row_count, fresh, *refs):
    metas, probe, total = refs[0], refs[1], refs[-1]
    _, tiles, rows, size = total.shape
    half = size // 2
    own_rows, own_columns = rows - 2 * size, (tiles - 2) * size
    lane = lanes(size, size)
    if fresh:
        total[...] = jnp.zeros_like(total)
    at_row = lax.rem(metas[0, 2 * scans + 1] + which_tile + row_count, row_count)
    for row, across in enumerate((0, -1, 1)):
        for down, which in steps:

            def add(slot, carry, row=row, across=across, down=down, which=which):
                y = metas[row, 2 * slot] + (down * own_rows + half)
                x = metas[row, 2 * slot + 1] + (across * own_columns + half)
                near = (y > 0) & (y < rows - size) & (x > 0) & (x < (tiles - 1) * size)
                below = at_row + down
                live = (slot < metas[row, 2 * scans]) & (below >= 0) & (below < row_count)

                @pl.when(near & live)
                def _():
                    beam = beam_of(metas, which, slot, scans, probe.shape[0])
                    probe_re, probe_im = probe[beam, 0], probe[beam, 1]
                    value = probe_re * probe_re + probe_im * probe_im
                    add_patch(total, 0, y, x // size, x % size, value, lane)

                return carry

            lax.fori_loop(0, scans, add, 0)


def gathered(total, side_l, side_r, in_top, in_bot, in_ctop, in_cbot, channel, chunk, half):
    _, tiles, rows, size = total.shape
    chunks = (rows - size) // half
    low = lanes(half, size) < half
    values = own_columns(total, channel, pl.ds((chunk + 1) * half, half), low)

    def add_sides(from_l, from_r):
        from_l = from_l if channel == 0 else turn(from_l)
        from_r = turn(from_r) if channel == 0 else from_r
        values[0] += jnp.where(low, from_l, 0.0)
        values[-1] += jnp.where(low, 0.0, from_r)

    own = pl.ds(chunk * half, half)
    add_sides(side_l[own, :], side_r[own, :])
    for at, rim, corner in ((0, in_top, in_ctop), (chunks - 1, in_bot, in_cbot)):
        if chunk == at:
            for t in range(tiles - 1):
                values[t] += rim[channel, :, t * size : (t + 1) * size]
            add_sides(corner[0], corner[1])
    return values


def final_kernel(*refs):
    obj, weight, out = refs[0], refs[1], refs[-1]
    grads = refs[2:9]
    size = grads[0].shape[-1]
    half = size // 2
    tiles = obj.shape[2] // size
    for chunk in range(obj.shape[1] // half):
        wide = pl.ds(size + chunk * half, half)
        scale = [1.0 / (weight[0, t + 1, wide, :] + DAMPING) for t in range(tiles)]
        rows = slice(chunk * half, (chunk + 1) * half)
        for ch in range(2):
            for t, value in enumerate(gathered(*grads, ch, chunk, half)):
                columns = slice(t * size, (t + 1) * size)
                out[ch, rows, columns] = obj[ch, rows, columns] + value * scale[t]


def swap(axis, first):
    lower = range(first, lax.axis_size(axis) - 1, 2)
    return [(i, i + 1) for i in lower] + [(i + 1, i) for i in lower]


def ring(axis, by):
    count = lax.axis_size(axis)
    return [(i, (i + by) % count) for i in range(count)]


def move(x, axis, pairs):
    return lax.ppermute(x, axis, pairs)


def send_rims(side_1, side_2, ends_2, rim_1, rim_2, odd_row, odd_col):
    rows, size = side_1.shape
    half = size // 2
    ends_2 = move(ends_2, "col", swap("col", 1))
    in_1 = move(side_1, "col", swap("col", 0))
    in_2 = move(side_2, "col", swap("col", 1))
    rim_1 = move(rim_1, "row", swap("row", 0))
    rim_2 = move(rim_2, "row", swap("row", 1))

    def both(of_1, of_2):
        return jnp.where(odd_col, jnp.stack([of_1, of_2]), jnp.stack([of_2, of_1]))

    tops, bottoms = both(in_1[:half], ends_2[:half]), both(in_1[rows - half :], ends_2[half:])
    in_1 = in_1[half : rows - half]
    in_l, in_r = jnp.where(odd_col, in_1, in_2), jnp.where(odd_col, in_2, in_1)
    corner_1 = move(jnp.where(odd_row, tops, bottoms), "row", swap("row", 0))
    corner_2 = move(jnp.where(odd_row, bottoms, tops), "row", swap("row", 1))
    in_top, in_bot = jnp.where(odd_row, rim_1, rim_2), jnp.where(odd_row, rim_2, rim_1)
    in_ctop, in_cbot = jnp.where(odd_row, corner_1, corner_2), jnp.where(odd_row, corner_2, corner_1)
    return in_l, in_r, in_top, in_bot, in_ctop, in_cbot


def on_device(obj, probe, positions, counts, offsets, measured):
    offsets_count, _, size, _ = probe.shape
    scans = positions.shape[2]
    half = size // 2
    tile_rows, tile_columns = obj.shape[1:]
    rows, tiles = tile_rows + size, tile_columns // size + 1
    row_count = lax.axis_size("row")
    tables = dft_tables(size)

    def packed(x):
        return jnp.concatenate([x[0], x[1]], axis=1)

    at_row, at_col = lax.axis_index("row").astype(jnp.int32), lax.axis_index("col").astype(jnp.int32)
    odd_row, odd_col = lax.rem(at_row, 2) == 1, lax.rem(at_col, 2) == 1
    ends = jnp.where(odd_row, 0, tile_rows - half), jnp.where(odd_row, tile_rows - half, 0)
    rows_1, rows_2 = (
        move(lax.dynamic_slice_in_dim(obj, ends[i], half, axis=1), "row", swap("row", i))
        for i in range(2)
    )
    top, bot = jnp.where(odd_row, rows_1, rows_2), jnp.where(odd_row, rows_2, rows_1)
    edge_l, edge_r, meta = call(
        edge_kernel,
        [(tile_rows, size)] * 2 + [jax.ShapeDtypeStruct((1, size), jnp.int32)],
        [VMEM, SMEM, SMEM, SMEM, SMEM],
        (obj, positions, counts, offsets, jnp.stack([at_row, at_col])),
        10**6,
    )

    most = offsets_count - 1
    metas = {0: meta, most: move(meta, "row", ring("row", most))}

    own_meta = jnp.broadcast_to(meta.astype(F32), (8, size))
    edge_l, edge_r = (
        jnp.concatenate([packed(top[:, :, part]), edge, packed(bot[:, :, part]), own_meta])
        for part, edge in ((slice(0, half), edge_l), (slice(tile_columns - half, None), edge_r))
    )
    columns_2 = move(jnp.where(odd_col, edge_r, edge_l), "col", swap("col", 1))
    columns_1 = move(jnp.where(odd_col, edge_l, edge_r), "col", swap("col", 0))
    left, right = jnp.where(odd_col, columns_1, columns_2), jnp.where(odd_col, columns_2, columns_1)
    (frame,) = call(frame_kernel, [(2, tiles, rows, size)], [VMEM] * 5, (obj, top, bot, left, right), 10**6)

    slots = scans // 2
    halves = ((0, slots), (slots, scans - slots))
    work = [
        pltpu.VMEM((slots * size, 2 * size), BF16),
        pltpu.VMEM((slots * size, 2 * size), BF16),
        pltpu.VMEM((2 * size, slots * size), BF16),
        pltpu.VMEM((2 * size, slots * size), BF16),
    ]
    flops = slots * 2 * 3 * 2 * size * (2 * size) ** 2

    far, wave, power = {}, {}, {}

    def forward(which, parts, arrived=None):
        outs = []
        for start, count in parts:
            tail = 8 if which and start == 0 else 0
            outs += [(2 * size, count * size), (count, 2, size, size), (count * size + tail, size)]
        adds = arrived is not None
        results = call(
            functools.partial(forward_kernel, [(which, *part) for part in parts], scans, adds),
            outs,
            [SMEM, VMEM, VMEM, VMEM] + [VMEM] * adds,
            (metas[which], frame, probe, tables) + ((arrived,) if adds else ()),
            flops * len(parts),
            work,
        )
        for at, (start, _) in enumerate(parts):
            far[which, start], wave[which, start], power[which, start] = results[3 * at : 3 * at + 3]

    forward(most, [halves[0]])
    forward(most, [halves[1]])
    forward(0, list(halves))
    for which in reversed(range(most)):
        for start, count in halves:
            arrived = move(power[which + 1, start], "row", ring("row", -1))
            if which:
                if start == 0:
                    metas[which] = arrived[count * size : count * size + 1].astype(jnp.int32)
                forward(which, [(start, count)], arrived)
            else:
                power[1, start] = arrived
    beside = jnp.concatenate([left[rows : rows + 1], right[rows : rows + 1], jnp.zeros((6, size), F32)])
    factors = {}
    for start, count in halves:
        args = [power[1, start], power[0, start], measured[0, 0, start : start + count].reshape(-1, size)]
        args += [beside] if start == 0 else []
        height = count * size + (beside.shape[0] if start == 0 else 0)
        (factors[start],) = call(factor_kernel, [(height, size)], [VMEM] * len(args), args, 10**6)

    row_count = lax.axis_size("row")
    kept = min(row_count, offsets_count + 2)
    weight = None

    def add_weight(index, shift, beside):
        nonlocal weight
        own = metas[shift] if shift in metas else None
        if own is None:
            span = move(jnp.concatenate([meta.astype(F32), beside[:2]]), "row", ring("row", shift))
            span = span.astype(jnp.int32)
        else:
            span = jnp.concatenate([own, beside[:2].astype(jnp.int32)])
        steps = [(d, w) for d in (-1, 0, 1) for w in range(offsets_count) if (w - d) % kept == index]
        (weight,) = call(
            functools.partial(weight_kernel, steps, scans, shift, row_count, weight is None),
            [(1, tiles + 1, tile_rows + 2 * size, size)],
            [SMEM, VMEM] + ([] if weight is None else [VMEM]),
            (span, probe) + (() if weight is None else (weight,)),
            flops,
            aliases={} if weight is None else {2: 0},
        )

    for index in range(offsets_count, kept):
        add_weight(index, index if index <= offsets_count else index - kept, beside)

    total = None
    for which in range(offsets_count):
        if which:
            for start, _ in halves:
                value = move(factors[start], "row", ring("row", 1))
                if start == 0 and which < most:
                    value, total = lax.optimization_barrier((value, total))
                factors[start] = value
            add_weight(which, which, factors[0][slots * size :])
        else:
            add_weight(0, 0, beside)
        groups = [[part] for part in halves] if which == most else [list(halves)]
        for group in groups:
            fresh, last = total is None, which == most and group[-1] == halves[-1]
            outs = [(2, tiles, rows, size)]
            if last:
                outs += [(rows, size), (tile_rows, size), (size, size)] + [(2, half, tile_columns)] * 2
            args = [metas[which], probe, tables]
            for start, _ in group:
                args += [far[which, start], wave[which, start], factors[start]]
            specs = [SMEM] + [VMEM] * (len(args) - 1)
            if not fresh:
                args, specs = args + [total], specs + [VMEM]
            total, *sides = call(
                functools.partial(backward_kernel, [(which, *part) for part in group], scans, row_count, fresh, last),
                outs,
                specs,
                args,
                flops * len(group),
                work,
                {} if fresh else {len(args) - 1: 0},
            )
    grad_in = send_rims(*sides, odd_row, odd_col)

    (new_object,) = call(final_kernel, [obj.shape], [VMEM] * 9, (obj, weight, total, *grad_in), 10**6)
    return new_object


def solution(mesh):
    return jax.shard_map(
        on_device,
        mesh=mesh,
        in_specs=(
            P(None, "row", "col"),
            P(),
            P("row", "col", None, None),
            P("row", "col"),
            P(),
            P("row", "col", None, None, None),
        ),
        out_specs=P(None, "row", "col"),
        check_vma=False,
    )
```

```python
import functools
import math

import jax
import jax.numpy as jnp
import numpy as np
from jax import lax
from jax.experimental import pallas as pl
from jax.experimental.pallas import tpu as pltpu
from jax.sharding import PartitionSpec as P

EPSILON = 0.5
DAMPING = 0.5


SMEM = pl.BlockSpec(memory_space=pltpu.SMEM)
VMEM = pl.BlockSpec(memory_space=pltpu.VMEM)
F32 = jnp.float32
BF16 = jnp.bfloat16


def call(kernel, outs, specs, args, flops, scratch=(), aliases=None):
    return pl.pallas_call(
        kernel,
        out_shape=[s if hasattr(s, "dtype") else jax.ShapeDtypeStruct(s, F32) for s in outs],
        in_specs=specs,
        out_specs=[VMEM] * len(outs),
        scratch_shapes=list(scratch),
        input_output_aliases=aliases or {},
        compiler_params=pltpu.CompilerParams(vmem_limit_bytes=16 * 2**20),
        cost_estimate=pl.CostEstimate(flops=flops, bytes_accessed=2**20, transcendentals=0),
    )(*args)


def dft_tables(length):
    index = np.arange(length)
    angle = (index[:, None] * index[None, :] % length) * (2.0 * math.pi / length)
    cos, sin = np.cos(angle) / math.sqrt(length), np.sin(angle) / math.sqrt(length)
    right = np.block([[cos, -sin], [sin, cos]])
    tables = []
    for table in (right, right.T):
        high = table.astype(BF16)
        tables += [high, (table - high.astype(np.float64)).astype(BF16)]
    return jnp.asarray(np.stack(tables))


def split(x):
    high = x.astype(BF16)
    return high, (x - high.astype(F32)).astype(BF16)


def dot3(a_high, a_low, b_high, b_low):
    dot = functools.partial(jnp.dot, preferred_element_type=F32)
    return dot(a_high, b_high) + (dot(a_low, b_high) + dot(a_high, b_low))


def lanes(rows, size):
    return lax.broadcasted_iota(jnp.int32, (rows, size), 1)


def turn(x):
    return pltpu.roll(x, x.shape[-1] // 2, 1)


def beam_of(meta, which, slot, scans, beams):
    beam = jnp.int32(0)
    for index in range(1, beams):
        beam = jnp.where(meta[0, 2 * scans + 3 + slot * beams + index] == which, index, beam)
    return beam


def place(meta, slot, size):
    y, x = meta[0, 2 * slot], meta[0, 2 * slot + 1]
    return y, x // size, x % size


def edge_kernel(obj, joined, edge_l, edge_r, meta):
    beams, scans = joined.shape[0] - 3, joined.shape[1]
    values = [joined[axis, slot] for slot in range(scans) for axis in range(2)]
    values += [joined[2 + beams, at] for at in range(3)]
    values += [joined[2 + beam, slot] for slot in range(scans) for beam in range(beams)]
    assert len(values) <= meta.shape[1]
    lane = lax.broadcasted_iota(jnp.int32, meta.shape, 1)
    row = jnp.zeros(meta.shape, jnp.int32)
    for at, value in enumerate(values):
        row = jnp.where(lane == at, value, row)
    meta[...] = row
    _, rows, columns = obj.shape
    size = edge_l.shape[1]
    low = lanes(rows, size) < size // 2
    near, far = slice(0, size), slice(columns - size, columns)
    edge_l[...] = jnp.where(low, obj[0, :, near], turn(obj[1, :, near]))
    edge_r[...] = jnp.where(low, turn(obj[0, :, far]), obj[1, :, far])


def frame_kernel(obj, top, bot, left, right, out):
    tiles, rows, size = out.shape[1:]
    half = size // 2
    low = lanes(half, size) < half
    for at in range(0, rows, half):
        body, src = obj, pl.ds(at - half, half)
        if at == 0:
            body, src = top, pl.ds(0, half)
        elif at == rows - half:
            body, src = bot, pl.ds(0, half)
        here = pl.ds(at, half)
        for ch in range(2):
            parts = [turn(body[ch, src, t * size : (t + 1) * size]) for t in range(tiles - 1)]
            edge_l, edge_r = left[here, :], right[here, :]
            edge_l = edge_l if ch == 0 else turn(edge_l)
            edge_r = turn(edge_r) if ch == 0 else edge_r
            parts = [edge_l, *parts, edge_r]
            for t in range(tiles):
                out[ch, t, here, :] = jnp.where(low, parts[t], parts[t + 1])


def forward_kernel(parts, scans, adds, *refs):
    meta, frame, probe, tables = refs[:4]
    refs = refs[4:]
    if adds:
        arrived, refs = refs[0], refs[1:]
    outs, (x_high, x_low, y_high, y_low) = refs[:-4], refs[-4:]
    size = probe.shape[-1]
    lane = lanes(size, size)
    for at, (which, start, slots) in enumerate(parts):
        far, wave, power = outs[3 * at : 3 * at + 3]
        for index in range(slots):
            slot = start + index
            y, tile, shift = place(meta, slot, size)
            beam = beam_of(meta, which, slot, scans, probe.shape[0])
            back = lax.rem(size - shift, size)
            patch = []
            for ch in range(2):
                near = pltpu.roll(frame[ch, tile, pl.ds(y, size), :], back, 1)
                rest = pltpu.roll(frame[ch, tile + 1, pl.ds(y, size), :], back, 1)
                patch.append(jnp.where(lane < size - shift, near, rest))
            probe_re, probe_im = probe[beam, 0], probe[beam, 1]
            waves = (
                probe_re * patch[0] - probe_im * patch[1],
                probe_re * patch[1] + probe_im * patch[0],
            )
            rows = slice(index * size, (index + 1) * size)
            for ch in range(2):
                wave[index, ch] = waves[ch]
                columns = slice(ch * size, (ch + 1) * size)
                x_high[rows, columns], x_low[rows, columns] = split(waves[ch])
        for slot in range(0, slots, 2):
            rows = slice(slot * size, (slot + 2) * size)
            mid = dot3(x_high[rows, :], x_low[rows, :], tables[0], tables[1])
            for sub in range(2):
                columns = slice((slot + sub) * size, (slot + sub + 1) * size)
                for ch in range(2):
                    piece = mid[sub * size : (sub + 1) * size, ch * size : (ch + 1) * size]
                    into = slice(ch * size, (ch + 1) * size)
                    y_high[into, columns], y_low[into, columns] = split(piece)
            columns = slice(slot * size, (slot + 2) * size)
            result = dot3(tables[2], tables[3], y_high[:, columns], y_low[:, columns])
            far[:, columns] = result
            for sub in range(2):
                inside = slice(sub * size, (sub + 1) * size)
                re, im = result[:size, inside], result[size:, inside]
                rows = slice((slot + sub) * size, (slot + sub + 1) * size)
                own = re * re + im * im
                power[rows, :] = own + arrived[rows, :] if adds else own
        if power.shape[0] > slots * size:
            lane = lanes(power.shape[0] - slots * size, size)
            row = jnp.zeros(lane.shape, jnp.int32)
            for index in range(2 * scans + 3 + scans * probe.shape[0]):
                row = jnp.where(lane == index, meta[0, index], row)
            power[slots * size :, :] = row.astype(F32)


def factor_kernel(arrived, own, measured, *refs):
    out = refs[-1]
    count = own.shape[0]
    total = own[...] + arrived[:count, :]
    out[:count, :] = measured[...] / jnp.sqrt(total + EPSILON)
    if len(refs) > 1:
        out[count:, :] = refs[0][...]


def add_patch(total, channel, y, tile, shift, value, lane):
    moved = pltpu.roll(value, shift, 1)
    rows = pl.ds(y, value.shape[0])
    total[channel, tile, rows, :] += jnp.where(lane >= shift, moved, 0.0)
    total[channel, tile + 1, rows, :] += jnp.where(lane < shift, moved, 0.0)


def write_sides(total, odd, side_1, side_2, ends_2):
    _, tiles, rows, size = total.shape
    low = lanes(rows, size) < size // 2
    left = jnp.where(low, total[0, 0], turn(total[1, 0]))
    right = jnp.where(low, turn(total[0, tiles - 1]), total[1, tiles - 1])
    side_1[...] = jnp.where(odd == 1, left, right)
    second = jnp.where(odd == 1, right, left)
    half = size // 2
    side_2[...] = second[half : rows - half, :]
    ends_2[:half, :] = second[:half, :]
    ends_2[half:, :] = second[rows - half :, :]


def own_columns(total, channel, rows, low):
    tiles = total.shape[1]
    turned = [turn(total[channel, t, rows, :]) for t in range(tiles)]
    return [jnp.where(low, turned[t], turned[t + 1]) for t in range(tiles - 1)]


def write_rims(total, odd, rim_1, rim_2):
    channels, _, rows, size = total.shape
    half = size // 2
    low = lanes(half, size) < half
    for ch in range(channels):
        tops = own_columns(total, ch, pl.ds(0, half), low)
        bottoms = own_columns(total, ch, pl.ds(rows - half, half), low)
        for t, (top, bottom) in enumerate(zip(tops, bottoms)):
            columns = slice(t * size, (t + 1) * size)
            rim_1[ch, :, columns] = jnp.where(odd == 1, top, bottom)
            rim_2[ch, :, columns] = jnp.where(odd == 1, bottom, top)


def backward_kernel(parts, scans, row_count, fresh, last, *refs):
    meta, probe, tables = refs[:3]
    inputs, refs = refs[3 : 3 + 3 * len(parts)], refs[3 + 3 * len(parts) :]
    if not fresh:
        refs = refs[1:]
    total, refs = refs[0], refs[1:]
    if last:
        (side_1, side_2, ends_2, rim_1, rim_2), refs = refs[:5], refs[5:]
    x_high, x_low, y_high, y_low = refs
    size = probe.shape[-1]
    lane = lanes(size, size)
    if fresh:
        total[...] = jnp.zeros_like(total)
    for at, (which, start, slots) in enumerate(parts):
        far, wave, factor = inputs[3 * at : 3 * at + 3]
        for slot in range(0, slots, 2):
            for sub in range(2):
                columns = slice((slot + sub) * size, (slot + sub + 1) * size)
                scale = factor[(slot + sub) * size : (slot + sub + 1) * size, :]
                for ch in range(2):
                    into = slice(ch * size, (ch + 1) * size)
                    y_high[into, columns], y_low[into, columns] = split(far[into, columns] * scale)
            columns = slice(slot * size, (slot + 2) * size)
            mid = dot3(tables[0], tables[1], y_high[:, columns], y_low[:, columns])
            for sub in range(2):
                rows = slice((slot + sub) * size, (slot + sub + 1) * size)
                for ch in range(2):
                    piece = mid[ch * size : (ch + 1) * size, sub * size : (sub + 1) * size]
                    into = slice(ch * size, (ch + 1) * size)
                    x_high[rows, into], x_low[rows, into] = split(piece)
            rows = slice(slot * size, (slot + 2) * size)
            result = dot3(x_high[rows, :], x_low[rows, :], tables[2], tables[3])
            for sub in range(2):
                true_slot = start + slot + sub
                live = (true_slot < meta[0, 2 * scans]).astype(F32)
                beam = beam_of(meta, which, true_slot, scans, probe.shape[0])
                probe_re, probe_im = probe[beam, 0], probe[beam, 1]
                inside = slice(sub * size, (sub + 1) * size)
                change_re = (result[inside, :size] - wave[slot + sub, 0]) * live
                change_im = (result[inside, size:] - wave[slot + sub, 1]) * live
                grad_re = probe_re * change_re + probe_im * change_im
                grad_im = probe_re * change_im - probe_im * change_re
                spot = place(meta, true_slot, size)
                add_patch(total, 0, *spot, grad_re, lane)
                add_patch(total, 1, *spot, grad_im, lane)
    if last:
        odd = lax.rem(meta[0, 2 * scans + 2], 2)
        write_sides(total, odd, side_1, side_2, ends_2)
        odd = lax.rem(lax.rem(meta[0, 2 * scans + 1] + parts[0][0], row_count), 2)
        write_rims(total, odd, rim_1, rim_2)


def weight_kernel(steps, scans, which_tile, row_count, fresh, *refs):
    metas, probe, total = refs[0], refs[1], refs[-1]
    _, tiles, rows, size = total.shape
    half = size // 2
    own_rows, own_columns = rows - 2 * size, (tiles - 2) * size
    lane = lanes(size, size)
    if fresh:
        total[...] = jnp.zeros_like(total)
    at_row = lax.rem(metas[0, 2 * scans + 1] + which_tile + row_count, row_count)
    for row, across in enumerate((0, -1, 1)):
        for down, which in steps:

            def add(slot, carry, row=row, across=across, down=down, which=which):
                y = metas[row, 2 * slot] + (down * own_rows + half)
                x = metas[row, 2 * slot + 1] + (across * own_columns + half)
                near = (y > 0) & (y < rows - size) & (x > 0) & (x < (tiles - 1) * size)
                below = at_row + down
                live = (slot < metas[row, 2 * scans]) & (below >= 0) & (below < row_count)

                @pl.when(near & live)
                def _():
                    beam = beam_of(metas, which, slot, scans, probe.shape[0])
                    probe_re, probe_im = probe[beam, 0], probe[beam, 1]
                    value = probe_re * probe_re + probe_im * probe_im
                    add_patch(total, 0, y, x // size, x % size, value, lane)

                return carry

            lax.fori_loop(0, scans, add, 0)


def inner_kernel(obj, weight, total, base, scale):
    _, tiles, _, size = total.shape
    half = size // 2
    low = lanes(half, size) < half
    for chunk in range(obj.shape[1] // half):
        own = slice(chunk * half, (chunk + 1) * half)
        for t in range(tiles - 1):
            columns = slice(t * size, (t + 1) * size)
            scale[own, columns] = 1.0 / (weight[0, t + 1, pl.ds(size + chunk * half, half), :] + DAMPING)
        for ch in range(2):
            for t, value in enumerate(own_columns(total, ch, pl.ds((chunk + 1) * half, half), low)):
                columns = slice(t * size, (t + 1) * size)
                base[ch, own, columns] = obj[ch, own, columns] + value * scale[own, columns]


def final_kernel(base, scale, side_l, side_r, in_top, in_bot, in_ctop, in_cbot, out):
    _, rows, columns = base.shape
    size = side_l.shape[1]
    half, tiles, chunks = size // 2, columns // size, rows // (size // 2)
    low = lanes(half, size) < half
    for chunk in range(chunks):
        own = slice(chunk * half, (chunk + 1) * half)
        for channel in range(2):

            def sides(from_l, from_r, channel=channel):
                from_l = from_l if channel == 0 else turn(from_l)
                from_r = turn(from_r) if channel == 0 else from_r
                return jnp.where(low, from_l, 0.0), jnp.where(low, 0.0, from_r)

            added = {}
            for where, rim, corner in ((0, in_top, in_ctop), (chunks - 1, in_bot, in_cbot)):
                if chunk == where:
                    for t in range(tiles):
                        value = rim[channel, :, t * size : (t + 1) * size]
                        added[t] = added[t] + value if t in added else value
                    for t, value in zip((0, tiles - 1), sides(corner[0], corner[1])):
                        added[t] = added[t] + value
            for t, value in zip((0, tiles - 1), sides(side_l[own, :], side_r[own, :])):
                added[t] = added[t] + value if t in added else value
            for t in range(tiles):
                at = slice(t * size, (t + 1) * size)
                value = base[channel, own, at]
                out[channel, own, at] = value + added[t] * scale[own, at] if t in added else value


def swap(axis, first):
    lower = range(first, lax.axis_size(axis) - 1, 2)
    return [(i, i + 1) for i in lower] + [(i + 1, i) for i in lower]


def ring(axis, by):
    count = lax.axis_size(axis)
    return [(i, (i + by) % count) for i in range(count)]


def move(x, axis, pairs):
    return lax.ppermute(x, axis, pairs)


def send_rims(side_1, side_2, ends_2, rim_1, rim_2, odd_row, odd_col):
    rows, size = side_1.shape
    half = size // 2
    ends_2 = move(ends_2, "col", swap("col", 1))
    in_1 = move(side_1, "col", swap("col", 0))
    in_2 = move(side_2, "col", swap("col", 1))
    rim_1 = move(rim_1, "row", swap("row", 0))
    rim_2 = move(rim_2, "row", swap("row", 1))

    def both(of_1, of_2):
        return jnp.where(odd_col, jnp.stack([of_1, of_2]), jnp.stack([of_2, of_1]))

    tops, bottoms = both(in_1[:half], ends_2[:half]), both(in_1[rows - half :], ends_2[half:])
    in_1 = in_1[half : rows - half]
    in_l, in_r = jnp.where(odd_col, in_1, in_2), jnp.where(odd_col, in_2, in_1)
    corner_1 = move(jnp.where(odd_row, tops, bottoms), "row", swap("row", 0))
    corner_2 = move(jnp.where(odd_row, bottoms, tops), "row", swap("row", 1))
    in_top, in_bot = jnp.where(odd_row, rim_1, rim_2), jnp.where(odd_row, rim_2, rim_1)
    in_ctop, in_cbot = jnp.where(odd_row, corner_1, corner_2), jnp.where(odd_row, corner_2, corner_1)
    return in_l, in_r, in_top, in_bot, in_ctop, in_cbot


def on_device(obj, probe, positions, counts, offsets, measured):
    offsets_count, _, size, _ = probe.shape
    scans = positions.shape[2]
    half = size // 2
    tile_rows, tile_columns = obj.shape[1:]
    rows, tiles = tile_rows + size, tile_columns // size + 1
    row_count = lax.axis_size("row")
    tables = dft_tables(size)

    def packed(x):
        return jnp.concatenate([x[0], x[1]], axis=1)

    at_row, at_col = lax.axis_index("row").astype(jnp.int32), lax.axis_index("col").astype(jnp.int32)
    odd_row, odd_col = lax.rem(at_row, 2) == 1, lax.rem(at_col, 2) == 1
    ends = jnp.where(odd_row, 0, tile_rows - half), jnp.where(odd_row, tile_rows - half, 0)
    which = lax.broadcasted_iota(jnp.int32, (1, scans), 1)
    places = jnp.where(which == 0, counts[0, 0], jnp.where(which == 1, at_row, at_col))
    joined = jnp.concatenate([positions[0, 0].T, offsets.T, places])
    first = lax.dynamic_slice_in_dim(obj, ends[0], half, axis=1)
    rows_1 = move(first, "row", swap("row", 0))
    later, _ = lax.optimization_barrier((obj, first))
    rows_2 = move(lax.dynamic_slice_in_dim(later, ends[1], half, axis=1), "row", swap("row", 1))
    top, bot = jnp.where(odd_row, rows_1, rows_2), jnp.where(odd_row, rows_2, rows_1)
    edge_l, edge_r, meta = call(
        edge_kernel,
        [(tile_rows, size)] * 2 + [jax.ShapeDtypeStruct((1, size), jnp.int32)],
        [VMEM, SMEM],
        (obj, joined),
        10**6,
    )

    most = offsets_count - 1
    metas = {0: meta, most: move(meta, "row", ring("row", most))}

    own_meta = jnp.broadcast_to(meta.astype(F32), (8, size))
    edge_l, edge_r = (
        jnp.concatenate([packed(top[:, :, part]), edge, packed(bot[:, :, part]), own_meta])
        for part, edge in ((slice(0, half), edge_l), (slice(tile_columns - half, None), edge_r))
    )
    columns_2 = move(jnp.where(odd_col, edge_r, edge_l), "col", swap("col", 1))
    columns_1 = move(jnp.where(odd_col, edge_l, edge_r), "col", swap("col", 0))
    left, right = jnp.where(odd_col, columns_1, columns_2), jnp.where(odd_col, columns_2, columns_1)
    (frame,) = call(frame_kernel, [(2, tiles, rows, size)], [VMEM] * 5, (obj, top, bot, left, right), 10**6)

    slots = scans // 2
    halves = ((0, slots), (slots, scans - slots))
    work = [
        pltpu.VMEM((slots * size, 2 * size), BF16),
        pltpu.VMEM((slots * size, 2 * size), BF16),
        pltpu.VMEM((2 * size, slots * size), BF16),
        pltpu.VMEM((2 * size, slots * size), BF16),
    ]
    flops = slots * 2 * 3 * 2 * size * (2 * size) ** 2

    far, wave, power = {}, {}, {}

    def forward(which, parts, arrived=None):
        outs = []
        for start, count in parts:
            tail = 8 if which and start == 0 else 0
            outs += [(2 * size, count * size), (count, 2, size, size), (count * size + tail, size)]
        adds = arrived is not None
        results = call(
            functools.partial(forward_kernel, [(which, *part) for part in parts], scans, adds),
            outs,
            [SMEM, VMEM, VMEM, VMEM] + [VMEM] * adds,
            (metas[which], frame, probe, tables) + ((arrived,) if adds else ()),
            flops * len(parts),
            work,
        )
        for at, (start, _) in enumerate(parts):
            far[which, start], wave[which, start], power[which, start] = results[3 * at : 3 * at + 3]

    forward(most, [halves[0]])
    forward(most, [halves[1]])
    forward(0, list(halves))
    for which in reversed(range(most)):
        for start, count in halves:
            arrived = move(power[which + 1, start], "row", ring("row", -1))
            if which:
                if start == 0:
                    metas[which] = arrived[count * size : count * size + 1].astype(jnp.int32)
                forward(which, [(start, count)], arrived)
            else:
                power[1, start] = arrived
    beside = jnp.concatenate([left[rows : rows + 1], right[rows : rows + 1], jnp.zeros((6, size), F32)])
    factors = {}
    for start, count in halves:
        args = [power[1, start], power[0, start], measured[0, 0, start : start + count].reshape(-1, size)]
        args += [beside] if start == 0 else []
        height = count * size + (beside.shape[0] if start == 0 else 0)
        (factors[start],) = call(factor_kernel, [(height, size)], [VMEM] * len(args), args, 10**6)

    row_count = lax.axis_size("row")
    kept = min(row_count, offsets_count + 2)
    weight = None

    def add_weight(index, shift, beside):
        nonlocal weight
        own = metas[shift] if shift in metas else None
        if own is None:
            span = move(jnp.concatenate([meta.astype(F32), beside[:2]]), "row", ring("row", shift))
            span = span.astype(jnp.int32)
        else:
            span = jnp.concatenate([own, beside[:2].astype(jnp.int32)])
        steps = [(d, w) for d in (-1, 0, 1) for w in range(offsets_count) if (w - d) % kept == index]
        (weight,) = call(
            functools.partial(weight_kernel, steps, scans, shift, row_count, weight is None),
            [(1, tiles + 1, tile_rows + 2 * size, size)],
            [SMEM, VMEM] + ([] if weight is None else [VMEM]),
            (span, probe) + (() if weight is None else (weight,)),
            flops,
            aliases={} if weight is None else {2: 0},
        )

    for index in range(offsets_count, kept):
        add_weight(index, index if index <= offsets_count else index - kept, beside)

    total = None
    for which in range(offsets_count):
        if which:
            for start, _ in halves:
                value = move(factors[start], "row", ring("row", 1))
                if start == 0 and which < most:
                    value, total = lax.optimization_barrier((value, total))
                factors[start] = value
            add_weight(which, which, factors[0][slots * size :])
        else:
            add_weight(0, 0, beside)
        groups = [[part] for part in halves] if which == most else [list(halves)]
        for group in groups:
            fresh, last = total is None, which == most and group[-1] == halves[-1]
            outs = [(2, tiles, rows, size)]
            if last:
                outs += [(rows, size), (tile_rows, size), (size, size)] + [(2, half, tile_columns)] * 2
            args = [metas[which], probe, tables]
            for start, _ in group:
                args += [far[which, start], wave[which, start], factors[start]]
            specs = [SMEM] + [VMEM] * (len(args) - 1)
            if not fresh:
                args, specs = args + [total], specs + [VMEM]
            total, *sides = call(
                functools.partial(backward_kernel, [(which, *part) for part in group], scans, row_count, fresh, last),
                outs,
                specs,
                args,
                flops * len(group),
                work,
                {} if fresh else {len(args) - 1: 0},
            )
    grad_in = send_rims(*sides, odd_row, odd_col)

    base, scale = call(inner_kernel, [obj.shape, obj.shape[1:]], [VMEM] * 3, (obj, weight, total), 10**6)
    (new_object,) = call(final_kernel, [obj.shape], [VMEM] * 8, (base, scale, *grad_in), 10**6)
    return new_object


def solution(mesh):
    return jax.shard_map(
        on_device,
        mesh=mesh,
        in_specs=(
            P(None, "row", "col"),
            P(),
            P("row", "col", None, None),
            P("row", "col"),
            P(),
            P("row", "col", None, None, None),
        ),
        out_specs=P(None, "row", "col"),
        check_vma=False,
    )
```

```python
import functools
import math

import jax
import jax.numpy as jnp
import numpy as np
from jax import lax
from jax.experimental import pallas as pl
from jax.experimental.pallas import tpu as pltpu
from jax.sharding import PartitionSpec as P

EPSILON = 0.5
DAMPING = 0.5


SMEM = pl.BlockSpec(memory_space=pltpu.SMEM)
VMEM = pl.BlockSpec(memory_space=pltpu.VMEM)
F32 = jnp.float32
BF16 = jnp.bfloat16


def call(kernel, outs, specs, args, flops, scratch=(), aliases=None):
    return pl.pallas_call(
        kernel,
        out_shape=[s if hasattr(s, "dtype") else jax.ShapeDtypeStruct(s, F32) for s in outs],
        in_specs=specs,
        out_specs=[VMEM] * len(outs),
        scratch_shapes=list(scratch),
        input_output_aliases=aliases or {},
        compiler_params=pltpu.CompilerParams(vmem_limit_bytes=16 * 2**20),
        cost_estimate=pl.CostEstimate(flops=flops, bytes_accessed=2**20, transcendentals=0),
    )(*args)


def dft_tables(length):
    index = np.arange(length)
    angle = (index[:, None] * index[None, :] % length) * (2.0 * math.pi / length)
    cos, sin = np.cos(angle) / math.sqrt(length), np.sin(angle) / math.sqrt(length)
    right = np.block([[cos, -sin], [sin, cos]])
    tables = []
    for table in (right, right.T):
        high = table.astype(BF16)
        tables += [high, (table - high.astype(np.float64)).astype(BF16)]
    return jnp.asarray(np.stack(tables))


def split(x):
    high = x.astype(BF16)
    return high, (x - high.astype(F32)).astype(BF16)


def dot3(a_high, a_low, b_high, b_low):
    dot = functools.partial(jnp.dot, preferred_element_type=F32)
    return dot(a_high, b_high) + (dot(a_low, b_high) + dot(a_high, b_low))


def lanes(rows, size):
    return lax.broadcasted_iota(jnp.int32, (rows, size), 1)


def turn(x):
    return pltpu.roll(x, x.shape[-1] // 2, 1)


def beam_of(meta, which, slot, scans, beams):
    beam = jnp.int32(0)
    for index in range(1, beams):
        beam = jnp.where(meta[0, 2 * scans + 3 + slot * beams + index] == which, index, beam)
    return beam


def place(meta, slot, size):
    y, x = meta[0, 2 * slot], meta[0, 2 * slot + 1]
    return y, x // size, x % size


def edge_kernel(obj, joined, edge_l, edge_r, meta):
    beams, scans = joined.shape[0] - 3, joined.shape[1]
    values = [joined[axis, slot] for slot in range(scans) for axis in range(2)]
    values += [joined[2 + beams, at] for at in range(3)]
    values += [joined[2 + beam, slot] for slot in range(scans) for beam in range(beams)]
    assert len(values) <= meta.shape[1]
    lane = lax.broadcasted_iota(jnp.int32, meta.shape, 1)
    row = jnp.zeros(meta.shape, jnp.int32)
    for at, value in enumerate(values):
        row = jnp.where(lane == at, value, row)
    meta[...] = row
    _, rows, columns = obj.shape
    size = edge_l.shape[1]
    low = lanes(rows, size) < size // 2
    near, far = slice(0, size), slice(columns - size, columns)
    edge_l[...] = jnp.where(low, obj[0, :, near], turn(obj[1, :, near]))
    edge_r[...] = jnp.where(low, turn(obj[0, :, far]), obj[1, :, far])


def frame_kernel(obj, top, bot, left, right, out):
    tiles, rows, size = out.shape[1:]
    half = size // 2
    low = lanes(half, size) < half
    for at in range(0, rows, half):
        body, src = obj, pl.ds(at - half, half)
        if at == 0:
            body, src = top, pl.ds(0, half)
        elif at == rows - half:
            body, src = bot, pl.ds(0, half)
        here = pl.ds(at, half)
        for ch in range(2):
            parts = [turn(body[ch, src, t * size : (t + 1) * size]) for t in range(tiles - 1)]
            edge_l, edge_r = left[here, :], right[here, :]
            edge_l = edge_l if ch == 0 else turn(edge_l)
            edge_r = turn(edge_r) if ch == 0 else edge_r
            parts = [edge_l, *parts, edge_r]
            for t in range(tiles):
                out[ch, t, here, :] = jnp.where(low, parts[t], parts[t + 1])


def forward_kernel(parts, scans, adds, *refs):
    meta, frame, probe, tables = refs[:4]
    refs = refs[4:]
    if adds:
        arrived, refs = refs[0], refs[1:]
    outs, (x_high, x_low, y_high, y_low) = refs[:-4], refs[-4:]
    size = probe.shape[-1]
    lane = lanes(size, size)
    for at, (which, start, slots) in enumerate(parts):
        far, wave, power = outs[3 * at : 3 * at + 3]
        for index in range(slots):
            slot = start + index
            y, tile, shift = place(meta, slot, size)
            beam = beam_of(meta, which, slot, scans, probe.shape[0])
            back = lax.rem(size - shift, size)
            patch = []
            for ch in range(2):
                near = pltpu.roll(frame[ch, tile, pl.ds(y, size), :], back, 1)
                rest = pltpu.roll(frame[ch, tile + 1, pl.ds(y, size), :], back, 1)
                patch.append(jnp.where(lane < size - shift, near, rest))
            probe_re, probe_im = probe[beam, 0], probe[beam, 1]
            waves = (
                probe_re * patch[0] - probe_im * patch[1],
                probe_re * patch[1] + probe_im * patch[0],
            )
            rows = slice(index * size, (index + 1) * size)
            for ch in range(2):
                wave[index, ch] = waves[ch]
                columns = slice(ch * size, (ch + 1) * size)
                x_high[rows, columns], x_low[rows, columns] = split(waves[ch])
        for slot in range(0, slots, 2):
            rows = slice(slot * size, (slot + 2) * size)
            mid = dot3(x_high[rows, :], x_low[rows, :], tables[0], tables[1])
            for sub in range(2):
                columns = slice((slot + sub) * size, (slot + sub + 1) * size)
                for ch in range(2):
                    piece = mid[sub * size : (sub + 1) * size, ch * size : (ch + 1) * size]
                    into = slice(ch * size, (ch + 1) * size)
                    y_high[into, columns], y_low[into, columns] = split(piece)
            columns = slice(slot * size, (slot + 2) * size)
            result = dot3(tables[2], tables[3], y_high[:, columns], y_low[:, columns])
            far[:, columns] = result
            for sub in range(2):
                inside = slice(sub * size, (sub + 1) * size)
                re, im = result[:size, inside], result[size:, inside]
                rows = slice((slot + sub) * size, (slot + sub + 1) * size)
                own = re * re + im * im
                power[rows, :] = own + arrived[rows, :] if adds else own
        if power.shape[0] > slots * size:
            lane = lanes(power.shape[0] - slots * size, size)
            row = jnp.zeros(lane.shape, jnp.int32)
            for index in range(2 * scans + 3 + scans * probe.shape[0]):
                row = jnp.where(lane == index, meta[0, index], row)
            power[slots * size :, :] = row.astype(F32)


def factor_kernel(arrived, own, measured, *refs):
    out = refs[-1]
    count = own.shape[0]
    total = own[...] + arrived[:count, :]
    out[:count, :] = measured[...] / jnp.sqrt(total + EPSILON)
    if len(refs) > 1:
        out[count:, :] = refs[0][...]


def add_patch(total, channel, y, tile, shift, value, lane):
    moved = pltpu.roll(value, shift, 1)
    rows = pl.ds(y, value.shape[0])
    total[channel, tile, rows, :] += jnp.where(lane >= shift, moved, 0.0)
    total[channel, tile + 1, rows, :] += jnp.where(lane < shift, moved, 0.0)


def write_sides(total, odd, side_1, side_2, ends_2):
    _, tiles, rows, size = total.shape
    low = lanes(rows, size) < size // 2
    left = jnp.where(low, total[0, 0], turn(total[1, 0]))
    right = jnp.where(low, turn(total[0, tiles - 1]), total[1, tiles - 1])
    side_1[...] = jnp.where(odd == 1, left, right)
    second = jnp.where(odd == 1, right, left)
    half = size // 2
    side_2[...] = second[half : rows - half, :]
    ends_2[:half, :] = second[:half, :]
    ends_2[half:, :] = second[rows - half :, :]


def own_columns(total, channel, rows, low):
    tiles = total.shape[1]
    turned = [turn(total[channel, t, rows, :]) for t in range(tiles)]
    return [jnp.where(low, turned[t], turned[t + 1]) for t in range(tiles - 1)]


def write_rims(total, odd, rim_1, rim_2):
    channels, _, rows, size = total.shape
    half = size // 2
    low = lanes(half, size) < half
    for ch in range(channels):
        tops = own_columns(total, ch, pl.ds(0, half), low)
        bottoms = own_columns(total, ch, pl.ds(rows - half, half), low)
        for t, (top, bottom) in enumerate(zip(tops, bottoms)):
            columns = slice(t * size, (t + 1) * size)
            rim_1[ch, :, columns] = jnp.where(odd == 1, top, bottom)
            rim_2[ch, :, columns] = jnp.where(odd == 1, bottom, top)


def backward_kernel(parts, scans, row_count, fresh, last, *refs):
    meta, probe, tables = refs[:3]
    inputs, refs = refs[3 : 3 + 3 * len(parts)], refs[3 + 3 * len(parts) :]
    if not fresh:
        refs = refs[1:]
    total, refs = refs[0], refs[1:]
    if last:
        (side_1, side_2, ends_2, rim_1, rim_2), refs = refs[:5], refs[5:]
    x_high, x_low, y_high, y_low = refs
    size = probe.shape[-1]
    lane = lanes(size, size)
    if fresh:
        total[...] = jnp.zeros_like(total)
    for at, (which, start, slots) in enumerate(parts):
        far, wave, factor = inputs[3 * at : 3 * at + 3]
        for slot in range(0, slots, 2):
            for sub in range(2):
                columns = slice((slot + sub) * size, (slot + sub + 1) * size)
                scale = factor[(slot + sub) * size : (slot + sub + 1) * size, :]
                for ch in range(2):
                    into = slice(ch * size, (ch + 1) * size)
                    y_high[into, columns], y_low[into, columns] = split(far[into, columns] * scale)
            columns = slice(slot * size, (slot + 2) * size)
            mid = dot3(tables[0], tables[1], y_high[:, columns], y_low[:, columns])
            for sub in range(2):
                rows = slice((slot + sub) * size, (slot + sub + 1) * size)
                for ch in range(2):
                    piece = mid[ch * size : (ch + 1) * size, sub * size : (sub + 1) * size]
                    into = slice(ch * size, (ch + 1) * size)
                    x_high[rows, into], x_low[rows, into] = split(piece)
            rows = slice(slot * size, (slot + 2) * size)
            result = dot3(x_high[rows, :], x_low[rows, :], tables[2], tables[3])
            for sub in range(2):
                true_slot = start + slot + sub
                live = (true_slot < meta[0, 2 * scans]).astype(F32)
                beam = beam_of(meta, which, true_slot, scans, probe.shape[0])
                probe_re, probe_im = probe[beam, 0], probe[beam, 1]
                inside = slice(sub * size, (sub + 1) * size)
                change_re = (result[inside, :size] - wave[slot + sub, 0]) * live
                change_im = (result[inside, size:] - wave[slot + sub, 1]) * live
                grad_re = probe_re * change_re + probe_im * change_im
                grad_im = probe_re * change_im - probe_im * change_re
                spot = place(meta, true_slot, size)
                add_patch(total, 0, *spot, grad_re, lane)
                add_patch(total, 1, *spot, grad_im, lane)
    if last:
        odd = lax.rem(meta[0, 2 * scans + 2], 2)
        write_sides(total, odd, side_1, side_2, ends_2)
        odd = lax.rem(lax.rem(meta[0, 2 * scans + 1] + parts[0][0], row_count), 2)
        write_rims(total, odd, rim_1, rim_2)


def weight_kernel(steps, scans, which_tile, row_count, fresh, *refs):
    metas, probe, total = refs[0], refs[1], refs[-1]
    _, tiles, rows, size = total.shape
    half = size // 2
    own_rows, own_columns = rows - 2 * size, (tiles - 2) * size
    lane = lanes(size, size)
    if fresh:
        total[...] = jnp.zeros_like(total)
    at_row = lax.rem(metas[0, 2 * scans + 1] + which_tile + row_count, row_count)
    for row, across in enumerate((0, -1, 1)):
        for down, which in steps:

            def add(slot, carry, row=row, across=across, down=down, which=which):
                y = metas[row, 2 * slot] + (down * own_rows + half)
                x = metas[row, 2 * slot + 1] + (across * own_columns + half)
                near = (y > 0) & (y < rows - size) & (x > 0) & (x < (tiles - 1) * size)
                below = at_row + down
                live = (slot < metas[row, 2 * scans]) & (below >= 0) & (below < row_count)

                @pl.when(near & live)
                def _():
                    beam = beam_of(metas, which, slot, scans, probe.shape[0])
                    probe_re, probe_im = probe[beam, 0], probe[beam, 1]
                    value = probe_re * probe_re + probe_im * probe_im
                    add_patch(total, 0, y, x // size, x % size, value, lane)

                return carry

            lax.fori_loop(0, scans, add, 0)


def inner_kernel(obj, weight, total, base, scale):
    _, tiles, _, size = total.shape
    half = size // 2
    low = lanes(half, size) < half
    for chunk in range(obj.shape[1] // half):
        own = slice(chunk * half, (chunk + 1) * half)
        for t in range(tiles - 1):
            columns = slice(t * size, (t + 1) * size)
            scale[own, columns] = 1.0 / (weight[0, t + 1, pl.ds(size + chunk * half, half), :] + DAMPING)
        for ch in range(2):
            for t, value in enumerate(own_columns(total, ch, pl.ds((chunk + 1) * half, half), low)):
                columns = slice(t * size, (t + 1) * size)
                base[ch, own, columns] = obj[ch, own, columns] + value * scale[own, columns]


def final_kernel(base, scale, side_l, side_r, in_top, in_bot, in_ctop, in_cbot, out):
    _, rows, columns = base.shape
    size = side_l.shape[1]
    half, tiles, chunks = size // 2, columns // size, rows // (size // 2)
    low = lanes(half, size) < half
    for chunk in range(chunks):
        own = slice(chunk * half, (chunk + 1) * half)
        for channel in range(2):

            def sides(from_l, from_r, channel=channel):
                from_l = from_l if channel == 0 else turn(from_l)
                from_r = turn(from_r) if channel == 0 else from_r
                return jnp.where(low, from_l, 0.0), jnp.where(low, 0.0, from_r)

            added = {}
            for where, rim, corner in ((0, in_top, in_ctop), (chunks - 1, in_bot, in_cbot)):
                if chunk == where:
                    for t in range(tiles):
                        value = rim[channel, :, t * size : (t + 1) * size]
                        added[t] = added[t] + value if t in added else value
                    for t, value in zip((0, tiles - 1), sides(corner[0], corner[1])):
                        added[t] = added[t] + value
            for t, value in zip((0, tiles - 1), sides(side_l[own, :], side_r[own, :])):
                added[t] = added[t] + value if t in added else value
            for t in range(tiles):
                at = slice(t * size, (t + 1) * size)
                value = base[channel, own, at]
                out[channel, own, at] = value + added[t] * scale[own, at] if t in added else value


def swap(axis, first):
    lower = range(first, lax.axis_size(axis) - 1, 2)
    return [(i, i + 1) for i in lower] + [(i + 1, i) for i in lower]


def ring(axis, by):
    count = lax.axis_size(axis)
    return [(i, (i + by) % count) for i in range(count)]


def move(x, axis, pairs):
    return lax.ppermute(x, axis, pairs)


def send_rims(side_1, side_2, ends_2, rim_1, rim_2, odd_row, odd_col):
    rows, size = side_1.shape
    half = size // 2
    ends_2 = move(ends_2, "col", swap("col", 1))
    in_1 = move(side_1, "col", swap("col", 0))
    in_2 = move(side_2, "col", swap("col", 1))
    rim_1 = move(rim_1, "row", swap("row", 0))
    rim_2 = move(rim_2, "row", swap("row", 1))

    def both(of_1, of_2):
        return jnp.where(odd_col, jnp.stack([of_1, of_2]), jnp.stack([of_2, of_1]))

    tops, bottoms = both(in_1[:half], ends_2[:half]), both(in_1[rows - half :], ends_2[half:])
    in_1 = in_1[half : rows - half]
    in_l, in_r = jnp.where(odd_col, in_1, in_2), jnp.where(odd_col, in_2, in_1)
    corner_1 = move(jnp.where(odd_row, tops, bottoms), "row", swap("row", 0))
    corner_2 = move(jnp.where(odd_row, bottoms, tops), "row", swap("row", 1))
    in_top, in_bot = jnp.where(odd_row, rim_1, rim_2), jnp.where(odd_row, rim_2, rim_1)
    in_ctop, in_cbot = jnp.where(odd_row, corner_1, corner_2), jnp.where(odd_row, corner_2, corner_1)
    return in_l, in_r, in_top, in_bot, in_ctop, in_cbot


def on_device(obj, probe, positions, counts, offsets, measured):
    offsets_count, _, size, _ = probe.shape
    scans = positions.shape[2]
    half = size // 2
    tile_rows, tile_columns = obj.shape[1:]
    rows, tiles = tile_rows + size, tile_columns // size + 1
    row_count = lax.axis_size("row")
    tables = dft_tables(size)

    def packed(x):
        return jnp.concatenate([x[0], x[1]], axis=1)

    at_row, at_col = lax.axis_index("row").astype(jnp.int32), lax.axis_index("col").astype(jnp.int32)
    odd_row, odd_col = lax.rem(at_row, 2) == 1, lax.rem(at_col, 2) == 1
    ends = jnp.where(odd_row, 0, tile_rows - half), jnp.where(odd_row, tile_rows - half, 0)
    which = lax.broadcasted_iota(jnp.int32, (1, scans), 1)
    places = jnp.where(which == 0, counts[0, 0], jnp.where(which == 1, at_row, at_col))
    joined = jnp.concatenate([positions[0, 0].T, offsets.T, places])
    rows_1, rows_2 = (
        move(lax.dynamic_slice_in_dim(obj, ends[i], half, axis=1), "row", swap("row", i))
        for i in range(2)
    )
    top, bot = jnp.where(odd_row, rows_1, rows_2), jnp.where(odd_row, rows_2, rows_1)
    edge_l, edge_r, meta = call(
        edge_kernel,
        [(tile_rows, size)] * 2 + [jax.ShapeDtypeStruct((1, size), jnp.int32)],
        [VMEM, SMEM],
        (obj, joined),
        10**6,
    )

    most = offsets_count - 1
    metas = {0: meta, most: move(meta, "row", ring("row", most))}

    own_meta = jnp.broadcast_to(meta.astype(F32), (8, size))
    edge_l, edge_r = (
        jnp.concatenate([packed(top[:, :, part]), edge, packed(bot[:, :, part]), own_meta])
        for part, edge in ((slice(0, half), edge_l), (slice(tile_columns - half, None), edge_r))
    )
    columns_2 = move(jnp.where(odd_col, edge_r, edge_l), "col", swap("col", 1))
    columns_1 = move(jnp.where(odd_col, edge_l, edge_r), "col", swap("col", 0))
    left, right = jnp.where(odd_col, columns_1, columns_2), jnp.where(odd_col, columns_2, columns_1)
    (frame,) = call(frame_kernel, [(2, tiles, rows, size)], [VMEM] * 5, (obj, top, bot, left, right), 10**6)

    slots = scans // 2
    halves = ((0, slots), (slots, scans - slots))
    work = [
        pltpu.VMEM((slots * size, 2 * size), BF16),
        pltpu.VMEM((slots * size, 2 * size), BF16),
        pltpu.VMEM((2 * size, slots * size), BF16),
        pltpu.VMEM((2 * size, slots * size), BF16),
    ]
    flops = slots * 2 * 3 * 2 * size * (2 * size) ** 2

    far, wave, power = {}, {}, {}

    def forward(which, parts, arrived=None):
        outs = []
        for start, count in parts:
            tail = 8 if which and start == 0 else 0
            outs += [(2 * size, count * size), (count, 2, size, size), (count * size + tail, size)]
        adds = arrived is not None
        results = call(
            functools.partial(forward_kernel, [(which, *part) for part in parts], scans, adds),
            outs,
            [SMEM, VMEM, VMEM, VMEM] + [VMEM] * adds,
            (metas[which], frame, probe, tables) + ((arrived,) if adds else ()),
            flops * len(parts),
            work,
        )
        for at, (start, _) in enumerate(parts):
            far[which, start], wave[which, start], power[which, start] = results[3 * at : 3 * at + 3]

    forward(most, [halves[0]])
    forward(most, [halves[1]])
    forward(0, list(halves))
    for which in reversed(range(most)):
        for start, count in halves:
            arrived = move(power[which + 1, start], "row", ring("row", -1))
            if which:
                if start == 0:
                    metas[which] = arrived[count * size : count * size + 1].astype(jnp.int32)
                forward(which, [(start, count)], arrived)
            else:
                power[1, start] = arrived
    beside = jnp.concatenate([left[rows : rows + 1], right[rows : rows + 1], jnp.zeros((6, size), F32)])
    factors = {}
    for start, count in halves:
        args = [power[1, start], power[0, start], measured[0, 0, start : start + count].reshape(-1, size)]
        args += [beside] if start == 0 else []
        height = count * size + (beside.shape[0] if start == 0 else 0)
        (factors[start],) = call(factor_kernel, [(height, size)], [VMEM] * len(args), args, 10**6)

    row_count = lax.axis_size("row")
    kept = min(row_count, offsets_count + 2)
    weight = None

    def add_weight(index, shift, beside):
        nonlocal weight
        own = metas[shift] if shift in metas else None
        if own is None:
            span = move(jnp.concatenate([meta.astype(F32), beside[:2]]), "row", ring("row", shift))
            span = span.astype(jnp.int32)
        else:
            span = jnp.concatenate([own, beside[:2].astype(jnp.int32)])
        steps = [(d, w) for d in (-1, 0, 1) for w in range(offsets_count) if (w - d) % kept == index]
        (weight,) = call(
            functools.partial(weight_kernel, steps, scans, shift, row_count, weight is None),
            [(1, tiles + 1, tile_rows + 2 * size, size)],
            [SMEM, VMEM] + ([] if weight is None else [VMEM]),
            (span, probe) + (() if weight is None else (weight,)),
            flops,
            aliases={} if weight is None else {2: 0},
        )

    for index in range(offsets_count, kept):
        add_weight(index, index if index <= offsets_count else index - kept, beside)

    total = None
    for which in range(offsets_count):
        if which:
            for start, _ in halves:
                value = move(factors[start], "row", ring("row", 1))
                if start == 0 and which < most:
                    value, total = lax.optimization_barrier((value, total))
                factors[start] = value
            add_weight(which, which, factors[0][slots * size :])
        else:
            add_weight(0, 0, beside)
        groups = [[part] for part in halves] if which == most else [list(halves)]
        for group in groups:
            fresh, last = total is None, which == most and group[-1] == halves[-1]
            outs = [(2, tiles, rows, size)]
            if last:
                outs += [(rows, size), (tile_rows, size), (size, size)] + [(2, half, tile_columns)] * 2
            args = [metas[which], probe, tables]
            for start, _ in group:
                args += [far[which, start], wave[which, start], factors[start]]
            specs = [SMEM] + [VMEM] * (len(args) - 1)
            if not fresh:
                args, specs = args + [total], specs + [VMEM]
            total, *sides = call(
                functools.partial(backward_kernel, [(which, *part) for part in group], scans, row_count, fresh, last),
                outs,
                specs,
                args,
                flops * len(group),
                work,
                {} if fresh else {len(args) - 1: 0},
            )
    grad_in = send_rims(*sides, odd_row, odd_col)

    base, scale = call(inner_kernel, [obj.shape, obj.shape[1:]], [VMEM] * 3, (obj, weight, total), 10**6)
    (new_object,) = call(final_kernel, [obj.shape], [VMEM] * 8, (base, scale, *grad_in), 10**6)
    return new_object


def solution(mesh):
    return jax.shard_map(
        on_device,
        mesh=mesh,
        in_specs=(
            P(None, "row", "col"),
            P(),
            P("row", "col", None, None),
            P("row", "col"),
            P(),
            P("row", "col", None, None, None),
        ),
        out_specs=P(None, "row", "col"),
        check_vma=False,
    )
```

```python
import functools
import math

import jax
import jax.numpy as jnp
import numpy as np
from jax import lax
from jax.experimental import pallas as pl
from jax.experimental.pallas import tpu as pltpu
from jax.sharding import PartitionSpec as P

EPSILON = 0.5
DAMPING = 0.5


SMEM = pl.BlockSpec(memory_space=pltpu.SMEM)
VMEM = pl.BlockSpec(memory_space=pltpu.VMEM)
F32 = jnp.float32
BF16 = jnp.bfloat16


def call(kernel, outs, specs, args, flops, scratch=(), aliases=None):
    return pl.pallas_call(
        kernel,
        out_shape=[s if hasattr(s, "dtype") else jax.ShapeDtypeStruct(s, F32) for s in outs],
        in_specs=specs,
        out_specs=[VMEM] * len(outs),
        scratch_shapes=list(scratch),
        input_output_aliases=aliases or {},
        compiler_params=pltpu.CompilerParams(vmem_limit_bytes=16 * 2**20),
        cost_estimate=pl.CostEstimate(flops=flops, bytes_accessed=2**20, transcendentals=0),
    )(*args)


def dft_tables(length):
    index = np.arange(length)
    angle = (index[:, None] * index[None, :] % length) * (2.0 * math.pi / length)
    cos, sin = np.cos(angle) / math.sqrt(length), np.sin(angle) / math.sqrt(length)
    right = np.block([[cos, -sin], [sin, cos]])
    tables = []
    for table in (right, right.T):
        high = table.astype(BF16)
        tables += [high, (table - high.astype(np.float64)).astype(BF16)]
    return jnp.asarray(np.stack(tables))


def split(x):
    high = x.astype(BF16)
    return high, (x - high.astype(F32)).astype(BF16)


def dot3(a_high, a_low, b_high, b_low):
    dot = functools.partial(jnp.dot, preferred_element_type=F32)
    return dot(a_high, b_high) + (dot(a_low, b_high) + dot(a_high, b_low))


def lanes(rows, size):
    return lax.broadcasted_iota(jnp.int32, (rows, size), 1)


def turn(x):
    return pltpu.roll(x, x.shape[-1] // 2, 1)


def beam_of(meta, which, slot, scans, beams):
    beam = jnp.int32(0)
    for index in range(1, beams):
        beam = jnp.where(meta[0, 2 * scans + 3 + slot * beams + index] == which, index, beam)
    return beam


def place(meta, slot, size):
    y, x = meta[0, 2 * slot], meta[0, 2 * slot + 1]
    return y, x // size, x % size


def edge_kernel(obj, positions, counts, offsets, place_of, edge_l, edge_r, meta):
    scans = positions.shape[2]
    values = [positions[0, 0, slot, axis] for slot in range(scans) for axis in range(2)]
    values += [counts[0, 0], place_of[0], place_of[1]]
    values += [offsets[slot, beam] for slot in range(scans) for beam in range(offsets.shape[1])]
    assert len(values) <= meta.shape[1]
    lane = lax.broadcasted_iota(jnp.int32, meta.shape, 1)
    row = jnp.zeros(meta.shape, jnp.int32)
    for at, value in enumerate(values):
        row = jnp.where(lane == at, value, row)
    meta[...] = row
    _, rows, columns = obj.shape
    size = edge_l.shape[1]
    low = lanes(rows, size) < size // 2
    near, far = slice(0, size), slice(columns - size, columns)
    edge_l[...] = jnp.where(low, obj[0, :, near], turn(obj[1, :, near]))
    edge_r[...] = jnp.where(low, turn(obj[0, :, far]), obj[1, :, far])


def frame_kernel(obj, top, bot, left, right, out):
    tiles, rows, size = out.shape[1:]
    half = size // 2
    low = lanes(half, size) < half
    for at in range(0, rows, half):
        body, src = obj, pl.ds(at - half, half)
        if at == 0:
            body, src = top, pl.ds(0, half)
        elif at == rows - half:
            body, src = bot, pl.ds(0, half)
        here = pl.ds(at, half)
        for ch in range(2):
            parts = [turn(body[ch, src, t * size : (t + 1) * size]) for t in range(tiles - 1)]
            edge_l, edge_r = left[here, :], right[here, :]
            edge_l = edge_l if ch == 0 else turn(edge_l)
            edge_r = turn(edge_r) if ch == 0 else edge_r
            parts = [edge_l, *parts, edge_r]
            for t in range(tiles):
                out[ch, t, here, :] = jnp.where(low, parts[t], parts[t + 1])


def forward_kernel(parts, scans, adds, *refs):
    meta, frame, probe, tables = refs[:4]
    refs = refs[4:]
    if adds:
        arrived, refs = refs[0], refs[1:]
    outs, (x_high, x_low, y_high, y_low) = refs[:-4], refs[-4:]
    size = probe.shape[-1]
    lane = lanes(size, size)
    for at, (which, start, slots) in enumerate(parts):
        far, wave, power = outs[3 * at : 3 * at + 3]
        for index in range(slots):
            slot = start + index
            y, tile, shift = place(meta, slot, size)
            beam = beam_of(meta, which, slot, scans, probe.shape[0])
            back = lax.rem(size - shift, size)
            patch = []
            for ch in range(2):
                near = pltpu.roll(frame[ch, tile, pl.ds(y, size), :], back, 1)
                rest = pltpu.roll(frame[ch, tile + 1, pl.ds(y, size), :], back, 1)
                patch.append(jnp.where(lane < size - shift, near, rest))
            probe_re, probe_im = probe[beam, 0], probe[beam, 1]
            waves = (
                probe_re * patch[0] - probe_im * patch[1],
                probe_re * patch[1] + probe_im * patch[0],
            )
            rows = slice(index * size, (index + 1) * size)
            for ch in range(2):
                wave[index, ch] = waves[ch]
                columns = slice(ch * size, (ch + 1) * size)
                x_high[rows, columns], x_low[rows, columns] = split(waves[ch])
        for slot in range(0, slots, 2):
            rows = slice(slot * size, (slot + 2) * size)
            mid = dot3(x_high[rows, :], x_low[rows, :], tables[0], tables[1])
            for sub in range(2):
                columns = slice((slot + sub) * size, (slot + sub + 1) * size)
                for ch in range(2):
                    piece = mid[sub * size : (sub + 1) * size, ch * size : (ch + 1) * size]
                    into = slice(ch * size, (ch + 1) * size)
                    y_high[into, columns], y_low[into, columns] = split(piece)
            columns = slice(slot * size, (slot + 2) * size)
            result = dot3(tables[2], tables[3], y_high[:, columns], y_low[:, columns])
            far[:, columns] = result
            for sub in range(2):
                inside = slice(sub * size, (sub + 1) * size)
                re, im = result[:size, inside], result[size:, inside]
                rows = slice((slot + sub) * size, (slot + sub + 1) * size)
                own = re * re + im * im
                power[rows, :] = own + arrived[rows, :] if adds else own
        if power.shape[0] > slots * size:
            lane = lanes(power.shape[0] - slots * size, size)
            row = jnp.zeros(lane.shape, jnp.int32)
            for index in range(2 * scans + 3 + scans * probe.shape[0]):
                row = jnp.where(lane == index, meta[0, index], row)
            power[slots * size :, :] = row.astype(F32)


def factor_kernel(arrived, own, measured, *refs):
    out = refs[-1]
    count = own.shape[0]
    total = own[...] + arrived[:count, :]
    out[:count, :] = measured[...] / jnp.sqrt(total + EPSILON)
    if len(refs) > 1:
        out[count:, :] = refs[0][...]


def add_patch(total, channel, y, tile, shift, value, lane):
    moved = pltpu.roll(value, shift, 1)
    rows = pl.ds(y, value.shape[0])
    total[channel, tile, rows, :] += jnp.where(lane >= shift, moved, 0.0)
    total[channel, tile + 1, rows, :] += jnp.where(lane < shift, moved, 0.0)


def write_sides(total, odd, side_1, side_2, ends_2):
    _, tiles, rows, size = total.shape
    low = lanes(rows, size) < size // 2
    left = jnp.where(low, total[0, 0], turn(total[1, 0]))
    right = jnp.where(low, turn(total[0, tiles - 1]), total[1, tiles - 1])
    side_1[...] = jnp.where(odd == 1, left, right)
    second = jnp.where(odd == 1, right, left)
    half = size // 2
    side_2[...] = second[half : rows - half, :]
    ends_2[:half, :] = second[:half, :]
    ends_2[half:, :] = second[rows - half :, :]


def own_columns(total, channel, rows, low):
    tiles = total.shape[1]
    turned = [turn(total[channel, t, rows, :]) for t in range(tiles)]
    return [jnp.where(low, turned[t], turned[t + 1]) for t in range(tiles - 1)]


def write_rims(total, odd, rim_1, rim_2):
    channels, _, rows, size = total.shape
    half = size // 2
    low = lanes(half, size) < half
    for ch in range(channels):
        tops = own_columns(total, ch, pl.ds(0, half), low)
        bottoms = own_columns(total, ch, pl.ds(rows - half, half), low)
        for t, (top, bottom) in enumerate(zip(tops, bottoms)):
            columns = slice(t * size, (t + 1) * size)
            rim_1[ch, :, columns] = jnp.where(odd == 1, top, bottom)
            rim_2[ch, :, columns] = jnp.where(odd == 1, bottom, top)


def backward_kernel(parts, scans, row_count, fresh, last, *refs):
    meta, probe, tables = refs[:3]
    inputs, refs = refs[3 : 3 + 3 * len(parts)], refs[3 + 3 * len(parts) :]
    if not fresh:
        refs = refs[1:]
    total, refs = refs[0], refs[1:]
    if last:
        (side_1, side_2, ends_2, rim_1, rim_2), refs = refs[:5], refs[5:]
    x_high, x_low, y_high, y_low = refs
    size = probe.shape[-1]
    lane = lanes(size, size)
    if fresh:
        total[...] = jnp.zeros_like(total)
    for at, (which, start, slots) in enumerate(parts):
        far, wave, factor = inputs[3 * at : 3 * at + 3]
        for slot in range(0, slots, 2):
            for sub in range(2):
                columns = slice((slot + sub) * size, (slot + sub + 1) * size)
                scale = factor[(slot + sub) * size : (slot + sub + 1) * size, :]
                for ch in range(2):
                    into = slice(ch * size, (ch + 1) * size)
                    y_high[into, columns], y_low[into, columns] = split(far[into, columns] * scale)
            columns = slice(slot * size, (slot + 2) * size)
            mid = dot3(tables[0], tables[1], y_high[:, columns], y_low[:, columns])
            for sub in range(2):
                rows = slice((slot + sub) * size, (slot + sub + 1) * size)
                for ch in range(2):
                    piece = mid[ch * size : (ch + 1) * size, sub * size : (sub + 1) * size]
                    into = slice(ch * size, (ch + 1) * size)
                    x_high[rows, into], x_low[rows, into] = split(piece)
            rows = slice(slot * size, (slot + 2) * size)
            result = dot3(x_high[rows, :], x_low[rows, :], tables[2], tables[3])
            for sub in range(2):
                true_slot = start + slot + sub
                live = (true_slot < meta[0, 2 * scans]).astype(F32)
                beam = beam_of(meta, which, true_slot, scans, probe.shape[0])
                probe_re, probe_im = probe[beam, 0], probe[beam, 1]
                inside = slice(sub * size, (sub + 1) * size)
                change_re = (result[inside, :size] - wave[slot + sub, 0]) * live
                change_im = (result[inside, size:] - wave[slot + sub, 1]) * live
                grad_re = probe_re * change_re + probe_im * change_im
                grad_im = probe_re * change_im - probe_im * change_re
                spot = place(meta, true_slot, size)
                add_patch(total, 0, *spot, grad_re, lane)
                add_patch(total, 1, *spot, grad_im, lane)
    if last:
        odd = lax.rem(meta[0, 2 * scans + 2], 2)
        write_sides(total, odd, side_1, side_2, ends_2)
        odd = lax.rem(lax.rem(meta[0, 2 * scans + 1] + parts[0][0], row_count), 2)
        write_rims(total, odd, rim_1, rim_2)


def weight_kernel(steps, scans, which_tile, row_count, fresh, *refs):
    metas, probe, total = refs[0], refs[1], refs[-1]
    _, tiles, rows, size = total.shape
    half = size // 2
    own_rows, own_columns = rows - 2 * size, (tiles - 2) * size
    lane = lanes(size, size)
    if fresh:
        total[...] = jnp.zeros_like(total)
    at_row = lax.rem(metas[0, 2 * scans + 1] + which_tile + row_count, row_count)
    for row, across in enumerate((0, -1, 1)):
        for down, which in steps:

            def add(slot, carry, row=row, across=across, down=down, which=which):
                y = metas[row, 2 * slot] + (down * own_rows + half)
                x = metas[row, 2 * slot + 1] + (across * own_columns + half)
                near = (y > 0) & (y < rows - size) & (x > 0) & (x < (tiles - 1) * size)
                below = at_row + down
                live = (slot < metas[row, 2 * scans]) & (below >= 0) & (below < row_count)

                @pl.when(near & live)
                def _():
                    beam = beam_of(metas, which, slot, scans, probe.shape[0])
                    probe_re, probe_im = probe[beam, 0], probe[beam, 1]
                    value = probe_re * probe_re + probe_im * probe_im
                    add_patch(total, 0, y, x // size, x % size, value, lane)

                return carry

            lax.fori_loop(0, scans, add, 0)


def inner_kernel(obj, weight, total, base, scale):
    _, tiles, _, size = total.shape
    half = size // 2
    low = lanes(half, size) < half
    for chunk in range(obj.shape[1] // half):
        own = slice(chunk * half, (chunk + 1) * half)
        for t in range(tiles - 1):
            columns = slice(t * size, (t + 1) * size)
            scale[own, columns] = 1.0 / (weight[0, t + 1, pl.ds(size + chunk * half, half), :] + DAMPING)
        for ch in range(2):
            for t, value in enumerate(own_columns(total, ch, pl.ds((chunk + 1) * half, half), low)):
                columns = slice(t * size, (t + 1) * size)
                base[ch, own, columns] = obj[ch, own, columns] + value * scale[own, columns]


def final_kernel(base, scale, side_l, side_r, in_top, in_bot, in_ctop, in_cbot, out):
    _, rows, columns = base.shape
    size = side_l.shape[1]
    half, tiles, chunks = size // 2, columns // size, rows // (size // 2)
    low = lanes(half, size) < half
    for chunk in range(chunks):
        own = slice(chunk * half, (chunk + 1) * half)
        for channel in range(2):

            def sides(from_l, from_r, channel=channel):
                from_l = from_l if channel == 0 else turn(from_l)
                from_r = turn(from_r) if channel == 0 else from_r
                return jnp.where(low, from_l, 0.0), jnp.where(low, 0.0, from_r)

            added = {}
            for where, rim, corner in ((0, in_top, in_ctop), (chunks - 1, in_bot, in_cbot)):
                if chunk == where:
                    for t in range(tiles):
                        value = rim[channel, :, t * size : (t + 1) * size]
                        added[t] = added[t] + value if t in added else value
                    for t, value in zip((0, tiles - 1), sides(corner[0], corner[1])):
                        added[t] = added[t] + value
            for t, value in zip((0, tiles - 1), sides(side_l[own, :], side_r[own, :])):
                added[t] = added[t] + value if t in added else value
            for t in range(tiles):
                at = slice(t * size, (t + 1) * size)
                value = base[channel, own, at]
                out[channel, own, at] = value + added[t] * scale[own, at] if t in added else value


def swap(axis, first):
    lower = range(first, lax.axis_size(axis) - 1, 2)
    return [(i, i + 1) for i in lower] + [(i + 1, i) for i in lower]


def ring(axis, by):
    count = lax.axis_size(axis)
    return [(i, (i + by) % count) for i in range(count)]


def move(x, axis, pairs):
    return lax.ppermute(x, axis, pairs)


def send_rims(side_1, side_2, ends_2, rim_1, rim_2, odd_row, odd_col):
    rows, size = side_1.shape
    half = size // 2
    ends_2 = move(ends_2, "col", swap("col", 1))
    in_1 = move(side_1, "col", swap("col", 0))
    in_2 = move(side_2, "col", swap("col", 1))
    rim_1 = move(rim_1, "row", swap("row", 0))
    rim_2 = move(rim_2, "row", swap("row", 1))

    def both(of_1, of_2):
        return jnp.where(odd_col, jnp.stack([of_1, of_2]), jnp.stack([of_2, of_1]))

    tops, bottoms = both(in_1[:half], ends_2[:half]), both(in_1[rows - half :], ends_2[half:])
    in_1 = in_1[half : rows - half]
    in_l, in_r = jnp.where(odd_col, in_1, in_2), jnp.where(odd_col, in_2, in_1)
    corner_1 = move(jnp.where(odd_row, tops, bottoms), "row", swap("row", 0))
    corner_2 = move(jnp.where(odd_row, bottoms, tops), "row", swap("row", 1))
    in_top, in_bot = jnp.where(odd_row, rim_1, rim_2), jnp.where(odd_row, rim_2, rim_1)
    in_ctop, in_cbot = jnp.where(odd_row, corner_1, corner_2), jnp.where(odd_row, corner_2, corner_1)
    return in_l, in_r, in_top, in_bot, in_ctop, in_cbot


def on_device(obj, probe, positions, counts, offsets, measured):
    offsets_count, _, size, _ = probe.shape
    scans = positions.shape[2]
    half = size // 2
    tile_rows, tile_columns = obj.shape[1:]
    rows, tiles = tile_rows + size, tile_columns // size + 1
    row_count = lax.axis_size("row")
    tables = dft_tables(size)

    def packed(x):
        return jnp.concatenate([x[0], x[1]], axis=1)

    at_row, at_col = lax.axis_index("row").astype(jnp.int32), lax.axis_index("col").astype(jnp.int32)
    odd_row, odd_col = lax.rem(at_row, 2) == 1, lax.rem(at_col, 2) == 1
    ends = jnp.where(odd_row, 0, tile_rows - half), jnp.where(odd_row, tile_rows - half, 0)
    rows_1, rows_2 = (
        move(lax.dynamic_slice_in_dim(obj, ends[i], half, axis=1), "row", swap("row", i))
        for i in range(2)
    )
    top, bot = jnp.where(odd_row, rows_1, rows_2), jnp.where(odd_row, rows_2, rows_1)
    edge_l, edge_r, meta = call(
        edge_kernel,
        [(tile_rows, size)] * 2 + [jax.ShapeDtypeStruct((1, size), jnp.int32)],
        [VMEM, SMEM, SMEM, SMEM, SMEM],
        (obj, positions, counts, offsets, jnp.stack([at_row, at_col])),
        10**6,
    )

    most = offsets_count - 1
    metas = {0: meta, most: move(meta, "row", ring("row", most))}

    own_meta = jnp.broadcast_to(meta.astype(F32), (8, size))
    edge_l, edge_r = (
        jnp.concatenate([packed(top[:, :, part]), edge, packed(bot[:, :, part]), own_meta])
        for part, edge in ((slice(0, half), edge_l), (slice(tile_columns - half, None), edge_r))
    )
    columns_2 = move(jnp.where(odd_col, edge_r, edge_l), "col", swap("col", 1))
    columns_1 = move(jnp.where(odd_col, edge_l, edge_r), "col", swap("col", 0))
    left, right = jnp.where(odd_col, columns_1, columns_2), jnp.where(odd_col, columns_2, columns_1)
    (frame,) = call(frame_kernel, [(2, tiles, rows, size)], [VMEM] * 5, (obj, top, bot, left, right), 10**6)

    slots = scans // 2
    halves = ((0, slots), (slots, scans - slots))
    work = [
        pltpu.VMEM((slots * size, 2 * size), BF16),
        pltpu.VMEM((slots * size, 2 * size), BF16),
        pltpu.VMEM((2 * size, slots * size), BF16),
        pltpu.VMEM((2 * size, slots * size), BF16),
    ]
    flops = slots * 2 * 3 * 2 * size * (2 * size) ** 2

    far, wave, power = {}, {}, {}

    def forward(which, parts, arrived=None):
        outs = []
        for start, count in parts:
            tail = 8 if which and start == 0 else 0
            outs += [(2 * size, count * size), (count, 2, size, size), (count * size + tail, size)]
        adds = arrived is not None
        results = call(
            functools.partial(forward_kernel, [(which, *part) for part in parts], scans, adds),
            outs,
            [SMEM, VMEM, VMEM, VMEM] + [VMEM] * adds,
            (metas[which], frame, probe, tables) + ((arrived,) if adds else ()),
            flops * len(parts),
            work,
        )
        for at, (start, _) in enumerate(parts):
            far[which, start], wave[which, start], power[which, start] = results[3 * at : 3 * at + 3]

    forward(most, [halves[0]])
    forward(most, [halves[1]])
    forward(0, list(halves))
    for which in reversed(range(most)):
        for start, count in halves:
            arrived = move(power[which + 1, start], "row", ring("row", -1))
            if which:
                if start == 0:
                    metas[which] = arrived[count * size : count * size + 1].astype(jnp.int32)
                forward(which, [(start, count)], arrived)
            else:
                power[1, start] = arrived
    beside = jnp.concatenate([left[rows : rows + 1], right[rows : rows + 1], jnp.zeros((6, size), F32)])
    factors = {}
    for start, count in halves:
        args = [power[1, start], power[0, start], measured[0, 0, start : start + count].reshape(-1, size)]
        args += [beside] if start == 0 else []
        height = count * size + (beside.shape[0] if start == 0 else 0)
        (factors[start],) = call(factor_kernel, [(height, size)], [VMEM] * len(args), args, 10**6)

    row_count = lax.axis_size("row")
    kept = min(row_count, offsets_count + 2)
    weight = None

    def add_weight(index, shift, beside):
        nonlocal weight
        own = metas[shift] if shift in metas else None
        if own is None:
            span = move(jnp.concatenate([meta.astype(F32), beside[:2]]), "row", ring("row", shift))
            span = span.astype(jnp.int32)
        else:
            span = jnp.concatenate([own, beside[:2].astype(jnp.int32)])
        steps = [(d, w) for d in (-1, 0, 1) for w in range(offsets_count) if (w - d) % kept == index]
        (weight,) = call(
            functools.partial(weight_kernel, steps, scans, shift, row_count, weight is None),
            [(1, tiles + 1, tile_rows + 2 * size, size)],
            [SMEM, VMEM] + ([] if weight is None else [VMEM]),
            (span, probe) + (() if weight is None else (weight,)),
            flops,
            aliases={} if weight is None else {2: 0},
        )

    for index in range(offsets_count, kept):
        add_weight(index, index if index <= offsets_count else index - kept, beside)

    total = None
    for which in range(offsets_count):
        if which:
            for start, _ in halves:
                value = move(factors[start], "row", ring("row", 1))
                if start == 0 and which < most:
                    value, total = lax.optimization_barrier((value, total))
                factors[start] = value
            add_weight(which, which, factors[0][slots * size :])
        else:
            add_weight(0, 0, beside)
        groups = [[part] for part in halves] if which == most else [list(halves)]
        for group in groups:
            fresh, last = total is None, which == most and group[-1] == halves[-1]
            outs = [(2, tiles, rows, size)]
            if last:
                outs += [(rows, size), (tile_rows, size), (size, size)] + [(2, half, tile_columns)] * 2
            args = [metas[which], probe, tables]
            for start, _ in group:
                args += [far[which, start], wave[which, start], factors[start]]
            specs = [SMEM] + [VMEM] * (len(args) - 1)
            if not fresh:
                args, specs = args + [total], specs + [VMEM]
            total, *sides = call(
                functools.partial(backward_kernel, [(which, *part) for part in group], scans, row_count, fresh, last),
                outs,
                specs,
                args,
                flops * len(group),
                work,
                {} if fresh else {len(args) - 1: 0},
            )
    grad_in = send_rims(*sides, odd_row, odd_col)

    base, scale = call(inner_kernel, [obj.shape, obj.shape[1:]], [VMEM] * 3, (obj, weight, total), 10**6)
    (new_object,) = call(final_kernel, [obj.shape], [VMEM] * 8, (base, scale, *grad_in), 10**6)
    return new_object


def solution(mesh):
    return jax.shard_map(
        on_device,
        mesh=mesh,
        in_specs=(
            P(None, "row", "col"),
            P(),
            P("row", "col", None, None),
            P("row", "col"),
            P(),
            P("row", "col", None, None, None),
        ),
        out_specs=P(None, "row", "col"),
        check_vma=False,
    )
```
